32 devices in a mesh: context: 2 (over core), tensor: 4 (over y, x), fsdp: 4 (over z).
Axes of the slice: x: 2, y: 2, z: 4, core: 2. Of those that a mesh axis runs over, the one named last changes fastest.
Arguments:
- input_raw: bfloat16 [4, 1024, 5120], P('fsdp', ('context', 'tensor')), may hold values from -6 to 6
- state_proj_raw: bfloat16 [4, 1024, 256], P('fsdp', ('context', 'tensor')), may hold values from -6 to 6
- gate_branch: bfloat16 [4, 1024, 5120], P('fsdp', ('context', 'tensor')), may hold values from -6 to 6
- step_raw: bfloat16 [4, 1024, 80], P('fsdp', ('context', 'tensor')), may hold values from -6 to 6
- convolution_taps: float32 [4, 5376], replicated, may hold values from -3 to 3
- convolution_bias: float32 [5376], replicated, may hold values from -3 to 3
- step_bias: float32 [80], P('tensor'), may hold values from -1.5 to 0.5
- decay_log_rate: float32 [80], P('tensor'), may hold values from -13 to -2, as said below
- skip_weight: float32 [80], P('tensor'), may hold values from 0.5 to 2
- gated_norm_gain: float32 [5120], P('tensor'), may hold values from 0.1 to 1.9
- output_weight: bfloat16 [5120, 2560], P('tensor', 'fsdp'), may hold values from -0.078125 to 0.078125
- adapter_down: bfloat16 [5120, 16], P('tensor'), may hold values from -0.078125 to 0.078125
- adapter_up: bfloat16 [16, 2560], replicated, may hold values from -0.29882812 to 0.29882812
- cotangent: bfloat16 [4, 1024, 2560], P('fsdp', ('context', 'tensor')), may hold values from -6 to 6
Outputs:
- mixed: bfloat16 [4, 1024, 2560], P('fsdp', ('context', 'tensor'))
- grad_a: float32 [5120, 16], P('tensor')
- grad_b: float32 [16, 2560], replicated
The draws below stay inside these ranges and needn't reach their ends.
Inputs may be any that keep to these rules, and one draw needn't show every extreme that they name: `decay_log_rate`: logarithms of positive decay rates.
All inputs are finite; a program needn't handle non-finite values.
Results may differ from the reference program's by a relative error of at most 0.017.
Values may be sent and summed in bfloat16 or wider, within the bound.
A program may use at most 128 MiB of HBM per device.

```python
import math
import jax
import jax.numpy as jnp
from jax import lax

MODEL_WIDTH = 2560
H = 80
N = 128
ADAPTER_RANK = 16
CONV = 4
MIXER_WIDTH = 5120
SEQS = 4
LEN = 1024


def draw_decay_log_rate(key, part):
    pick_key, slow_key, fast_key = jax.random.split(jax.random.fold_in(key, 11), 3)
    keep_share = 5
    slow_mask = jax.random.randint(pick_key, (H,), 0, 10) < keep_share
    low_log = jnp.log(0.5 / LEN)
    high_log = jnp.log(2.5 / LEN)
    slow_rate = jax.random.uniform(slow_key, (H,), jnp.float32, low_log, high_log)
    fast_rate = jnp.log(jax.random.uniform(fast_key, (H,), jnp.float32, 1.0 / 60.0, 1.0 / 20.0))
    return jnp.where(slow_mask, slow_rate, fast_rate)


def block_levels(rng, dims, cuts, low, largest):
    gain, own = 1.0, jax.random.fold_in(rng, 6)
    for position, parts in cuts:
        heights = jnp.exp(jax.random.uniform(jax.random.fold_in(own, position), (parts,), jnp.float32, low / len(cuts), largest / len(cuts)))
        gain = gain * jnp.repeat(heights, dims[position] // parts).reshape([-1 if axis == position else 1 for axis in range(len(dims))])
    return gain


def centred(stream_key, dims, width, reach, cuts=(), held_as=jnp.bfloat16):
    level = block_levels(stream_key, dims, cuts, -0.22, 0.18) if cuts else 1.0
    result = jax.random.normal(stream_key, dims, jnp.float32) * width * level
    return jnp.minimum(jnp.maximum(result, -reach), reach).astype(held_as)


def setup_inputs(seed: int = 0) -> dict:
    arg_keys = jax.random.split(jax.random.key(seed), 15)
    input_raw = centred(arg_keys[0], (SEQS, LEN, MIXER_WIDTH), 1.0, 6.0, ((0, 4), (1, 8)))
    state_proj_raw = centred(arg_keys[1], (SEQS, LEN, 2 * N), 1.0, 6.0, ((0, 4), (1, 8)))
    gate_branch = centred(arg_keys[2], (SEQS, LEN, MIXER_WIDTH), 1.0, 6.0, ((0, 4), (1, 8)))
    step_raw = centred(arg_keys[3], (SEQS, LEN, H), 1.0, 6.0, ((0, 4), (1, 8)))
    convolution_taps = centred(arg_keys[4], (CONV, MIXER_WIDTH + 2 * N), CONV ** -0.5, 3.0, (), jnp.float32)
    convolution_bias = centred(arg_keys[5], (MIXER_WIDTH + 2 * N,), 0.5, 3.0, (), jnp.float32)
    step_bias = jnp.clip(-1.5 + 2.0 * jax.random.uniform(arg_keys[6], (H,), jnp.float32) ** block_levels(arg_keys[6], (H,), ((0, 4),), -0.2, 0.2), -1.5, 0.5)
    decay_log_rate = draw_decay_log_rate(jax.random.fold_in(arg_keys[14], 71), 0)
    skip_weight = jnp.clip(0.5 + 1.5 * jax.random.uniform(arg_keys[8], (H,), jnp.float32) ** block_levels(arg_keys[8], (H,), ((0, 4),), -0.2, 0.2), 0.5, 2.0)
    gated_norm_gain = jnp.clip(1.0 + 0.18 * jax.random.normal(arg_keys[9], (MIXER_WIDTH,), jnp.float32), 0.1, 1.9)
    output_weight = centred(arg_keys[10], (MIXER_WIDTH, MODEL_WIDTH), MIXER_WIDTH ** -0.5, 0.078125, ((0, 4), (1, 4)))
    adapter_down = centred(arg_keys[11], (MIXER_WIDTH, ADAPTER_RANK), MIXER_WIDTH ** -0.5, 0.078125, ((0, 4),))
    adapter_up = centred(arg_keys[12], (ADAPTER_RANK, MODEL_WIDTH), 0.05, 0.29882812)
    cotangent = centred(arg_keys[13], (SEQS, LEN, MODEL_WIDTH), 1.0, 6.0, ((0, 4), (1, 8)))
    return dict(input_raw=input_raw, state_proj_raw=state_proj_raw, gate_branch=gate_branch, step_raw=step_raw, convolution_taps=convolution_taps, convolution_bias=convolution_bias, step_bias=step_bias, decay_log_rate=decay_log_rate, skip_weight=skip_weight, gated_norm_gain=gated_norm_gain, output_weight=output_weight, adapter_down=adapter_down, adapter_up=adapter_up, cotangent=cotangent)


def ssd_blocks(x_heads, b_rows, c_rows, step_size, log_decay, block_len):
    highest = lax.Precision.HIGHEST
    length = x_heads.shape[0]
    head_count = x_heads.shape[1]
    head_size = x_heads.shape[2]
    state_size = b_rows.shape[1]
    blocks = length // block_len
    causal = jnp.arange(block_len)[:, None] >= jnp.arange(block_len)[None, :]

    def advance(state_now, pieces):
        x_block, b_block, c_block, step_block, decay_block = pieces
        cum_decay = jnp.cumsum(decay_block, axis=0)
        cum_heads = cum_decay.T
        gap_decay = cum_heads[:, :, None] - cum_heads[:, None, :]
        decay_mat = jnp.where(causal[None], jnp.exp(jnp.where(causal[None], gap_decay, 0.0)), 0.0)
        gram_mat = jnp.dot(c_block, b_block.T, precision=highest)
        x_scaled = x_block * step_block[:, :, None]
        y_inner = jnp.einsum('hij,jhp->ihp', decay_mat * gram_mat[None], x_scaled, precision=highest)
        y_state = jnp.exp(cum_decay)[:, :, None] * jnp.einsum('in,hpn->ihp', c_block, state_now, precision=highest)
        tail_decay = jnp.exp(cum_decay[-1][None, :] - cum_decay)
        state_next = jnp.exp(cum_decay[-1])[:, None, None] * state_now + jnp.einsum('jhp,jn->hpn', x_scaled * tail_decay[:, :, None], b_block, precision=highest)
        return (state_next, y_inner + y_state)
    start_state = jnp.zeros((head_count, head_size, state_size), jnp.float32)
    state_end, y_blocks = lax.scan(advance, start_state, (x_heads.reshape(blocks, block_len, head_count, head_size), b_rows.reshape(blocks, block_len, state_size), c_rows.reshape(blocks, block_len, state_size), step_size.reshape(blocks, block_len, head_count), log_decay.reshape(blocks, block_len, head_count)))
    return (y_blocks.reshape(length, head_count, head_size), state_end)

def reference(input_raw, state_proj_raw, gate_branch, step_raw, convolution_taps, convolution_bias, step_bias, decay_log_rate, skip_weight, gated_norm_gain, output_weight, adapter_down, adapter_up, cotangent):
    highest = lax.Precision.HIGHEST
    inner_width = input_raw.shape[2]
    state_size = state_proj_raw.shape[2] // 2
    head_count = decay_log_rate.shape[0]
    head_size = inner_width // head_count
    length = input_raw.shape[1]
    taps = convolution_taps.shape[0]
    block_len = math.gcd(length, 256)
    lowrank_factor = 2.0 / math.sqrt(input_raw.shape[0] * length)
    decay_rate = jnp.exp(decay_log_rate)

    def one_sequence(pieces):
        x_seq, bc_seq, z_seq, dt_seq, cotangent_sequence = pieces
        joined = jnp.concatenate([x_seq, bc_seq], axis=1)
        padded = jnp.concatenate([jnp.zeros((taps - 1, joined.shape[1]), joined.dtype), joined], axis=0)
        pre_act = convolution_bias[None, :] + convolution_taps[0][None, :] * padded[0:length].astype(jnp.float32)
        for tap_index in range(1, taps):
            pre_act = pre_act + convolution_taps[tap_index][None, :] * padded[tap_index:tap_index + length].astype(jnp.float32)
        xbc = jax.nn.silu(pre_act).astype(jnp.bfloat16)
        x_heads = xbc[:, :inner_width].astype(jnp.float32).reshape(length, head_count, head_size)
        b_rows = xbc[:, inner_width:inner_width + state_size].astype(jnp.float32)
        c_rows = xbc[:, inner_width + state_size:].astype(jnp.float32)
        step_size = jax.nn.softplus(dt_seq.astype(jnp.float32) + step_bias[None, :])
        log_decay = -step_size * decay_rate[None, :]
        y_heads, state_end = ssd_blocks(x_heads, b_rows, c_rows, step_size, log_decay, block_len)
        y_heads = y_heads + skip_weight[None, :, None] * x_heads
        gated = y_heads.reshape(length, inner_width) * jax.nn.silu(z_seq.astype(jnp.float32))
        row_norm_scale = lax.rsqrt(lax.optimization_barrier(jnp.mean(gated * gated, axis=1)) + 1e-05)
        gated_output = (gated * gated_norm_gain[None, :]).astype(jnp.bfloat16)
        adapter_branch = jnp.dot(gated_output, adapter_down, preferred_element_type=jnp.float32).astype(jnp.bfloat16)
        frozen_piece = jnp.dot(gated_output, output_weight, preferred_element_type=jnp.float32)
        frozen_piece = frozen_piece + 2.0 * jnp.dot(adapter_branch, adapter_up, preferred_element_type=jnp.float32)
        mixed = (row_norm_scale[:, None] * frozen_piece).astype(jnp.bfloat16)
        weighted = lowrank_factor * row_norm_scale[:, None] * adapter_branch.astype(jnp.float32)
        grad_b_part = jnp.dot(weighted.T, cotangent_sequence.astype(jnp.float32), precision=highest)
        adapter_gradient = lowrank_factor * row_norm_scale[:, None] * jnp.dot(cotangent_sequence, adapter_up.T, preferred_element_type=jnp.float32)
        grad_a_part = jnp.dot(gated_output.astype(jnp.float32).T, adapter_gradient, precision=highest)
        return (mixed, grad_a_part, grad_b_part)
    mixed, grad_a_parts, grad_b_parts = lax.map(one_sequence, (input_raw, state_proj_raw, gate_branch, step_raw, cotangent))
    return (mixed, lax.optimization_barrier(jnp.sum(grad_a_parts, axis=0)), lax.optimization_barrier(jnp.sum(grad_b_parts, axis=0)))
```

```python
import functools
import math

import jax
import jax.numpy as jnp
from jax import lax
from jax.experimental import pallas as pl
from jax.experimental.pallas import tpu as pltpu
from jax.sharding import PartitionSpec as P

EPS = 1e-05
MESH = pl.DeviceIdType.MESH
HI = lax.Precision.HIGHEST
BF = jnp.bfloat16
F32 = jnp.float32
HALO = 16


def dot(a, b, ca=1, cb=0, precision=None):
    return lax.dot_general(
        a, b, (((ca,), (cb,)), ((), ())), preferred_element_type=F32, precision=precision
    )


def iota(shape, dim):
    return lax.broadcasted_iota(jnp.int32, shape, dim)


def pick(values, i):
    out = jnp.int32(values[0])
    for k in range(1, len(values)):
        out = jnp.where(i == k, jnp.int32(values[k]), out)
    return out


def column_chunks(width):
    lanes = width // 128
    first = -(-lanes // 2)
    return [(0, first * 128), (first * 128, (lanes - first) * 128)] if lanes > 1 else [(0, width)]


def kernel(
    nt, nf, nc, hl,
    x_hbm, bc_hbm, z_ref, dt_hbm, taps_hbm, bias_hbm, sb_ref, dr_ref, sk_ref, gain_hbm, w_ref, down_hbm, up_hbm, cot_hbm,
    mixed_ref, ga_ref, gb_ref,
    x_ref, bc_ref, dt_ref, taps_ref, bias_ref, gain_ref, down_ref, up_ref, cot_ref,
    halo_x, halo_bc, x_send, x_all, z_all, bc_all, dt_all, wbuf, a_s, step_s, at_s, stept_s,
    stl, msg, st_in, inc_s, e_s, y_s, g_s, adx, ad_in, ag_own, ag_all, gb_own, gb_in,
    comb, comb_c, comb2, comb_f, seg_own, seg_in, full, fin, rs_send, rs_recv,
    ld, h_ss, h_rs, dt_ss, dt_rs, bc_ss, bc_rs, x_ss, x_rs, z_ss, z_rs, w_ss, w_rs, wf_ss, wf_rs, st_ss, st_rs,
    ad_ss, ad_rs, ag_ss, ag_rs, ga_ss, ga_rs, cc_ss, cc_rs, cf_ss, cf_rs, sg_ss, sg_rs, fin_ss, fin_rs, r_ss, r_rs, loc,
):
    t = lax.axis_index("tensor")
    f = lax.axis_index("fsdp")
    c = lax.axis_index("context")
    L = x_ref.shape[0]
    LW = x_all.shape[1]
    W = w_ref.shape[1]
    N = bc_ref.shape[1] // 2
    R = w_ref.shape[0] // nc
    HS = LW // hl
    idx = c * nt + t
    total = nc * nt
    bits = [1 << i for i in range(nt.bit_length() - 1)]
    chunks = column_chunks(W)
    steps = nf - 1

    def peer(e):
        out = 0
        for bit in bits:
            out = out + bit * lax.rem(lax.div(t, bit) + lax.div(e, bit), 2)
        return out

    def peers():
        return [peer(jnp.int32(e)) for e in range(nt)]

    pt = peers()

    def place(i):
        return {"context": i // nt, "tensor": lax.rem(i, nt)}

    def remote(src, dst, ss, rs, dev):
        return pltpu.make_async_remote_copy(
            src_ref=src, dst_ref=dst, send_sem=ss, recv_sem=rs, device_id=dev, device_id_type=MESH
        )

    def copy(src, dst, ss, rs, dev):
        cp = remote(src, dst, ss, rs, dev)
        cp.start()
        return cp

    loads = []
    for i, (src, dst) in enumerate((
        (x_hbm, x_ref), (bc_hbm, bc_ref), (dt_hbm, dt_ref), (taps_hbm, taps_ref), (bias_hbm, bias_ref),
        (gain_hbm, gain_ref), (down_hbm, down_ref), (up_hbm, up_ref), (cot_hbm, cot_ref),
    )):
        cp = pltpu.make_async_copy(src, dst, ld.at[i])
        cp.start()
        loads.append(cp)
    own_w = pltpu.make_async_copy(w_ref, wbuf.at[f], loc.at[0])
    own_w.start()
    own_rows = pl.ds(pl.multiple_of(t * L, L), L)
    own_cols = pl.ds(pl.multiple_of(t * LW, 128), LW)
    own_z = pltpu.make_async_copy(z_ref.at[:, own_cols], z_all.at[own_rows, :], loc.at[1])
    own_z.start()

    nxt, prv = lax.rem(idx + 1, total), lax.rem(idx + total - 1, total)
    bar = pltpu.get_barrier_semaphore()
    greet = [{"tensor": pt[e]} for e in range(1, nt)]
    greet += [{"fsdp": lax.rem(f + d, nf)} for d in range(1, nf)]
    greet += [{"context": lax.rem(c + k, nc)} for k in range(1, nc)]
    greet += [place(nxt), place(prv)]
    for dev in greet:
        pl.semaphore_signal(bar, inc=1, device_id=dev, device_id_type=MESH)
    for cp in loads:
        cp.wait()
    dt_all[t] = dt_ref[...]
    pl.semaphore_wait(bar, len(greet))

    h1 = copy(x_ref.at[L - HALO : L, :], halo_x, h_ss.at[0], h_rs.at[0], place(nxt))
    h2 = copy(bc_ref.at[L - HALO : L, :], halo_bc, h_ss.at[1], h_rs.at[1], place(nxt))
    dts = [copy(dt_ref, dt_all.at[t], dt_ss.at[e], dt_rs.at[e], {"tensor": pt[e]}) for e in range(1, nt)]
    share = pl.ds(pl.multiple_of(c * R, 16), R)

    def w_copy(dr, s, ch, q):
        cols = pl.ds(chunks[ch][0], chunks[ch][1])
        src = w_ref.at[share, cols] if s == 0 else wbuf.at[q, share, cols]
        to = f + 1 if dr == 0 else f - 1
        return remote(src, wbuf.at[q, share, cols], w_ss.at[dr, s, ch], w_rs.at[dr, s, ch], {"fsdp": to})

    def w_share(dr, s, ch, q, k):
        region = wbuf.at[q, share, pl.ds(chunks[ch][0], chunks[ch][1])]
        return remote(region, region, wf_ss.at[dr, s, ch, k], wf_rs.at[dr, s, ch, k], {"context": lax.rem(c + k, nc)})

    def has_next(dr):
        return f + 1 < nf if dr == 0 else f >= 1

    def sends(dr, s):
        return (f - s >= 0) & (f + 1 < nf) if dr == 0 else (f + s < nf) & (f >= 1)

    def gets(dr, s):
        return f - 1 - s >= 0 if dr == 0 else f + 1 + s < nf

    def came(dr, s):
        return f - 1 - s if dr == 0 else f + 1 + s

    for ch in range(len(chunks)):
        for dr in range(2):
            @pl.when(sends(dr, 0))
            def _(dr=dr, ch=ch):
                w_copy(dr, 0, ch, f).start()

    def w_arrive(s, ch):
        for dr in range(2):
            @pl.when(gets(dr, s))
            def _(dr=dr):
                q = came(dr, s)
                w_copy(dr, s, ch, q).wait_recv()
                if s + 1 < steps:
                    @pl.when(has_next(dr))
                    def _():
                        w_copy(dr, s + 1, ch, q).start()
                for k in range(1, nc):
                    w_share(dr, s, ch, q, k).start()

    table = [sorted(range(nf), key=lambda q, g=g: (abs(q - g), q)) for g in range(nf)]
    order = [pick([table[g][i] for g in range(nf)], f) for i in range(nf)]
    way = [pick([int(table[g][i] > g) for g in range(nf)], f) for i in range(nf)]
    dist = [pick([max(abs(table[g][i] - g) - 1, 0) for g in range(nf)], f) for i in range(nf)]

    def w_ready(slot, ch):
        region = wbuf.at[order[slot], share, pl.ds(chunks[ch][0], chunks[ch][1])]
        for k in range(1, nc):
            remote(
                region, region, wf_ss.at[way[slot], dist[slot], ch, k], wf_rs.at[way[slot], dist[slot], ch, k],
                {"context": lax.rem(c + k, nc)},
            ).wait_recv()

    def send_gate(e):
        cols = pl.ds(pl.multiple_of(pt[e] * LW, 128), LW)
        return copy(z_ref.at[:, cols], z_all.at[own_rows, :], z_ss.at[e], z_rs.at[e], {"tensor": pt[e]})

    early = nt - 1 if nt > 2 else nt
    zs = [send_gate(e) for e in range(1, early)]
    h1.wait()
    h2.wait()
    live = (idx > 0).astype(F32)

    def conv(src, halo, col, tap_col):
        lanes = pl.ds(col, 128)
        wide = pl.ds(tap_col, 128)
        ext = jnp.concatenate([halo[HALO - 8 : HALO, lanes].astype(F32) * live, src[:, lanes].astype(F32)], axis=0)
        acc = bias_ref[:, wide] + taps_ref[0:1, wide] * ext[5 : 5 + L]
        for k in range(1, 4):
            acc = acc + taps_ref[k : k + 1, wide] * ext[5 + k : 5 + k + L]
        return (acc / (1.0 + jnp.exp(-acc))).astype(BF)

    wide0 = x_ref.shape[1]
    for j in range(2 * N // 128):
        bc_all[own_rows, j * 128 : (j + 1) * 128] = conv(bc_ref, halo_bc, j * 128, wide0 + j * 128)
    bcs = [
        copy(bc_all.at[own_rows, :], bc_all.at[own_rows, :], bc_ss.at[e], bc_rs.at[e], {"tensor": pt[e]})
        for e in range(1, nt)
    ]
    xs = []

    def conv_group(e, store):
        base = pt[e] * LW

        def lap(j, carry):
            col = pl.multiple_of(base + j * 128, 128)
            store(pl.ds(pl.multiple_of(j * 128, 128), 128), conv(x_ref, halo_x, col, col))
            return carry

        lax.fori_loop(0, LW // 128, lap, 0)

    for e in range(nt - 1, 0, -1):
        def put(lanes, val, e=e):
            x_send[e - 1, :, lanes] = val

        conv_group(e, put)
        xs.append(copy(x_send.at[e - 1], x_all.at[own_rows, :], x_ss.at[e], x_rs.at[e], {"tensor": pt[e]}))
    zs += [send_gate(e) for e in range(early, nt)]

    def put_own(lanes, val):
        x_all[own_rows, lanes] = val

    conv_group(0, put_own)
    e_s[...] = (iota((128, LW), 1) // HS == iota((128, LW), 0)).astype(F32)
    spread16 = e_s[...].astype(BF)

    def spread(rows):
        return dot(jnp.broadcast_to(rows, (8, 128)), e_s[...], precision=HI)

    for cp in dts:
        cp.wait()
    HR = at_s.shape[1]
    HA = dt_ref.shape[0]
    sel = ((iota((HA, 128), 0) == iota((HA, 128), 1) + t * hl) & (iota((HA, 128), 1) < hl)).astype(BF)
    sel_t = ((iota((HR, HA), 1) == iota((HR, HA), 0) + t * hl) & (iota((HR, HA), 0) < hl)).astype(BF)
    eye = (iota((HR, 128), 0) == iota((HR, 128), 1)).astype(F32)
    place_head = (iota((hl, 128), 0) == iota((hl, 128), 1)).astype(F32)
    hp = [
        dot(jnp.broadcast_to(v[...], (8, hl)), place_head, precision=HI)[0:1, :] for v in (sb_ref, dr_ref, sk_ref)
    ]
    hp_t = [dot(eye, jnp.broadcast_to(v, (8, 128)), 1, 1, HI)[:, 0:1] for v in hp[0:2]]
    tri = (iota((L, L), 0) >= iota((L, L), 1)).astype(F32)

    def softplus(v):
        return jnp.maximum(v, 0.0) + jnp.log1p(jnp.exp(-jnp.abs(v)))

    for b in range(nt):
        rows = slice(b * L, (b + 1) * L)
        raw = dt_all[b]
        step = softplus(dot(raw, sel, 0, 0) + hp[0])
        step_s[rows, :] = step
        a_s[rows, :] = dot(tri, -step * jnp.exp(hp[1]), precision=HI)
        step_t = softplus(dot(sel_t, raw) + hp_t[0])
        stept_s[b] = step_t
        at_s[b] = dot(-step_t * jnp.exp(hp_t[1]), tri, 1, 1, HI)
    cu = dot(up_ref[...], cot_ref[...], 1, 1)
    for ch in range(len(chunks)):
        w_arrive(0, ch)
    for cp in bcs:
        cp.wait()
    for cp in xs:
        cp.wait()

    state = jnp.zeros((N, LW), F32)
    before = jnp.zeros((1, 128), F32)
    for b in range(nt):
        rows = slice(b * L, (b + 1) * L)
        stl[b, 0:N, :] = state
        stl[b, N : N + 8, :] = spread(jnp.exp(before))
        a = a_s[rows, :]
        last = a[L - 1 : L, :]
        weight = (jnp.exp(last - a) * step_s[rows, :]).astype(BF)
        xw = (x_all[rows, :].astype(F32) * dot(weight, spread16)).astype(BF)
        state = spread(jnp.exp(last))[0:1, :] * state + dot(bc_all[rows, 0:N], xw, 0, 0)
        before = before + last
    msg[0:N, :] = state
    msg[N : N + 8, :] = spread(before)
    sts = [
        copy(msg, st_in.at[c], st_ss.at[k], st_rs.at[k], {"context": lax.rem(c + k, nc)})
        for k in range(1, nc)
    ]

    left = iota((L, 2 * HS), 1) < HS

    def inner(b, carry):
        rows = pl.ds(pl.multiple_of(b * L, L), L)
        gram = dot(bc_all[rows, N : 2 * N], bc_all[rows, 0:N], 1, 1)
        gram = jnp.where(iota((L, L), 0) >= iota((L, L), 1), gram, 0.0)
        a = a_s[rows, :]
        at = at_s[b]
        stt = stept_s[b]
        for pair in range(hl // 2):
            lanes = slice(pair * 2 * HS, (pair + 1) * 2 * HS)
            xp = x_all[rows, lanes]
            out = []
            for h in (2 * pair, 2 * pair + 1):
                gap = jnp.minimum(a[:, h : h + 1] - at[h : h + 1, :], 0.0)
                m = (jnp.exp(gap) * gram * stt[h : h + 1, :]).astype(BF)
                out.append(dot(m, xp))
            y_s[rows, lanes] = jnp.where(left, out[0], out[1])
        return carry

    lax.fori_loop(0, nt, inner, 0)

    for cp in sts:
        cp.wait()
    inc_s[...] = jnp.zeros_like(inc_s)

    def chain(k, carry):
        inc_s[...] = jnp.exp(st_in[k, N : N + 1, :]) * inc_s[...] + st_in[k, 0:N, :]
        return carry

    lax.fori_loop(0, c, chain, 0)
    own_w.wait()
    skip = spread(hp[2])[0:1, :]
    ones = jnp.ones((8, LW), BF)

    def scatter(unit, b, cols):
        return remote(
            rs_send.at[pl.ds(pl.multiple_of(b * L, L), L), cols], rs_recv.at[t, :, cols],
            r_ss.at[unit, b], r_rs.at[unit, t], {"tensor": b},
        )

    def scattered(unit, b, cols):
        return remote(
            rs_send.at[pl.ds(pl.multiple_of(b * L, L), L), cols], rs_recv.at[b, :, cols],
            r_ss.at[unit, b], r_rs.at[unit, b], {"tensor": b},
        )

    units = [(0, None, 0, W)] + [(s, ch) + chunks[ch] for s in range(1, nf) for ch in range(len(chunks))]
    spans = [pl.ds(pl.multiple_of(order[s] * W + off, 128), wide) for s, _, off, wide in units]

    def gate(e, carry):
        b = peer(e)
        rows = pl.ds(pl.multiple_of(b * L, L), L)

        @pl.when(e == 0)
        def _():
            own_z.wait()

        @pl.when(e > 0)
        def _():
            remote(
                z_ref.at[:, own_cols], z_all.at[rows, :], z_ss.at[e], z_rs.at[e], {"tensor": b}
            ).wait_recv()

        start = (stl[b, 0:N, :] + stl[b, N : N + 1, :] * inc_s[...]).astype(BF)
        reach = dot(jnp.exp(a_s[rows, :]).astype(BF), spread16)
        y = y_s[rows, :] + reach * dot(bc_all[rows, N : 2 * N], start)
        y = y + skip * x_all[rows, :].astype(F32)
        z = z_all[rows, :].astype(F32)
        g = y * (z / (1.0 + jnp.exp(-z)))
        out = (g * gain_ref[...]).astype(BF)
        g_s[rows, :] = out
        adx[b, 0:16, :] = dot(down_ref[...], out, 1, 1)
        adx[b, 16:24, :] = dot(ones, (g * g).astype(BF), 1, 1)

        @pl.when(e > 0)
        def _():
            remote(adx.at[b], ad_in.at[e], ad_ss.at[e], ad_rs.at[e], {"tensor": b}).start()

        rs_send[rows, spans[0]] = dot(out, wbuf[f]).astype(BF)

        @pl.when(e > 0)
        def _():
            scatter(0, b, spans[0]).start()

        return carry

    lax.fori_loop(0, nt, gate, 0)

    half = (nt * L) // 2

    def project(u):
        slot, ch, off, wide = units[u]
        w_ready(slot, ch)

        def lap(i, carry):
            rows = pl.ds(pl.multiple_of(i * half, half), half)
            rs_send[rows, spans[u]] = dot(g_s[rows, :], wbuf[order[slot], :, off : off + wide]).astype(BF)
            for j in range(half // L):
                b = i * (half // L) + j

                @pl.when(b != t)
                def _():
                    scatter(u, b, spans[u]).start()

            return carry

        lax.fori_loop(0, 2, lap, 0)

    nch = len(chunks)
    if steps > 1:
        w_arrive(1, 0)
    for ch in range(nch):
        project(1 + ch)
    for e in range(1, nt):
        remote(adx.at[pt[e]], ad_in.at[e], ad_ss.at[e], ad_rs.at[e], {"tensor": pt[e]}).wait()
    red = adx[t]
    for e in range(1, nt):
        red = red + ad_in[e]
    scale_row = lax.rsqrt(red[16:17, :] / (LW * nt) + EPS)
    ad16 = red[0:16, :].astype(BF)
    factor = 2.0 / math.sqrt(L * nt * nc * nf)
    ag_own[...] = (factor * scale_row * cu).astype(BF)
    ags = [copy(ag_own, ag_all.at[t], ag_ss.at[e], ag_rs.at[e], {"tensor": pt[e]}) for e in range(1, nt)]
    gb_own[...] = dot((factor * scale_row * ad16.astype(F32)).astype(BF), cot_ref[...]).astype(BF)
    part = gb_own.shape[1] // nt
    own_part = pl.ds(pl.multiple_of(t * part, 128), part)
    gbs = [
        copy(
            gb_own.at[:, pl.ds(pl.multiple_of(pt[e] * part, 128), part)],
            gb_in.at[e], ga_ss.at[e], ga_rs.at[e], {"tensor": pt[e]},
        )
        for e in range(1, nt)
    ]
    scale_col = dot(jnp.broadcast_to(scale_row, (8, L)), jnp.full((8, 128), 0.125, F32), 0, 0, HI)[:, 0:1]
    for s in range(1, steps):
        for ch in range(nch):
            if s > 1 or ch > 0:
                if s == 1:
                    w_arrive(s, ch)
    for s in range(2, nf - 1):
        if s > 2:
            for ch in range(nch):
                w_arrive(s - 1, ch)
        for ch in range(nch):
            project(1 + (s - 1) * nch + ch)
    for cp in ags + gbs:
        cp.wait()
    ag_all[t] = ag_own[...]
    grad = jnp.zeros((16, LW), F32)
    for s in range(nt):
        grad = grad + dot(ag_all[s], g_s[s * L : (s + 1) * L, :])
    comb[:, 0:LW] = grad
    acc = gb_own[:, own_part].astype(F32)
    for e in range(1, nt):
        acc = acc + gb_in[e].astype(F32)
    comb[:, LW : LW + part] = acc
    lanes = (LW + part) // 128
    per = -(-lanes // nc)

    def seg(i):
        return pl.ds(pl.multiple_of(jnp.minimum(i * per, lanes - per) * 128, 128), per * 128)

    ccs = [
        copy(comb.at[:, seg(lax.rem(c + k, nc))], comb_c.at[k], cc_ss.at[k], cc_rs.at[k], {"context": lax.rem(c + k, nc)})
        for k in range(1, nc)
    ]
    if steps > 2:
        w_arrive(steps - 1, 0)
    for cp in ccs:
        cp.wait()
    acc = comb[:, seg(c)]
    for k in range(1, nc):
        acc = acc + comb_c[k]
    comb2[...] = acc.astype(BF)
    cfs = [copy(comb2, comb_f.at[f], cf_ss.at[k], cf_rs.at[k], {"fsdp": lax.rem(f + k, nf)}) for k in range(1, nf)]
    comb_f[f] = comb2[...]
    last = nf - 1
    if last > 1:
        project(1 + (last - 1) * nch)
        for ch in range(1, nch):
            if steps > 2:
                w_arrive(steps - 1, ch)
            project(1 + (last - 1) * nch + ch)

    def finish(u):
        slot, ch, off, wide = units[u]
        for e in range(1, nt):
            scattered(u, pt[e], spans[u]).wait()
        acc = rs_send[own_rows, spans[u]].astype(F32)
        for e in range(1, nt):
            acc = acc + rs_recv[pt[e], :, spans[u]].astype(F32)
        acc = acc + 2.0 * dot(ad16, up_ref[:, spans[u]], 0, 0)
        mixed_ref[:, spans[u]] = (scale_col * acc).astype(BF)

    finish(0)
    for ch in range(nch):
        finish(1 + ch)
    for cp in cfs:
        cp.wait()
    acc = comb_f[0].astype(F32)
    for k in range(1, nf):
        acc = acc + comb_f[k].astype(F32)
    seg_own[...] = acc
    sgs = [copy(seg_own, seg_in.at[c], sg_ss.at[k], sg_rs.at[k], {"context": lax.rem(c + k, nc)}) for k in range(1, nc)]
    seg_in[c] = acc
    for cp in sgs:
        cp.wait()
    for i in range(nc):
        full[:, seg(i)] = seg_in[i]
    ga_ref[...] = full[:, 0:LW]
    fin[t] = full[:, LW : LW + part]
    fins = [copy(fin.at[t], fin.at[t], fin_ss.at[e], fin_rs.at[e], {"tensor": pt[e]}) for e in range(1, nt)]
    for u in range(1 + nch, len(units)):
        finish(u)
    for cp in fins:
        cp.wait()
    for s in range(nt):
        gb_ref[:, s * part : (s + 1) * part] = fin[s]
    for cp in zs:
        cp.wait_send()
    for ch in range(nch):
        for s in range(steps):
            for dr in range(2):
                @pl.when(sends(dr, s))
                def _(dr=dr, s=s, ch=ch):
                    w_copy(dr, s, ch, f - s if dr == 0 else f + s).wait_send()

                @pl.when(gets(dr, s))
                def _(dr=dr, s=s, ch=ch):
                    for k in range(1, nc):
                        w_share(dr, s, ch, came(dr, s), k).wait_send()


def shards(x, bc, z, dt, taps, bias, step_bias, rate, skip, gain, w, down, up, cot):
    nt, nf, nc = lax.axis_size("tensor"), lax.axis_size("fsdp"), lax.axis_size("context")
    L, full = x.shape[1], x.shape[2]
    LW, hl, W, M = gain.shape[0], step_bias.shape[0], w.shape[1], cot.shape[2]
    BC = bc.shape[2]
    N = BC // 2
    HR = -(-hl // 8) * 8
    T = nt * L
    part = M // nt
    dt = dt[0].T
    down = down.T
    nch = len(column_chunks(W))
    units = 1 + (nf - 1) * nch
    lanes = (LW + part) // 128
    SW = -(-lanes // nc) * 128
    vm = pl.BlockSpec(memory_space=pltpu.VMEM)
    hbm = pl.BlockSpec(memory_space=pl.ANY)
    V = pltpu.VMEM
    D = pltpu.SemaphoreType.DMA
    scratch = [
        V((L, full), BF), V((L, BC), BF), V(dt.shape, BF), V(taps.shape, F32), V((1, full + BC), F32), V((1, LW), F32),
        V(down.shape, BF), V(up.shape, BF), V((L, M), BF),
        V((HALO, full), BF), V((HALO, BC), BF), V((nt - 1, L, LW), BF), V((T, LW), BF), V((T, LW), BF),
        V((T, BC), BF), V((nt,) + dt.shape, BF), V((nf, LW, W), BF), V((T, 128), F32), V((T, 128), F32),
        V((nt, HR, L), F32), V((nt, HR, L), F32),
        V((nt, N + 8, LW), F32), V((N + 8, LW), F32), V((nc, N + 8, LW), F32), V((N, LW), F32),
        V((128, LW), F32), V((T, LW), F32), V((T, LW), BF), V((nt, 24, L), F32), V((nt, 24, L), F32),
        V((16, L), BF), V((nt, 16, L), BF), V((16, M), BF), V((nt, 16, part), BF),
        V((16, LW + part), F32), V((nc, 16, SW), F32), V((16, SW), BF), V((nf, 16, SW), BF),
        V((16, SW), F32), V((nc, 16, SW), F32), V((16, LW + part), F32),
        V((nt, 16, part), F32), V((T, M), BF), V((nt, L, M), BF),
        D((9,)), D((2,)), D((2,)), D((nt,)), D((nt,)), D((nt,)), D((nt,)), D((nt,)), D((nt,)), D((nt,)), D((nt,)),
        D((2, nf - 1, nch)), D((2, nf - 1, nch)), D((2, nf - 1, nch, nc)), D((2, nf - 1, nch, nc)), D((nc,)), D((nc,)),
        D((nt,)), D((nt,)), D((nt,)), D((nt,)), D((nt,)), D((nt,)), D((nc,)), D((nc,)), D((nf,)), D((nf,)),
        D((nc,)), D((nc,)), D((nt,)), D((nt,)), D((units, nt)), D((units, nt)), D((2,)),
    ]
    mixed, ga, gb = pl.pallas_call(
        functools.partial(kernel, nt, nf, nc, hl),
        out_shape=(
            jax.ShapeDtypeStruct((L, M), BF),
            jax.ShapeDtypeStruct((16, LW), F32),
            jax.ShapeDtypeStruct((16, M), F32),
        ),
        in_specs=[hbm, hbm, hbm, hbm, hbm, hbm, vm, vm, vm, hbm, hbm, hbm, hbm, hbm],
        out_specs=(vm, vm, vm),
        scratch_shapes=scratch,
        compiler_params=pltpu.CompilerParams(
            collective_id=0, has_side_effects=True, vmem_limit_bytes=62 * 1024 * 1024
        ),
    )(x[0], bc[0], z[0], dt, taps, bias[None], step_bias[None], rate[None], skip[None], gain[None], w, down, up, cot[0])
    return mixed[None], ga.T, gb


def solution(mesh):
    tokens = P("fsdp", ("context", "tensor"), None)
    placed = (
        tokens, tokens, tokens, tokens, P(), P(), P("tensor"), P("tensor"), P("tensor"), P("tensor"),
        P("tensor", "fsdp"), P("tensor", None), P(), tokens,
    )
    return jax.shard_map(
        shards, mesh=mesh, in_specs=placed, out_specs=(tokens, P("tensor", None), P()), check_vma=False
    )
```

```python
import functools
import math

import jax
import jax.numpy as jnp
from jax import lax
from jax.experimental import pallas as pl
from jax.experimental.pallas import tpu as pltpu
from jax.sharding import PartitionSpec as P

EPS = 1e-05
MESH = pl.DeviceIdType.MESH
HI = lax.Precision.HIGHEST
BF = jnp.bfloat16
F32 = jnp.float32
HALO = 8


def dot(a, b, ca=1, cb=0, precision=None):
    return lax.dot_general(
        a, b, (((ca,), (cb,)), ((), ())), preferred_element_type=F32, precision=precision
    )


def iota(shape, dim):
    return lax.broadcasted_iota(jnp.int32, shape, dim)


def pick(values, i):
    out = jnp.int32(values[0])
    for k in range(1, len(values)):
        out = jnp.where(i == k, jnp.int32(values[k]), out)
    return out


def column_chunks(width):
    lanes = width // 128
    first = -(-lanes // 2)
    return [(0, first * 128), (first * 128, (lanes - first) * 128)] if lanes > 1 else [(0, width)]


def kernel(
    nt, nf, nc, hl,
    x_hbm, bc_hbm, z_ref, dt_hbm, taps_hbm, bias_hbm, sb_ref, dr_ref, sk_ref, gain_hbm, w_ref, down_hbm, up_hbm, cot_hbm,
    mixed_ref, ga_ref, gb_ref,
    x_ref, bc_ref, dt_ref, taps_ref, bias_ref, gain_ref, down_ref, up_ref, cot_ref,
    halo_x, halo_bc, x_send, x_all, z_all, bc_all, dt_all, wbuf, a_s, step_s, at_s, stept_s,
    stl, loc_s, skip_s, msg, st_in, inc_s, e_s, y_s, g_s, adx, ad_in, ag_own, ag_all, gb_own, gb_in,
    comb, comb_c, comb2, comb_f, seg_own, seg_in, full, fin, rs_send, rs_recv,
    ld, h_ss, h_rs, dt_ss, dt_rs, bc_ss, bc_rs, x_ss, x_rs, z_ss, z_rs, w_ss, w_rs, wf_ss, wf_rs, st_ss, st_rs,
    ad_ss, ad_rs, ag_ss, ag_rs, ga_ss, ga_rs, cc_ss, cc_rs, cf_ss, cf_rs, sg_ss, sg_rs, fin_ss, fin_rs, r_ss, r_rs, loc,
):
    t = lax.axis_index("tensor")
    f = lax.axis_index("fsdp")
    c = lax.axis_index("context")
    L = x_ref.shape[0]
    LW = x_all.shape[1]
    W = w_ref.shape[1]
    N = bc_ref.shape[1] // 2
    R = w_ref.shape[0] // nc
    HS = LW // hl
    idx = c * nt + t
    total = nc * nt
    bits = [1 << i for i in range(nt.bit_length() - 1)]
    chunks = column_chunks(W)
    steps = nf - 1

    def peer(e):
        out = 0
        for bit in bits:
            out = out + bit * lax.rem(lax.div(t, bit) + lax.div(e, bit), 2)
        return out

    def peers():
        return [peer(jnp.int32(e)) for e in range(nt)]

    pt = peers()

    def place(i):
        return {"context": i // nt, "tensor": lax.rem(i, nt)}

    def remote(src, dst, ss, rs, dev):
        return pltpu.make_async_remote_copy(
            src_ref=src, dst_ref=dst, send_sem=ss, recv_sem=rs, device_id=dev, device_id_type=MESH
        )

    def copy(src, dst, ss, rs, dev):
        cp = remote(src, dst, ss, rs, dev)
        cp.start()
        return cp

    loads = []
    for i, (src, dst) in enumerate((
        (x_hbm, x_ref), (bc_hbm, bc_ref), (dt_hbm, dt_ref), (taps_hbm, taps_ref), (bias_hbm, bias_ref),
        (gain_hbm, gain_ref), (down_hbm, down_ref), (up_hbm, up_ref), (cot_hbm, cot_ref),
    )):
        cp = pltpu.make_async_copy(src, dst, ld.at[i])
        cp.start()
        loads.append(cp)
    own_w = pltpu.make_async_copy(w_ref, wbuf.at[f], loc.at[0])
    own_w.start()
    own_rows = pl.ds(pl.multiple_of(t * L, L), L)
    own_cols = pl.ds(pl.multiple_of(t * LW, 128), LW)
    own_z = pltpu.make_async_copy(z_ref.at[:, own_cols], z_all.at[own_rows, :], loc.at[1])
    own_z.start()

    nxt, prv = lax.rem(idx + 1, total), lax.rem(idx + total - 1, total)
    bar = pltpu.get_barrier_semaphore()
    greet = [{"tensor": pt[e]} for e in range(1, nt)]
    greet += [{"fsdp": lax.rem(f + d, nf)} for d in range(1, nf)]
    greet += [{"context": lax.rem(c + k, nc)} for k in range(1, nc)]
    greet += [place(nxt), place(prv)]
    for dev in greet:
        pl.semaphore_signal(bar, inc=1, device_id=dev, device_id_type=MESH)
    for cp in loads:
        cp.wait()
    dt_all[t] = dt_ref[...]
    pl.semaphore_wait(bar, len(greet))

    h1 = copy(x_ref.at[L - HALO : L, :], halo_x, h_ss.at[0], h_rs.at[0], place(nxt))
    h2 = copy(bc_ref.at[L - HALO : L, :], halo_bc, h_ss.at[1], h_rs.at[1], place(nxt))
    dts = [copy(dt_ref, dt_all.at[t], dt_ss.at[e], dt_rs.at[e], {"tensor": pt[e]}) for e in range(1, nt)]
    share = pl.ds(pl.multiple_of(c * R, 16), R)

    def w_copy(dr, s, ch, q):
        cols = pl.ds(chunks[ch][0], chunks[ch][1])
        src = w_ref.at[share, cols] if s == 0 else wbuf.at[q, share, cols]
        to = f + 1 if dr == 0 else f - 1
        return remote(src, wbuf.at[q, share, cols], w_ss.at[dr, s, ch], w_rs.at[dr, s, ch], {"fsdp": to})

    def w_share(dr, s, ch, q, k):
        region = wbuf.at[q, share, pl.ds(chunks[ch][0], chunks[ch][1])]
        return remote(region, region, wf_ss.at[dr, s, ch, k], wf_rs.at[dr, s, ch, k], {"context": lax.rem(c + k, nc)})

    def has_next(dr):
        return f + 1 < nf if dr == 0 else f >= 1

    def sends(dr, s):
        return (f - s >= 0) & (f + 1 < nf) if dr == 0 else (f + s < nf) & (f >= 1)

    def gets(dr, s):
        return f - 1 - s >= 0 if dr == 0 else f + 1 + s < nf

    def came(dr, s):
        return f - 1 - s if dr == 0 else f + 1 + s

    for ch in range(len(chunks)):
        for dr in range(2):
            @pl.when(sends(dr, 0))
            def _(dr=dr, ch=ch):
                w_copy(dr, 0, ch, f).start()

    def w_arrive(s, ch):
        for dr in range(2):
            @pl.when(gets(dr, s))
            def _(dr=dr):
                q = came(dr, s)
                w_copy(dr, s, ch, q).wait_recv()
                if s + 1 < steps:
                    @pl.when(has_next(dr))
                    def _():
                        w_copy(dr, s + 1, ch, q).start()
                for k in range(1, nc):
                    w_share(dr, s, ch, q, k).start()

    table = [sorted(range(nf), key=lambda q, g=g: (abs(q - g), q)) for g in range(nf)]
    order = [pick([table[g][i] for g in range(nf)], f) for i in range(nf)]
    way = [pick([int(table[g][i] > g) for g in range(nf)], f) for i in range(nf)]
    dist = [pick([max(abs(table[g][i] - g) - 1, 0) for g in range(nf)], f) for i in range(nf)]

    def w_ready(slot, ch):
        region = wbuf.at[order[slot], share, pl.ds(chunks[ch][0], chunks[ch][1])]
        for k in range(1, nc):
            remote(
                region, region, wf_ss.at[way[slot], dist[slot], ch, k], wf_rs.at[way[slot], dist[slot], ch, k],
                {"context": lax.rem(c + k, nc)},
            ).wait_recv()

    def send_gate(e):
        cols = pl.ds(pl.multiple_of(pt[e] * LW, 128), LW)
        return copy(z_ref.at[:, cols], z_all.at[own_rows, :], z_ss.at[e], z_rs.at[e], {"tensor": pt[e]})

    early = nt - 1 if nt > 2 else nt
    zs = [send_gate(e) for e in range(1, early)]
    h1.wait()
    h2.wait()
    live = (idx > 0).astype(F32)

    def conv(src, halo, col, tap_col):
        lanes = pl.ds(col, 128)
        wide = pl.ds(tap_col, 128)
        ext = jnp.concatenate([halo[HALO - 8 : HALO, lanes].astype(F32) * live, src[:, lanes].astype(F32)], axis=0)
        acc = bias_ref[wide][None, :] + taps_ref[0:1, wide] * ext[5 : 5 + L]
        for k in range(1, 4):
            acc = acc + taps_ref[k : k + 1, wide] * ext[5 + k : 5 + k + L]
        return (acc / (1.0 + jnp.exp(-acc))).astype(BF)

    wide0 = x_ref.shape[1]
    for j in range(2 * N // 128):
        bc_all[own_rows, j * 128 : (j + 1) * 128] = conv(bc_ref, halo_bc, j * 128, wide0 + j * 128)
    bcs = [
        copy(bc_all.at[own_rows, :], bc_all.at[own_rows, :], bc_ss.at[e], bc_rs.at[e], {"tensor": pt[e]})
        for e in range(1, nt)
    ]
    xs = []

    def conv_group(e, store):
        base = pt[e] * LW

        def lap(j, carry):
            col = pl.multiple_of(base + j * 128, 128)
            store(pl.ds(pl.multiple_of(j * 128, 128), 128), conv(x_ref, halo_x, col, col))
            return carry

        lax.fori_loop(0, LW // 128, lap, 0)

    for e in range(1, nt):
        def put(lanes, val, e=e):
            x_send[e - 1, :, lanes] = val

        conv_group(e, put)
        xs.append(copy(x_send.at[e - 1], x_all.at[own_rows, :], x_ss.at[e], x_rs.at[e], {"tensor": pt[e]}))
    def put_own(lanes, val):
        x_all[own_rows, lanes] = val

    conv_group(0, put_own)
    e_s[...] = (iota((128, LW), 1) // HS == iota((128, LW), 0)).astype(F32)
    spread16 = e_s[...].astype(BF)

    def spread(rows):
        return dot(jnp.broadcast_to(rows, (8, 128)), e_s[...], precision=HI)

    for cp in dts:
        cp.wait()
    HR = at_s.shape[1]
    HA = dt_ref.shape[0]
    sel = ((iota((HA, 128), 0) == iota((HA, 128), 1) + t * hl) & (iota((HA, 128), 1) < hl)).astype(BF)
    sel_t = ((iota((HR, HA), 1) == iota((HR, HA), 0) + t * hl) & (iota((HR, HA), 0) < hl)).astype(BF)
    eye = (iota((HR, 128), 0) == iota((HR, 128), 1)).astype(F32)
    place_head = (iota((hl, 128), 0) == iota((hl, 128), 1)).astype(F32)
    hp = [
        dot(jnp.broadcast_to(v[...], (8, hl)), place_head, precision=HI)[0:1, :] for v in (sb_ref, dr_ref, sk_ref)
    ]
    hp_t = [dot(eye, jnp.broadcast_to(v, (8, 128)), 1, 1, HI)[:, 0:1] for v in hp[0:2]]
    tri = (iota((L, L), 0) >= iota((L, L), 1)).astype(F32)

    def softplus(v):
        return jnp.maximum(v, 0.0) + jnp.log1p(jnp.exp(-jnp.abs(v)))

    for b in range(nt):
        rows = slice(b * L, (b + 1) * L)
        raw = dt_all[b]
        step = softplus(dot(raw, sel, 0, 0) + hp[0])
        step_s[rows, :] = step
        a_s[rows, :] = dot(tri, -step * jnp.exp(hp[1]), precision=HI)
        step_t = softplus(dot(sel_t, raw) + hp_t[0])
        stept_s[b] = step_t
        at_s[b] = dot(-step_t * jnp.exp(hp_t[1]), tri, 1, 1, HI)
    before = jnp.zeros((1, 128), F32)
    for b in range(nt):
        last = a_s[(b + 1) * L - 1 : (b + 1) * L, :]
        stl[b, N : N + 8, :] = spread(jnp.exp(before))
        loc_s[b, N : N + 8, :] = spread(jnp.exp(last))
        before = before + last
    msg[N : N + 8, :] = spread(before)
    skip_s[...] = spread(hp[2])
    cu = dot(up_ref[...], cot_ref[...], 1, 1)
    left = iota((L, 2 * HS), 1) < HS

    def spans_of(e):
        b = pt[e]
        rows = pl.ds(pl.multiple_of(b * L, L), L)
        if e > 0:
            bcs[e - 1].wait_recv()
            xs[e - 1].wait_recv()
        a = a_s[rows, :]
        weight = (jnp.exp(a[L - 1 : L, :] - a) * step_s[rows, :]).astype(BF)
        xw = (x_all[rows, :].astype(F32) * dot(weight, spread16)).astype(BF)
        loc_s[b, 0:N, :] = dot(bc_all[rows, 0:N], xw, 0, 0)
        gram = dot(bc_all[rows, N : 2 * N], bc_all[rows, 0:N], 1, 1)
        gram = jnp.where(iota((L, L), 0) >= iota((L, L), 1), gram, 0.0)
        at = at_s[b]
        stt = stept_s[b]
        for pair in range(hl // 2):
            lanes = slice(pair * 2 * HS, (pair + 1) * 2 * HS)
            xp = x_all[rows, lanes]
            out = []
            for h in (2 * pair, 2 * pair + 1):
                gap = jnp.minimum(a[:, h : h + 1] - at[h : h + 1, :], 0.0)
                m = (jnp.exp(gap) * gram * stt[h : h + 1, :]).astype(BF)
                out.append(dot(m, xp))
            y_s[rows, lanes] = jnp.where(left, out[0], out[1])

    for e in range(nt):

        spans_of(e)
        if e == 0:
            w_arrive(0, 0)
        if e == min(1, nt - 2):
            for ch in range(1, len(chunks)):
                w_arrive(0, ch)
        if e == nt - 2:
            for cp in xs:
                cp.wait_send()
            zs += [send_gate(i) for i in range(early, nt)]
    for cp in bcs:
        cp.wait_send()

    state = jnp.zeros((N, LW), F32)
    for b in range(nt):
        stl[b, 0:N, :] = state
        state = loc_s[b, N : N + 1, :] * state + loc_s[b, 0:N, :]
    msg[0:N, :] = state
    sts = [
        copy(msg, st_in.at[c], st_ss.at[k], st_rs.at[k], {"context": lax.rem(c + k, nc)})
        for k in range(1, nc)
    ]

    if steps > 1:
        w_arrive(1, 0)
    for cp in sts:
        cp.wait()
    inc_s[...] = jnp.zeros_like(inc_s)

    def chain(k, carry):
        inc_s[...] = jnp.exp(st_in[k, N : N + 1, :]) * inc_s[...] + st_in[k, 0:N, :]
        return carry

    lax.fori_loop(0, c, chain, 0)
    own_w.wait()
    skip = skip_s[0:1, :]
    ones = jnp.ones((8, LW), BF)

    def scatter(unit, b, cols):
        return remote(
            rs_send.at[pl.ds(pl.multiple_of(b * L, L), L), cols], rs_recv.at[t, :, cols],
            r_ss.at[unit, b], r_rs.at[unit, t], {"tensor": b},
        )

    def scattered(unit, b, cols):
        return remote(
            rs_send.at[pl.ds(pl.multiple_of(b * L, L), L), cols], rs_recv.at[b, :, cols],
            r_ss.at[unit, b], r_rs.at[unit, b], {"tensor": b},
        )

    units = [(0, None, 0, W)] + [(s, ch) + chunks[ch] for s in range(1, nf) for ch in range(len(chunks))]
    spans = [pl.ds(pl.multiple_of(order[s] * W + off, 128), wide) for s, _, off, wide in units]

    held = max(nt - 1, 1)

    def gate(e, carry):
        b = peer(e)
        rows = pl.ds(pl.multiple_of(b * L, L), L)

        @pl.when(e == 0)
        def _():
            own_z.wait()

        @pl.when(e > 0)
        def _():
            remote(
                z_ref.at[:, own_cols], z_all.at[rows, :], z_ss.at[e], z_rs.at[e], {"tensor": b}
            ).wait_recv()

        start = (stl[b, 0:N, :] + stl[b, N : N + 1, :] * inc_s[...]).astype(BF)
        reach = dot(jnp.exp(a_s[rows, :]).astype(BF), spread16)
        y = y_s[rows, :] + reach * dot(bc_all[rows, N : 2 * N], start)
        y = y + skip * x_all[rows, :].astype(F32)
        z = z_all[rows, :].astype(F32)
        g = y * (z / (1.0 + jnp.exp(-z)))
        out = (g * gain_ref[...][None, :]).astype(BF)
        g_s[rows, :] = out
        adx[b, 0:16, :] = dot(down_ref[...], out, 1, 1)
        adx[b, 16:24, :] = dot(ones, (g * g).astype(BF), 1, 1)

        @pl.when(e > 0)
        def _():
            remote(adx.at[b], ad_in.at[e], ad_ss.at[e], ad_rs.at[e], {"tensor": b}).start()

        rs_send[rows, spans[0]] = dot(out, wbuf[f]).astype(BF)

        @pl.when((e > 0) & (e < held))
        def _():
            scatter(0, b, spans[0]).start()

        return carry

    lax.fori_loop(0, nt, gate, 0)

    half = (nt * L) // 2

    def project(u, send=True):
        slot, ch, off, wide = units[u]
        w_ready(slot, ch)

        def lap(i, carry):
            rows = pl.ds(pl.multiple_of(i * half, half), half)
            rs_send[rows, spans[u]] = dot(g_s[rows, :], wbuf[order[slot], :, off : off + wide]).astype(BF)
            if send:
                for j in range(half // L):
                    b = i * (half // L) + j

                    @pl.when(b != t)
                    def _():
                        scatter(u, b, spans[u]).start()

            return carry

        lax.fori_loop(0, 2, lap, 0)

    nch = len(chunks)
    if steps > 1:
        for ch in range(1, nch):
            w_arrive(1, ch)
    for ch in range(nch):
        project(1 + ch, send=False)
    for e in range(1, nt):
        remote(adx.at[pt[e]], ad_in.at[e], ad_ss.at[e], ad_rs.at[e], {"tensor": pt[e]}).wait()
    red = adx[t]
    for e in range(1, nt):
        red = red + ad_in[e]
    scale_row = lax.rsqrt(red[16:17, :] / (LW * nt) + EPS)
    ad16 = red[0:16, :].astype(BF)
    factor = 2.0 / math.sqrt(L * nt * nc * nf)
    ag_own[...] = (factor * scale_row * cu).astype(BF)
    ags = [copy(ag_own, ag_all.at[t], ag_ss.at[e], ag_rs.at[e], {"tensor": pt[e]}) for e in range(1, nt)]
    gb_own[...] = dot((factor * scale_row * ad16.astype(F32)).astype(BF), cot_ref[...]).astype(BF)
    part = gb_own.shape[1] // nt
    own_part = pl.ds(pl.multiple_of(t * part, 128), part)
    gbs = [
        copy(
            gb_own.at[:, pl.ds(pl.multiple_of(pt[e] * part, 128), part)],
            gb_in.at[e], ga_ss.at[e], ga_rs.at[e], {"tensor": pt[e]},
        )
        for e in range(1, nt)
    ]
    for e in range(held, nt):
        scatter(0, pt[e], spans[0]).start()
    for ch in range(nch):
        for e in range(1, nt):
            scatter(1 + ch, pt[e], spans[1 + ch]).start()
    scale_col = dot(jnp.broadcast_to(scale_row, (8, L)), jnp.full((8, 128), 0.125, F32), 0, 0, HI)[:, 0:1]
    for s in range(2, nf - 1):
        if s > 2:
            for ch in range(nch):
                w_arrive(s - 1, ch)
        for ch in range(nch):
            project(1 + (s - 1) * nch + ch)
    for cp in ags + gbs:
        cp.wait()
    ag_all[t] = ag_own[...]
    grad = jnp.zeros((16, LW), F32)
    for s in range(nt):
        grad = grad + dot(ag_all[s], g_s[s * L : (s + 1) * L, :])
    comb[:, 0:LW] = grad
    acc = gb_own[:, own_part].astype(F32)
    for e in range(1, nt):
        acc = acc + gb_in[e].astype(F32)
    comb[:, LW : LW + part] = acc
    lanes = (LW + part) // 128
    per = -(-lanes // nc)

    def seg(i):
        return pl.ds(pl.multiple_of(jnp.minimum(i * per, lanes - per) * 128, 128), per * 128)

    ccs = [
        copy(comb.at[:, seg(lax.rem(c + k, nc))], comb_c.at[k], cc_ss.at[k], cc_rs.at[k], {"context": lax.rem(c + k, nc)})
        for k in range(1, nc)
    ]
    if steps > 2:
        w_arrive(steps - 1, 0)
    for cp in ccs:
        cp.wait()
    acc = comb[:, seg(c)]
    for k in range(1, nc):
        acc = acc + comb_c[k]
    comb2[...] = acc.astype(BF)
    cfs = [copy(comb2, comb_f.at[f], cf_ss.at[k], cf_rs.at[k], {"fsdp": lax.rem(f + k, nf)}) for k in range(1, nf)]
    comb_f[f] = comb2[...]
    last = nf - 1
    if last > 1:
        project(1 + (last - 1) * nch)
        for ch in range(1, nch):
            if steps > 2:
                w_arrive(steps - 1, ch)
            project(1 + (last - 1) * nch + ch)

    def finish(u):
        slot, ch, off, wide = units[u]
        for e in range(1, nt):
            scattered(u, pt[e], spans[u]).wait()
        acc = rs_send[own_rows, spans[u]].astype(F32)
        for e in range(1, nt):
            acc = acc + rs_recv[pt[e], :, spans[u]].astype(F32)
        acc = acc + 2.0 * dot(ad16, up_ref[:, spans[u]], 0, 0)
        mixed_ref[:, spans[u]] = (scale_col * acc).astype(BF)

    finish(0)
    for ch in range(nch):
        finish(1 + ch)
    for cp in cfs:
        cp.wait()
    acc = comb_f[0].astype(F32)
    for k in range(1, nf):
        acc = acc + comb_f[k].astype(F32)
    seg_own[...] = acc
    sgs = [copy(seg_own, seg_in.at[c], sg_ss.at[k], sg_rs.at[k], {"context": lax.rem(c + k, nc)}) for k in range(1, nc)]
    seg_in[c] = acc
    for cp in sgs:
        cp.wait()
    for i in range(nc):
        full[:, seg(i)] = seg_in[i]
    ga_ref[...] = full[:, 0:LW]
    fin[t] = full[:, LW : LW + part]
    fins = [copy(fin.at[t], fin.at[t], fin_ss.at[e], fin_rs.at[e], {"tensor": pt[e]}) for e in range(1, nt)]
    for u in range(1 + nch, len(units)):
        finish(u)
    for cp in fins:
        cp.wait()
    for s in range(nt):
        gb_ref[:, s * part : (s + 1) * part] = fin[s]
    for cp in zs:
        cp.wait_send()
    for ch in range(nch):
        for s in range(steps):
            for dr in range(2):
                @pl.when(sends(dr, s))
                def _(dr=dr, s=s, ch=ch):
                    w_copy(dr, s, ch, f - s if dr == 0 else f + s).wait_send()

                @pl.when(gets(dr, s))
                def _(dr=dr, s=s, ch=ch):
                    for k in range(1, nc):
                        w_share(dr, s, ch, came(dr, s), k).wait_send()


def write_out(mixed, ga, gb, mixed_out, ga_out, gb_out, sem):
    copies = [
        pltpu.make_async_copy(src, dst, sem.at[i])
        for i, (src, dst) in enumerate(((mixed, mixed_out), (ga, ga_out), (gb, gb_out)))
    ]
    for cp in copies:
        cp.start()
    for cp in copies:
        cp.wait()


def shards(x, bc, z, dt, taps, bias, step_bias, rate, skip, gain, w, down, up, cot):
    nt, nf, nc = lax.axis_size("tensor"), lax.axis_size("fsdp"), lax.axis_size("context")
    L, full = x.shape[1], x.shape[2]
    LW, hl, W, M = gain.shape[0], step_bias.shape[0], w.shape[1], cot.shape[2]
    BC = bc.shape[2]
    N = BC // 2
    HR = -(-hl // 8) * 8
    T = nt * L
    part = M // nt
    dt = dt[0].T
    down = down.T
    nch = len(column_chunks(W))
    units = 1 + (nf - 1) * nch
    lanes = (LW + part) // 128
    SW = -(-lanes // nc) * 128
    vm = pl.BlockSpec(memory_space=pltpu.VMEM)
    hbm = pl.BlockSpec(memory_space=pl.ANY)
    V = pltpu.VMEM
    D = pltpu.SemaphoreType.DMA
    scratch = [
        V((L, full), BF), V((L, BC), BF), V(dt.shape, BF), V(taps.shape, F32), V((full + BC,), F32), V((LW,), F32),
        V(down.shape, BF), V(up.shape, BF), V((L, M), BF),
        V((HALO, full), BF), V((HALO, BC), BF), V((nt - 1, L, LW), BF), V((T, LW), BF), V((T, LW), BF),
        V((T, BC), BF), V((nt,) + dt.shape, BF), V((nf, LW, W), BF), V((T, 128), F32), V((T, 128), F32),
        V((nt, HR, L), F32), V((nt, HR, L), F32),
        V((nt, N + 8, LW), F32), V((nt, N + 8, LW), F32), V((8, LW), F32), V((N + 8, LW), F32), V((nc, N + 8, LW), F32), V((N, LW), F32),
        V((128, LW), F32), V((T, LW), F32), V((T, LW), BF), V((nt, 24, L), F32), V((nt, 24, L), F32),
        V((16, L), BF), V((nt, 16, L), BF), V((16, M), BF), V((nt, 16, part), BF),
        V((16, LW + part), F32), V((nc, 16, SW), F32), V((16, SW), BF), V((nf, 16, SW), BF),
        V((16, SW), F32), V((nc, 16, SW), F32), V((16, LW + part), F32),
        V((nt, 16, part), F32), V((T, M), BF), V((nt, L, M), BF),
        D((9,)), D((2,)), D((2,)), D((nt,)), D((nt,)), D((nt,)), D((nt,)), D((nt,)), D((nt,)), D((nt,)), D((nt,)),
        D((2, nf - 1, nch)), D((2, nf - 1, nch)), D((2, nf - 1, nch, nc)), D((2, nf - 1, nch, nc)), D((nc,)), D((nc,)),
        D((nt,)), D((nt,)), D((nt,)), D((nt,)), D((nt,)), D((nt,)), D((nc,)), D((nc,)), D((nf,)), D((nf,)),
        D((nc,)), D((nc,)), D((nt,)), D((nt,)), D((units, nt)), D((units, nt)), D((2,)),
    ]
    mixed, ga, gb = pl.pallas_call(
        functools.partial(kernel, nt, nf, nc, hl),
        out_shape=(V((L, M), BF), V((16, LW), F32), V((16, M), F32)),
        in_specs=[hbm, hbm, hbm, hbm, hbm, hbm, vm, vm, vm, hbm, hbm, hbm, hbm, hbm],
        out_specs=(vm, vm, vm),
        scratch_shapes=scratch,
        compiler_params=pltpu.CompilerParams(
            collective_id=0, has_side_effects=True, vmem_limit_bytes=62 * 1024 * 1024
        ),
    )(x[0], bc[0], z[0], dt, taps, bias, step_bias[None], rate[None], skip[None], gain, w, down, up, cot[0])
    mixed, ga, gb = (pltpu.with_memory_space_constraint(v, pltpu.VMEM) for v in (mixed, ga, gb))
    mixed, ga, gb = pl.pallas_call(
        write_out,
        out_shape=(
            jax.ShapeDtypeStruct((L, M), BF),
            jax.ShapeDtypeStruct((16, LW), F32),
            jax.ShapeDtypeStruct((16, M), F32),
        ),
        in_specs=[vm, vm, vm],
        out_specs=(hbm, hbm, hbm),
        scratch_shapes=[D((3,))],
    )(mixed, ga, gb)
    return mixed[None], ga.T, gb


def solution(mesh):
    tokens = P("fsdp", ("context", "tensor"), None)
    placed = (
        tokens, tokens, tokens, tokens, P(), P(), P("tensor"), P("tensor"), P("tensor"), P("tensor"),
        P("tensor", "fsdp"), P("tensor", None), P(), tokens,
    )
    return jax.shard_map(
        shards, mesh=mesh, in_specs=placed, out_specs=(tokens, P("tensor", None), P()), check_vma=False
    )
```

```python
import functools
import math

import jax
import jax.numpy as jnp
from jax import lax
from jax.experimental import pallas as pl
from jax.experimental.pallas import tpu as pltpu
from jax.sharding import PartitionSpec as P

EPS = 1e-05
MESH = pl.DeviceIdType.MESH
HI = lax.Precision.HIGHEST
BF = jnp.bfloat16
F32 = jnp.float32
HALO = 8


def dot(a, b, ca=1, cb=0, precision=None):
    return lax.dot_general(
        a, b, (((ca,), (cb,)), ((), ())), preferred_element_type=F32, precision=precision
    )


def iota(shape, dim):
    return lax.broadcasted_iota(jnp.int32, shape, dim)


def pick(values, i):
    out = jnp.int32(values[0])
    for k in range(1, len(values)):
        out = jnp.where(i == k, jnp.int32(values[k]), out)
    return out


def grid_of(count):
    return (2, count // 2) if count % 2 == 0 else (1, count)


def column_chunks(width):
    lanes = width // 128
    first = -(-lanes // 2)
    return [(0, first * 128), (first * 128, (lanes - first) * 128)] if lanes > 1 else [(0, width)]


def kernel(
    nt, nf, nc, hl,
    x_hbm, bc_hbm, z_ref, dt_hbm, taps_hbm, bias_hbm, sb_ref, dr_ref, sk_ref, gain_hbm, w_ref, down_hbm, up_hbm, cot_hbm,
    mixed_ref, ga_ref, gb_ref,
    x_ref, bc_ref, dt_ref, taps_ref, bias_ref, gain_ref, down_ref, up_ref, cot_ref,
    halo_x, halo_bc, x_send, x_all, z_all, bc_all, dt_all, wbuf, a_s, step_s, at_s, stept_s,
    stl, loc_s, skip_s, msg, st_in, inc_s, e_s, y_s, g_s, adx, ad_in, ag_own, ag_all, gb_own, gb_in,
    comb, comb_c, comb2, comb_f, seg_own, seg_in, full, fin, rs_send, rs_xa, rs_yb, sum_a, in_a, sum_b, in_b,
    ld, h_ss, h_rs, dt_ss, dt_rs, bc_ss, bc_rs, x_ss, x_rs, z_ss, z_rs, w_ss, w_rs, wf_ss, wf_rs, st_ss, st_rs,
    ad_ss, ad_rs, ag_ss, ag_rs, ga_ss, ga_rs, cc_ss, cc_rs, cf_ss, cf_rs, sg_ss, sg_rs, fin_ss, fin_rs, rs_ss, rs_rs, loc,
):
    t = lax.axis_index("tensor")
    f = lax.axis_index("fsdp")
    c = lax.axis_index("context")
    L = x_ref.shape[0]
    LW = x_all.shape[1]
    W = w_ref.shape[1]
    N = bc_ref.shape[1] // 2
    R = w_ref.shape[0] // nc
    HS = LW // hl
    idx = c * nt + t
    total = nc * nt
    bits = [1 << i for i in range(nt.bit_length() - 1)]
    chunks = column_chunks(W)
    steps = nf - 1

    def peer(e):
        out = 0
        for bit in bits:
            out = out + bit * lax.rem(lax.div(t, bit) + lax.div(e, bit), 2)
        return out

    def peers():
        return [peer(jnp.int32(e)) for e in range(nt)]

    pt = peers()

    def place(i):
        return {"context": i // nt, "tensor": lax.rem(i, nt)}

    def remote(src, dst, ss, rs, dev):
        return pltpu.make_async_remote_copy(
            src_ref=src, dst_ref=dst, send_sem=ss, recv_sem=rs, device_id=dev, device_id_type=MESH
        )

    def sent(region, sem):
        remote(region, region, sem, sem, {"tensor": pt[nt - 1]}).wait_send()

    def landed(region, sem):
        remote(region, region, sem, sem, {"tensor": pt[nt - 1]}).wait_recv()

    def copy(src, dst, ss, rs, dev):
        cp = remote(src, dst, ss, rs, dev)
        cp.start()
        return cp

    loads = []
    for i, (src, dst) in enumerate((
        (x_hbm, x_ref), (bc_hbm, bc_ref), (dt_hbm, dt_ref), (taps_hbm, taps_ref), (bias_hbm, bias_ref),
        (gain_hbm, gain_ref), (down_hbm, down_ref), (up_hbm, up_ref), (cot_hbm, cot_ref),
    )):
        cp = pltpu.make_async_copy(src, dst, ld.at[i])
        cp.start()
        loads.append(cp)
    own_w = pltpu.make_async_copy(w_ref, wbuf.at[f], loc.at[0])
    own_w.start()
    own_rows = pl.ds(pl.multiple_of(t * L, L), L)
    own_cols = pl.ds(pl.multiple_of(t * LW, 128), LW)
    own_z = pltpu.make_async_copy(z_ref.at[:, own_cols], z_all.at[own_rows, :], loc.at[1])
    own_z.start()

    nxt, prv = lax.rem(idx + 1, total), lax.rem(idx + total - 1, total)
    bar = pltpu.get_barrier_semaphore()
    greet = [{"tensor": pt[e]} for e in range(1, nt)]
    greet += [{"fsdp": lax.rem(f + d, nf)} for d in range(1, nf)]
    greet += [{"context": lax.rem(c + k, nc)} for k in range(1, nc)]
    greet += [place(nxt), place(prv)]
    for dev in greet:
        pl.semaphore_signal(bar, inc=1, device_id=dev, device_id_type=MESH)
    for cp in loads:
        cp.wait()
    dt_all[t] = dt_ref[...]
    pl.semaphore_wait(bar, len(greet))

    h1 = copy(x_ref.at[L - HALO : L, :], halo_x, h_ss.at[0], h_rs.at[0], place(nxt))
    h2 = copy(bc_ref.at[L - HALO : L, :], halo_bc, h_ss.at[1], h_rs.at[1], place(nxt))
    for e in range(1, nt):
        copy(dt_ref, dt_all.at[t], dt_ss.at[0], dt_rs.at[0], {"tensor": pt[e]})
    share = pl.ds(pl.multiple_of(c * R, 16), R)

    def w_copy(dr, s, ch, q):
        cols = pl.ds(chunks[ch][0], chunks[ch][1])
        src = w_ref.at[share, cols] if s == 0 else wbuf.at[q, share, cols]
        to = f + 1 if dr == 0 else f - 1
        return remote(src, wbuf.at[q, share, cols], w_ss.at[dr, s], w_rs.at[dr, s, ch], {"fsdp": to})

    def w_share(dr, s, ch, q, k):
        region = wbuf.at[q, share, pl.ds(chunks[ch][0], chunks[ch][1])]
        return remote(region, region, wf_ss.at[dr, s], wf_rs.at[dr, s, ch], {"context": lax.rem(c + k, nc)})

    def has_next(dr):
        return f + 1 < nf if dr == 0 else f >= 1

    def sends(dr, s):
        return (f - s >= 0) & (f + 1 < nf) if dr == 0 else (f + s < nf) & (f >= 1)

    def gets(dr, s):
        return f - 1 - s >= 0 if dr == 0 else f + 1 + s < nf

    def came(dr, s):
        return f - 1 - s if dr == 0 else f + 1 + s

    for ch in range(len(chunks)):
        for dr in range(2):
            @pl.when(sends(dr, 0))
            def _(dr=dr, ch=ch):
                w_copy(dr, 0, ch, f).start()

    def w_arrive(s, ch):
        for dr in range(2):
            @pl.when(gets(dr, s))
            def _(dr=dr):
                q = came(dr, s)
                w_copy(dr, s, ch, q).wait_recv()
                if s + 1 < steps:
                    @pl.when(has_next(dr))
                    def _():
                        w_copy(dr, s + 1, ch, q).start()
                for k in range(1, nc):
                    w_share(dr, s, ch, q, k).start()

    table = [sorted(range(nf), key=lambda q, g=g: (abs(q - g), q)) for g in range(nf)]
    order = [pick([table[g][i] for g in range(nf)], f) for i in range(nf)]
    way = [pick([int(table[g][i] > g) for g in range(nf)], f) for i in range(nf)]
    dist = [pick([max(abs(table[g][i] - g) - 1, 0) for g in range(nf)], f) for i in range(nf)]

    def w_ready(slot, ch):
        region = wbuf.at[order[slot], 0 : (nc - 1) * R, pl.ds(chunks[ch][0], chunks[ch][1])]
        if nc > 1:
            landed(region, wf_rs.at[way[slot], dist[slot], ch])

    def send_gate(e):
        cols = pl.ds(pl.multiple_of(pt[e] * LW, 128), LW)
        return copy(z_ref.at[:, cols], z_all.at[own_rows, :], z_ss.at[0], z_rs.at[e], {"tensor": pt[e]})

    early = nt - 1 if nt > 2 else nt
    for e in range(1, early):
        send_gate(e)
    h1.wait()
    h2.wait()
    live = (idx > 0).astype(F32)

    def conv(src, halo, col, tap_col):
        lanes = pl.ds(col, 128)
        wide = pl.ds(tap_col, 128)
        ext = jnp.concatenate([halo[HALO - 8 : HALO, lanes].astype(F32) * live, src[:, lanes].astype(F32)], axis=0)
        acc = bias_ref[wide][None, :] + taps_ref[0:1, wide] * ext[5 : 5 + L]
        for k in range(1, 4):
            acc = acc + taps_ref[k : k + 1, wide] * ext[5 + k : 5 + k + L]
        return (acc / (1.0 + jnp.exp(-acc))).astype(BF)

    wide0 = x_ref.shape[1]
    for j in range(2 * N // 128):
        bc_all[own_rows, j * 128 : (j + 1) * 128] = conv(bc_ref, halo_bc, j * 128, wide0 + j * 128)
    bcs = [
        copy(bc_all.at[own_rows, :], bc_all.at[own_rows, :], bc_ss.at[0], bc_rs.at[e], {"tensor": pt[e]})
        for e in range(1, nt)
    ]
    xs = []

    def conv_group(e, store):
        base = pt[e] * LW

        def lap(j, carry):
            col = pl.multiple_of(base + j * 128, 128)
            store(pl.ds(pl.multiple_of(j * 128, 128), 128), conv(x_ref, halo_x, col, col))
            return carry

        lax.fori_loop(0, LW // 128, lap, 0)

    for e in range(1, nt):
        def put(lanes, val, e=e):
            x_send[e - 1, :, lanes] = val

        conv_group(e, put)
        xs.append(copy(x_send.at[e - 1], x_all.at[own_rows, :], x_ss.at[0], x_rs.at[e], {"tensor": pt[e]}))
    def put_own(lanes, val):
        x_all[own_rows, lanes] = val

    conv_group(0, put_own)
    e_s[...] = (iota((128, LW), 1) // HS == iota((128, LW), 0)).astype(F32)
    spread16 = e_s[...].astype(BF)

    def spread(rows):
        return dot(jnp.broadcast_to(rows, (8, 128)), e_s[...], precision=HI)

    landed(dt_all.at[0 : nt - 1], dt_rs.at[0])
    HR = at_s.shape[1]
    HA = dt_ref.shape[0]
    sel = ((iota((HA, 128), 0) == iota((HA, 128), 1) + t * hl) & (iota((HA, 128), 1) < hl)).astype(BF)
    sel_t = ((iota((HR, HA), 1) == iota((HR, HA), 0) + t * hl) & (iota((HR, HA), 0) < hl)).astype(BF)
    eye = (iota((HR, 128), 0) == iota((HR, 128), 1)).astype(F32)
    place_head = (iota((hl, 128), 0) == iota((hl, 128), 1)).astype(F32)
    hp = [
        dot(jnp.broadcast_to(v[...], (8, hl)), place_head, precision=HI)[0:1, :] for v in (sb_ref, dr_ref, sk_ref)
    ]
    hp_t = [dot(eye, jnp.broadcast_to(v, (8, 128)), 1, 1, HI)[:, 0:1] for v in hp[0:2]]
    tri = (iota((L, L), 0) >= iota((L, L), 1)).astype(F32)

    def softplus(v):
        return jnp.maximum(v, 0.0) + jnp.log1p(jnp.exp(-jnp.abs(v)))

    for b in range(nt):
        rows = slice(b * L, (b + 1) * L)
        raw = dt_all[b]
        step = softplus(dot(raw, sel, 0, 0) + hp[0])
        step_s[rows, :] = step
        a_s[rows, :] = dot(tri, -step * jnp.exp(hp[1]), precision=HI)
        step_t = softplus(dot(sel_t, raw) + hp_t[0])
        stept_s[b] = step_t
        at_s[b] = dot(-step_t * jnp.exp(hp_t[1]), tri, 1, 1, HI)
    before = jnp.zeros((1, 128), F32)
    for b in range(nt):
        last = a_s[(b + 1) * L - 1 : (b + 1) * L, :]
        stl[b, N : N + 8, :] = spread(jnp.exp(before))
        loc_s[b, N : N + 8, :] = spread(jnp.exp(last))
        before = before + last
    msg[N : N + 16, :] = jnp.broadcast_to(spread(jnp.exp(before))[0:1, :], (16, LW)).astype(BF)
    skip_s[...] = spread(hp[2])
    cu = dot(up_ref[...], cot_ref[...], 1, 1)
    left = iota((L, 2 * HS), 1) < HS

    def spans_of(e):
        b = pt[e]
        rows = pl.ds(pl.multiple_of(b * L, L), L)
        if e > 0:
            bcs[e - 1].wait_recv()
            xs[e - 1].wait_recv()
        a = a_s[rows, :]
        weight = (jnp.exp(a[L - 1 : L, :] - a) * step_s[rows, :]).astype(BF)
        xw = (x_all[rows, :].astype(F32) * dot(weight, spread16)).astype(BF)
        loc_s[b, 0:N, :] = dot(bc_all[rows, 0:N], xw, 0, 0)
        gram = dot(bc_all[rows, N : 2 * N], bc_all[rows, 0:N], 1, 1)
        gram = jnp.where(iota((L, L), 0) >= iota((L, L), 1), gram, 0.0)
        at = at_s[b]
        stt = stept_s[b]
        for pair in range(hl // 2):
            lanes = slice(pair * 2 * HS, (pair + 1) * 2 * HS)
            xp = x_all[rows, lanes]
            out = []
            for h in (2 * pair, 2 * pair + 1):
                gap = jnp.minimum(a[:, h : h + 1] - at[h : h + 1, :], 0.0)
                m = (jnp.exp(gap) * gram * stt[h : h + 1, :]).astype(BF)
                out.append(dot(m, xp))
            y_s[rows, lanes] = jnp.where(left, out[0], out[1])

    for e in range(nt):

        spans_of(e)
        if e == 0:
            w_arrive(0, 0)
        if e == min(1, nt - 2):
            for ch in range(1, len(chunks)):
                w_arrive(0, ch)
        if e == nt - 2:
            sent(x_send, x_ss.at[0])
            for i in range(early, nt):
                send_gate(i)

    state = jnp.zeros((N, LW), F32)
    for b in range(nt):
        stl[b, 0:N, :] = state
        state = loc_s[b, N : N + 1, :] * state + loc_s[b, 0:N, :]
    msg[0:N, :] = state.astype(BF)
    sts = [
        copy(msg, st_in.at[c], st_ss.at[k], st_rs.at[k], {"context": lax.rem(c + k, nc)})
        for k in range(1, nc)
    ]

    for cp in sts:
        cp.wait()
    inc_s[...] = jnp.zeros_like(inc_s)

    def chain(k, carry):
        inc_s[...] = st_in[k, N : N + 16, :].astype(F32)[0:1, :] * inc_s[...] + st_in[k, 0:N, :].astype(F32)
        return carry

    lax.fori_loop(0, c, chain, 0)
    own_w.wait()
    skip = skip_s[0:1, :]
    ones = jnp.ones((8, LW), BF)

    nx, ny = grid_of(nt)
    xi, yi = lax.rem(t, nx), lax.div(t, nx)
    top, low = slice(0, L // 2), slice(L // 2, L)
    xo = nx - 1 - xi

    def to_x(u, by):
        return remote(
            rs_send.at[by, xo, top, spans[u]], rs_xa.at[by, :, spans[u]], rs_ss.at[0], rs_rs.at[u, 0],
            {"tensor": yi * nx + xo},
        )

    def to_y(u, j, bx):
        ty = lax.rem(yi + j, ny)
        return remote(
            rs_send.at[ty, bx, low, spans[u]], rs_yb.at[ny - j - 1, bx, :, spans[u]], rs_ss.at[1], rs_rs.at[u, 1],
            {"tensor": ty * nx + xi},
        )

    def send_block(u, by, bx):
        @pl.when(bx != xi)
        def _():
            to_x(u, by).start()

        for j in range(1, ny):
            @pl.when(lax.rem(yi + j, ny) == by)
            def _(j=j):
                to_y(u, j, bx).start()

    def send_unit(u):
        if nx > 1:
            to_x(u, slice(None)).start()
        for j in range(1, ny):
            to_y(u, j, slice(None)).start()

    def second(u):
        cols = spans[u]
        if nx > 1:
            landed(rs_xa.at[:, :, cols], rs_rs.at[u, 0])
        if ny > 1:
            landed(rs_yb.at[:, :, :, cols], rs_rs.at[u, 1])
        for j in range(1, ny):
            ty = lax.rem(yi + j, ny)
            acc = rs_send[ty, xi, top, cols].astype(F32)
            if nx > 1:
                acc = acc + rs_xa[ty, :, cols].astype(F32)
            sum_a[j - 1, :, cols] = acc.astype(BF)
            remote(
                sum_a.at[j - 1, :, cols], in_a.at[ny - j - 1, :, cols], rs_ss.at[2], rs_rs.at[u, 2], {"tensor": ty * nx + xi}
            ).start()
        if nx > 1:
            acc = rs_send[yi, xo, low, cols].astype(F32)
            for j in range(1, ny):
                acc = acc + rs_yb[j - 1, xo, :, cols].astype(F32)
            sum_b[:, cols] = acc.astype(BF)
            remote(
                sum_b.at[:, cols], in_b.at[:, cols], rs_ss.at[3], rs_rs.at[u, 3], {"tensor": yi * nx + xo}
            ).start()

    units = [(0, None, 0, W)] + [(s, ch) + chunks[ch] for s in range(1, nf) for ch in range(len(chunks))]
    spans = [pl.ds(pl.multiple_of(order[s] * W + off, 128), wide) for s, _, off, wide in units]

    held = max(nt - 1, 1)

    def gate(e, carry):
        b = peer(e)
        rows = pl.ds(pl.multiple_of(b * L, L), L)

        @pl.when(e == 0)
        def _():
            own_z.wait()

        if steps > 1:
            @pl.when(e == nt - 1)
            def _():
                w_arrive(1, 0)

        @pl.when(e > 0)
        def _():
            remote(
                z_ref.at[:, own_cols], z_all.at[rows, :], z_ss.at[0], z_rs.at[e], {"tensor": b}
            ).wait_recv()

        start = (stl[b, 0:N, :] + stl[b, N : N + 1, :] * inc_s[...]).astype(BF)
        reach = dot(jnp.exp(a_s[rows, :]).astype(BF), spread16)
        y = y_s[rows, :] + reach * dot(bc_all[rows, N : 2 * N], start)
        y = y + skip * x_all[rows, :].astype(F32)
        z = z_all[rows, :].astype(F32)
        g = y * (z / (1.0 + jnp.exp(-z)))
        out = (g * gain_ref[...][None, :]).astype(BF)
        g_s[rows, :] = out
        adx[b, 0:16, :] = dot(down_ref[...], out, 1, 1)
        adx[b, 16:24, :] = dot(ones, (g * g).astype(BF), 1, 1)

        @pl.when(e > 0)
        def _():
            remote(adx.at[b], ad_in.at[e], ad_ss.at[0], ad_rs.at[0], {"tensor": b}).start()

        by, bx = lax.div(b, nx), lax.rem(b, nx)
        rs_send[by, bx, :, spans[0]] = dot(out, wbuf[f]).astype(BF)

        @pl.when((e > 0) & (e < held))
        def _():
            send_block(0, by, bx)

        return carry

    lax.fori_loop(0, nt, gate, 0)

    def project(u):
        slot, ch, off, wide = units[u]
        w_ready(slot, ch)

        def lap(by, carry):
            rows = pl.ds(pl.multiple_of(by * (nx * L), L), nx * L)
            out = dot(g_s[rows, :], wbuf[order[slot], :, off : off + wide]).astype(BF)
            for bx in range(nx):
                rs_send[by, bx, :, spans[u]] = out[bx * L : (bx + 1) * L]
            return carry

        lax.fori_loop(0, ny, lap, 0)

    nch = len(chunks)
    for ch in range(nch):
        project(1 + ch)
    landed(ad_in.at[1:nt], ad_rs.at[0])
    red = adx[t]
    for e in range(1, nt):
        red = red + ad_in[e]
    scale_row = lax.rsqrt(red[16:17, :] / (LW * nt) + EPS)
    ad16 = red[0:16, :].astype(BF)
    factor = 2.0 / math.sqrt(L * nt * nc * nf)
    ag_own[...] = (factor * scale_row * cu).astype(BF)
    for e in range(1, nt):
        copy(ag_own, ag_all.at[t], ag_ss.at[0], ag_rs.at[0], {"tensor": pt[e]})
    gb_own[...] = dot((factor * scale_row * ad16.astype(F32)).astype(BF), cot_ref[...]).astype(BF)
    part = gb_own.shape[1] // nt
    own_part = pl.ds(pl.multiple_of(t * part, 128), part)
    for e in range(1, nt):
        copy(
            gb_own.at[:, pl.ds(pl.multiple_of(pt[e] * part, 128), part)],
            gb_in.at[e], ga_ss.at[0], ga_rs.at[0], {"tensor": pt[e]},
        )
    for e in range(held, nt):
        send_block(0, lax.div(pt[e], nx), lax.rem(pt[e], nx))
    for ch in range(nch):
        send_unit(1 + ch)
    scale_col = dot(jnp.broadcast_to(scale_row, (8, L)), jnp.full((8, 128), 0.125, F32), 0, 0, HI)[:, 0:1]
    if steps > 1:
        for ch in range(1, nch):
            w_arrive(1, ch)
    for s in range(2, nf - 1):
        if s > 2:
            for ch in range(nch):
                w_arrive(s - 1, ch)
        for ch in range(nch):
            project(1 + (s - 1) * nch + ch)
            send_unit(1 + (s - 1) * nch + ch)
    second(0)
    landed(ag_all.at[0 : nt - 1], ag_rs.at[0])
    landed(gb_in.at[1:nt], ga_rs.at[0])
    ag_all[t] = ag_own[...]
    grad = jnp.zeros((16, LW), F32)
    for s in range(nt):
        grad = grad + dot(ag_all[s], g_s[s * L : (s + 1) * L, :])
    comb[:, 0:LW] = grad
    acc = gb_own[:, own_part].astype(F32)
    for e in range(1, nt):
        acc = acc + gb_in[e].astype(F32)
    comb[:, LW : LW + part] = acc
    lanes = (LW + part) // 128
    per = -(-lanes // nc)

    def seg(i):
        return pl.ds(pl.multiple_of(jnp.minimum(i * per, lanes - per) * 128, 128), per * 128)

    ccs = [
        copy(comb.at[:, seg(lax.rem(c + k, nc))], comb_c.at[k], cc_ss.at[k], cc_rs.at[k], {"context": lax.rem(c + k, nc)})
        for k in range(1, nc)
    ]
    for ch in range(nch):
        second(1 + ch)
    for cp in ccs:
        cp.wait()
    acc = comb[:, seg(c)]
    for k in range(1, nc):
        acc = acc + comb_c[k]
    comb2[...] = acc.astype(BF)
    for k in range(1, nf):
        copy(comb2, comb_f.at[f], cf_ss.at[0], cf_rs.at[0], {"fsdp": lax.rem(f + k, nf)})
    comb_f[f] = comb2[...]
    def finish(u):
        cols = spans[u]
        up_part = rs_send[yi, xi, top, cols].astype(F32)
        low_part = rs_send[yi, xi, low, cols].astype(F32)
        if nx > 1:
            landed(in_b.at[:, cols], rs_rs.at[u, 3])
            up_part = up_part + rs_xa[yi, :, cols].astype(F32)
            low_part = low_part + in_b[:, cols].astype(F32)
        if ny > 1:
            landed(in_a.at[:, :, cols], rs_rs.at[u, 2])
        for j in range(1, ny):
            up_part = up_part + in_a[j - 1, :, cols].astype(F32)
            low_part = low_part + rs_yb[j - 1, xi, :, cols].astype(F32)
        acc = jnp.concatenate([up_part, low_part], axis=0) + 2.0 * dot(ad16, up_ref[:, cols], 0, 0)
        mixed_ref[:, cols] = (scale_col * acc).astype(BF)

    finish(0)
    for u in range(1 + nch, 1 + (nf - 2) * nch):
        second(u)
    for ch in range(nch):
        finish(1 + ch)
    last = 1 + (nf - 2) * nch
    for ch in range(nch):
        if steps > 2:
            w_arrive(steps - 1, ch)
        if nf > 2:
            project(last + ch)
            send_unit(last + ch)
        if ch == 0:
            for u in range(1 + nch, last):
                finish(u)
    if nf > 2:
        for ch in range(nch - 1):
            second(last + ch)
    landed(comb_f.at[0 : nf - 1], cf_rs.at[0])
    acc = comb_f[0].astype(F32)
    for k in range(1, nf):
        acc = acc + comb_f[k].astype(F32)
    seg_own[...] = acc
    sgs = [copy(seg_own, seg_in.at[c], sg_ss.at[k], sg_rs.at[k], {"context": lax.rem(c + k, nc)}) for k in range(1, nc)]
    seg_in[c] = acc
    if nf > 2:
        second(last + nch - 1)
    for cp in sgs:
        cp.wait()
    for i in range(nc):
        full[:, seg(i)] = seg_in[i]
    ga_ref[...] = full[:, 0:LW]
    fin[t] = full[:, LW : LW + part]
    for e in range(1, nt):
        copy(fin.at[t], fin.at[t], fin_ss.at[0], fin_rs.at[0], {"tensor": pt[e]})
    if nf > 2:
        for ch in range(nch):
            finish(last + ch)
    landed(fin.at[0 : nt - 1], fin_rs.at[0])
    for s in range(nt):
        gb_ref[:, s * part : (s + 1) * part] = fin[s]
    sent(dt_all.at[0 : nt - 1], dt_ss.at[0])
    sent(bc_all.at[0 : (nt - 1) * L, :], bc_ss.at[0])
    sent(z_all.at[0 : (nt - 1) * L, :], z_ss.at[0])
    sent(ad_in.at[1:nt], ad_ss.at[0])
    sent(ag_all.at[0 : nt - 1], ag_ss.at[0])
    sent(gb_in.at[1:nt], ga_ss.at[0])
    sent(comb_f.at[0 : nf - 1], cf_ss.at[0])
    sent(fin.at[0 : nt - 1], fin_ss.at[0])
    if nx > 1:
        sent(rs_xa, rs_ss.at[0])
        sent(in_b, rs_ss.at[3])
    if ny > 1:
        sent(rs_yb, rs_ss.at[1])
        sent(in_a, rs_ss.at[2])
    for s in range(steps):
        for dr in range(2):
            @pl.when(sends(dr, s))
            def _(dr=dr, s=s):
                sent(wbuf.at[0, 0:R, :], w_ss.at[dr, s])

            if nc > 1:
                @pl.when(gets(dr, s))
                def _(dr=dr, s=s):
                    sent(wbuf.at[0, 0 : (nc - 1) * R, :], wf_ss.at[dr, s])


def write_out(mixed, ga, gb, mixed_out, ga_out, gb_out, sem):
    copies = [
        pltpu.make_async_copy(src, dst, sem.at[i])
        for i, (src, dst) in enumerate(((mixed, mixed_out), (ga, ga_out), (gb, gb_out)))
    ]
    for cp in copies:
        cp.start()
    for cp in copies:
        cp.wait()


def shards(x, bc, z, dt, taps, bias, step_bias, rate, skip, gain, w, down, up, cot):
    nt, nf, nc = lax.axis_size("tensor"), lax.axis_size("fsdp"), lax.axis_size("context")
    L, full = x.shape[1], x.shape[2]
    LW, hl, W, M = gain.shape[0], step_bias.shape[0], w.shape[1], cot.shape[2]
    BC = bc.shape[2]
    N = BC // 2
    HR = -(-hl // 8) * 8
    T = nt * L
    part = M // nt
    nx, ny = grid_of(nt)
    my = max(ny - 1, 1)
    dt = dt[0].T
    down = down.T
    nch = len(column_chunks(W))
    units = 1 + (nf - 1) * nch
    lanes = (LW + part) // 128
    SW = -(-lanes // nc) * 128
    vm = pl.BlockSpec(memory_space=pltpu.VMEM)
    hbm = pl.BlockSpec(memory_space=pl.ANY)
    V = pltpu.VMEM
    D = pltpu.SemaphoreType.DMA
    scratch = [
        V((L, full), BF), V((L, BC), BF), V(dt.shape, BF), V(taps.shape, F32), V((full + BC,), F32), V((LW,), F32),
        V(down.shape, BF), V(up.shape, BF), V((L, M), BF),
        V((HALO, full), BF), V((HALO, BC), BF), V((nt - 1, L, LW), BF), V((T, LW), BF), V((T, LW), BF),
        V((T, BC), BF), V((nt,) + dt.shape, BF), V((nf, LW, W), BF), V((T, 128), F32), V((T, 128), F32),
        V((nt, HR, L), F32), V((nt, HR, L), F32),
        V((nt, N + 8, LW), F32), V((nt, N + 8, LW), F32), V((8, LW), F32), V((N + 16, LW), BF), V((nc, N + 16, LW), BF), V((N, LW), F32),
        V((128, LW), F32), V((T, LW), F32), V((T, LW), BF), V((nt, 24, L), F32), V((nt, 24, L), F32),
        V((16, L), BF), V((nt, 16, L), BF), V((16, M), BF), V((nt, 16, part), BF),
        V((16, LW + part), F32), V((nc, 16, SW), F32), V((16, SW), BF), V((nf, 16, SW), BF),
        V((16, SW), F32), V((nc, 16, SW), F32), V((16, LW + part), F32),
        V((nt, 16, part), F32), V((ny, nx, L, M), BF), V((ny, L // 2, M), BF), V((my, nx, L // 2, M), BF),
        V((my, L // 2, M), BF), V((my, L // 2, M), BF), V((L // 2, M), BF), V((L // 2, M), BF),
        D((9,)), D((2,)), D((2,)), D((1,)), D((1,)), D((1,)), D((nt,)), D((1,)), D((nt,)), D((1,)), D((nt,)),
        D((2, nf - 1)), D((2, nf - 1, nch)), D((2, nf - 1)), D((2, nf - 1, nch)), D((nc,)), D((nc,)),
        D((1,)), D((1,)), D((1,)), D((1,)), D((1,)), D((1,)), D((nc,)), D((nc,)), D((1,)), D((1,)),
        D((nc,)), D((nc,)), D((1,)), D((1,)), D((4,)), D((units, 4)), D((2,)),
    ]
    mixed, ga, gb = pl.pallas_call(
        functools.partial(kernel, nt, nf, nc, hl),
        out_shape=(V((L, M), BF), V((16, LW), F32), V((16, M), F32)),
        in_specs=[hbm, hbm, hbm, hbm, hbm, hbm, vm, vm, vm, hbm, hbm, hbm, hbm, hbm],
        out_specs=(vm, vm, vm),
        scratch_shapes=scratch,
        compiler_params=pltpu.CompilerParams(
            collective_id=0, has_side_effects=True, vmem_limit_bytes=62 * 1024 * 1024
        ),
    )(x[0], bc[0], z[0], dt, taps, bias, step_bias[None], rate[None], skip[None], gain, w, down, up, cot[0])
    mixed, ga, gb = (pltpu.with_memory_space_constraint(v, pltpu.VMEM) for v in (mixed, ga, gb))
    mixed, ga, gb = pl.pallas_call(
        write_out,
        out_shape=(
            jax.ShapeDtypeStruct((L, M), BF),
            jax.ShapeDtypeStruct((16, LW), F32),
            jax.ShapeDtypeStruct((16, M), F32),
        ),
        in_specs=[vm, vm, vm],
        out_specs=(hbm, hbm, hbm),
        scratch_shapes=[D((3,))],
    )(mixed, ga, gb)
    return mixed[None], ga.T, gb


def solution(mesh):
    tokens = P("fsdp", ("context", "tensor"), None)
    placed = (
        tokens, tokens, tokens, tokens, P(), P(), P("tensor"), P("tensor"), P("tensor"), P("tensor"),
        P("tensor", "fsdp"), P("tensor", None), P(), tokens,
    )
    return jax.shard_map(
        shards, mesh=mesh, in_specs=placed, out_specs=(tokens, P("tensor", None), P()), check_vma=False
    )
```

```python
import functools
import math

import jax
import jax.numpy as jnp
from jax import lax
from jax.experimental import pallas as pl
from jax.experimental.pallas import tpu as pltpu
from jax.sharding import PartitionSpec as P

EPS = 1e-05
MESH = pl.DeviceIdType.MESH
HI = lax.Precision.HIGHEST
BF = jnp.bfloat16
F32 = jnp.float32
HALO = 8


def dot(a, b, ca=1, cb=0, precision=None):
    return lax.dot_general(
        a, b, (((ca,), (cb,)), ((), ())), preferred_element_type=F32, precision=precision
    )


def iota(shape, dim):
    return lax.broadcasted_iota(jnp.int32, shape, dim)


def pick(values, i):
    out = jnp.int32(values[0])
    for k in range(1, len(values)):
        out = jnp.where(i == k, jnp.int32(values[k]), out)
    return out


def grid_of(count):
    return (2, count // 2) if count % 2 == 0 else (1, count)


def column_chunks(width):
    first = max(width - 128, 128)
    return [(0, first), (first, width - first)] if width > first else [(0, width)]


def kernel(
    nt, nf, nc, hl,
    x_hbm, bc_hbm, z_ref, dt_hbm, taps_hbm, bias_hbm, sb_ref, dr_ref, sk_ref, gain_hbm, w_ref, down_hbm, up_hbm, cot_hbm,
    mixed_ref, ga_ref, gb_ref,
    x_ref, bc_ref, dt_ref, taps_ref, bias_ref, gain_ref, down_ref, up_ref, cot_ref,
    halo_x, halo_bc, x_send, x_all, z_all, bc_all, dt_all, wbuf, a_s, step_s, at_s, stept_s,
    stl, loc_s, skip_s, msg, st_in, inc_s, e_s, y_s, g_s, adx, ad_in, ag_own, ag_all, gb_own, gb_in,
    comb, comb_c, comb2, comb_f, seg_own, seg_in, full, fin, rs_send, rs_xa, rs_yb, sum_a, in_a, sum_b, in_b,
    ld, h_ss, h_rs, dt_ss, dt_rs, bc_ss, bc_rs, x_ss, x_rs, z_ss, z_rs, w_ss, w_rs, wf_ss, wf_rs, st_ss, st_rs,
    ad_ss, ad_rs, ag_ss, ag_rs, ga_ss, ga_rs, cc_ss, cc_rs, cf_ss, cf_rs, sg_ss, sg_rs, fin_ss, fin_rs, rs_ss, rs_rs, loc,
):
    t = lax.axis_index("tensor")
    f = lax.axis_index("fsdp")
    c = lax.axis_index("context")
    L = x_ref.shape[0]
    LW = x_all.shape[1]
    W = w_ref.shape[1]
    N = bc_ref.shape[1] // 2
    R = w_ref.shape[0] // nc
    HS = LW // hl
    idx = c * nt + t
    total = nc * nt
    bits = [1 << i for i in range(nt.bit_length() - 1)]
    chunks = column_chunks(W)
    steps = nf - 1

    def peer(e):
        out = 0
        for bit in bits:
            out = out + bit * lax.rem(lax.div(t, bit) + lax.div(e, bit), 2)
        return out

    def peers():
        return [peer(jnp.int32(e)) for e in range(nt)]

    pt = peers()

    def place(i):
        return {"context": i // nt, "tensor": lax.rem(i, nt)}

    def remote(src, dst, ss, rs, dev):
        return pltpu.make_async_remote_copy(
            src_ref=src, dst_ref=dst, send_sem=ss, recv_sem=rs, device_id=dev, device_id_type=MESH
        )

    def sent(region, sem):
        remote(region, region, sem, sem, {"tensor": pt[nt - 1]}).wait_send()

    def landed(region, sem):
        remote(region, region, sem, sem, {"tensor": pt[nt - 1]}).wait_recv()

    def copy(src, dst, ss, rs, dev):
        cp = remote(src, dst, ss, rs, dev)
        cp.start()
        return cp

    loads = []
    for i, (src, dst) in enumerate((
        (x_hbm, x_ref), (bc_hbm, bc_ref), (dt_hbm, dt_ref), (taps_hbm, taps_ref), (bias_hbm, bias_ref),
        (gain_hbm, gain_ref), (down_hbm, down_ref), (up_hbm, up_ref), (cot_hbm, cot_ref),
    )):
        cp = pltpu.make_async_copy(src, dst, ld.at[i])
        cp.start()
        loads.append(cp)
    own_w = pltpu.make_async_copy(w_ref, wbuf.at[f], loc.at[0])
    own_w.start()
    own_rows = pl.ds(pl.multiple_of(t * L, L), L)
    own_cols = pl.ds(pl.multiple_of(t * LW, 128), LW)
    own_z = pltpu.make_async_copy(z_ref.at[:, own_cols], z_all.at[own_rows, :], loc.at[1])
    own_z.start()

    nxt, prv = lax.rem(idx + 1, total), lax.rem(idx + total - 1, total)
    bar = pltpu.get_barrier_semaphore()
    greet = [{"tensor": pt[e]} for e in range(1, nt)]
    greet += [{"context": lax.rem(c + k, nc)} for k in range(1, nc)]
    greet += [place(nxt), place(prv)]
    for dev in greet:
        pl.semaphore_signal(bar, inc=1, device_id=dev, device_id_type=MESH)
    for near, to in ((f >= 1, f - 1), (f + 1 < nf, f + 1)):
        @pl.when(near)
        def _(to=to):
            pl.semaphore_signal(bar, inc=1, device_id={"fsdp": to}, device_id_type=MESH)

    pl.semaphore_wait(bar, len(greet) + (f >= 1).astype(jnp.int32) + (f + 1 < nf).astype(jnp.int32))

    share = pl.ds(pl.multiple_of(c * R, 16), R)

    def w_copy(dr, s, ch, q):
        cols = pl.ds(chunks[ch][0], chunks[ch][1])
        src = w_ref.at[share, cols] if s == 0 else wbuf.at[q, share, cols]
        to = f + 1 if dr == 0 else f - 1
        return remote(src, wbuf.at[q, share, cols], w_ss.at[dr, s], w_rs.at[dr, s, ch], {"fsdp": to})

    def w_share(dr, s, ch, q, k):
        region = wbuf.at[q, share, pl.ds(chunks[ch][0], chunks[ch][1])]
        return remote(region, region, wf_ss.at[dr, s], wf_rs.at[dr, s, ch], {"context": lax.rem(c + k, nc)})

    def has_next(dr):
        return f + 1 < nf if dr == 0 else f >= 1

    def sends(dr, s):
        return (f - s >= 0) & (f + 1 < nf) if dr == 0 else (f + s < nf) & (f >= 1)

    def gets(dr, s):
        return f - 1 - s >= 0 if dr == 0 else f + 1 + s < nf

    def came(dr, s):
        return f - 1 - s if dr == 0 else f + 1 + s

    for ch in range(len(chunks)):
        for dr in range(2):
            @pl.when(sends(dr, 0))
            def _(dr=dr, ch=ch):
                w_copy(dr, 0, ch, f).start()

    for cp in loads:
        cp.wait()
    h1 = copy(x_ref.at[L - HALO : L, :], halo_x, h_ss.at[0], h_rs.at[0], place(nxt))
    h2 = copy(bc_ref.at[L - HALO : L, :], halo_bc, h_ss.at[1], h_rs.at[1], place(nxt))
    for e in range(1, nt):
        copy(dt_ref, dt_all.at[t], dt_ss.at[0], dt_rs.at[0], {"tensor": pt[e]})
    dt_all[t] = dt_ref[...]

    def w_arrive(s, ch):
        for dr in range(2):
            @pl.when(gets(dr, s))
            def _(dr=dr):
                q = came(dr, s)
                w_copy(dr, s, ch, q).wait_recv()
                if s + 1 < steps:
                    @pl.when(has_next(dr))
                    def _():
                        w_copy(dr, s + 1, ch, q).start()
                for k in range(1, nc):
                    w_share(dr, s, ch, q, k).start()

    table = [sorted(range(nf), key=lambda q, g=g: (abs(q - g), q)) for g in range(nf)]
    order = [pick([table[g][i] for g in range(nf)], f) for i in range(nf)]
    way = [pick([int(table[g][i] > g) for g in range(nf)], f) for i in range(nf)]
    dist = [pick([max(abs(table[g][i] - g) - 1, 0) for g in range(nf)], f) for i in range(nf)]

    def w_ready(slot, ch):
        region = wbuf.at[order[slot], 0 : (nc - 1) * R, pl.ds(chunks[ch][0], chunks[ch][1])]
        if nc > 1:
            landed(region, wf_rs.at[way[slot], dist[slot], ch])

    def send_gate(e):
        cols = pl.ds(pl.multiple_of(pt[e] * LW, 128), LW)
        return copy(z_ref.at[:, cols], z_all.at[own_rows, :], z_ss.at[0], z_rs.at[e], {"tensor": pt[e]})

    early = nt - 1 if nt > 2 else nt
    for e in range(1, early):
        send_gate(e)
    h1.wait()
    h2.wait()
    live = (idx > 0).astype(F32)

    def conv(src, halo, col, tap_col):
        lanes = pl.ds(col, 128)
        wide = pl.ds(tap_col, 128)
        ext = jnp.concatenate([halo[HALO - 8 : HALO, lanes].astype(F32) * live, src[:, lanes].astype(F32)], axis=0)
        acc = bias_ref[wide][None, :] + taps_ref[0:1, wide] * ext[5 : 5 + L]
        for k in range(1, 4):
            acc = acc + taps_ref[k : k + 1, wide] * ext[5 + k : 5 + k + L]
        return (acc / (1.0 + jnp.exp(-acc))).astype(BF)

    wide0 = x_ref.shape[1]
    for j in range(2 * N // 128):
        bc_all[own_rows, j * 128 : (j + 1) * 128] = conv(bc_ref, halo_bc, j * 128, wide0 + j * 128)
    bcs = [
        copy(bc_all.at[own_rows, :], bc_all.at[own_rows, :], bc_ss.at[0], bc_rs.at[e], {"tensor": pt[e]})
        for e in range(1, nt)
    ]
    xs = []

    def conv_group(e, store):
        base = pt[e] * LW

        def lap(j, carry):
            col = pl.multiple_of(base + j * 128, 128)
            store(pl.ds(pl.multiple_of(j * 128, 128), 128), conv(x_ref, halo_x, col, col))
            return carry

        lax.fori_loop(0, LW // 128, lap, 0)

    for e in range(1, nt):
        def put(lanes, val, e=e):
            x_send[e - 1, :, lanes] = val

        conv_group(e, put)
        xs.append(copy(x_send.at[e - 1], x_all.at[own_rows, :], x_ss.at[0], x_rs.at[e], {"tensor": pt[e]}))
    def put_own(lanes, val):
        x_all[own_rows, lanes] = val

    conv_group(0, put_own)
    e_s[...] = (iota((128, LW), 1) // HS == iota((128, LW), 0)).astype(F32)
    spread16 = e_s[...].astype(BF)

    def spread(rows):
        return dot(jnp.broadcast_to(rows, (8, 128)), e_s[...], precision=HI)

    landed(dt_all.at[0 : nt - 1], dt_rs.at[0])
    HR = at_s.shape[1]
    HA = dt_ref.shape[0]
    sel = ((iota((HA, 128), 0) == iota((HA, 128), 1) + t * hl) & (iota((HA, 128), 1) < hl)).astype(BF)
    sel_t = ((iota((HR, HA), 1) == iota((HR, HA), 0) + t * hl) & (iota((HR, HA), 0) < hl)).astype(BF)
    eye = (iota((HR, 128), 0) == iota((HR, 128), 1)).astype(F32)
    place_head = (iota((hl, 128), 0) == iota((hl, 128), 1)).astype(F32)
    hp = [
        dot(jnp.broadcast_to(v[...], (8, hl)), place_head, precision=HI)[0:1, :] for v in (sb_ref, dr_ref, sk_ref)
    ]
    hp_t = [dot(eye, jnp.broadcast_to(v, (8, 128)), 1, 1, HI)[:, 0:1] for v in hp[0:2]]
    tri = (iota((L, L), 0) >= iota((L, L), 1)).astype(F32)

    def softplus(v):
        return jnp.maximum(v, 0.0) + jnp.log1p(jnp.exp(-jnp.abs(v)))

    for b in range(nt):
        rows = slice(b * L, (b + 1) * L)
        raw = dt_all[b]
        step = softplus(dot(raw, sel, 0, 0) + hp[0])
        step_s[rows, :] = step
        a_s[rows, :] = dot(tri, -step * jnp.exp(hp[1]), precision=HI)
        step_t = softplus(dot(sel_t, raw) + hp_t[0])
        stept_s[b] = step_t
        at_s[b] = dot(-step_t * jnp.exp(hp_t[1]), tri, 1, 1, HI)
    before = jnp.zeros((1, 128), F32)
    for b in range(nt):
        last = a_s[(b + 1) * L - 1 : (b + 1) * L, :]
        stl[b, N : N + 8, :] = spread(jnp.exp(before))
        loc_s[b, N : N + 8, :] = spread(jnp.exp(last))
        before = before + last
    msg[N : N + 16, :] = jnp.broadcast_to(spread(jnp.exp(before))[0:1, :], (16, LW)).astype(BF)
    skip_s[...] = spread(hp[2])
    cu = dot(up_ref[...], cot_ref[...], 1, 1)
    left = iota((L, 2 * HS), 1) < HS

    def spans_of(e):
        b = pt[e]
        rows = pl.ds(pl.multiple_of(b * L, L), L)
        if e > 0:
            bcs[e - 1].wait_recv()
            xs[e - 1].wait_recv()
        a = a_s[rows, :]
        weight = (jnp.exp(a[L - 1 : L, :] - a) * step_s[rows, :]).astype(BF)
        xw = (x_all[rows, :].astype(F32) * dot(weight, spread16)).astype(BF)
        loc_s[b, 0:N, :] = dot(bc_all[rows, 0:N], xw, 0, 0)
        gram = dot(bc_all[rows, N : 2 * N], bc_all[rows, 0:N], 1, 1)
        gram = jnp.where(iota((L, L), 0) >= iota((L, L), 1), gram, 0.0)
        at = at_s[b]
        stt = stept_s[b]
        for pair in range(hl // 2):
            lanes = slice(pair * 2 * HS, (pair + 1) * 2 * HS)
            xp = x_all[rows, lanes]
            out = []
            for h in (2 * pair, 2 * pair + 1):
                gap = jnp.minimum(a[:, h : h + 1] - at[h : h + 1, :], 0.0)
                m = (jnp.exp(gap) * gram * stt[h : h + 1, :]).astype(BF)
                out.append(dot(m, xp))
            y_s[rows, lanes] = jnp.where(left, out[0], out[1])

    for e in range(nt):

        spans_of(e)
        if e == 0:
            w_arrive(0, 0)
        if e == min(1, nt - 2):
            for ch in range(1, len(chunks)):
                w_arrive(0, ch)
        if e == nt - 2:
            sent(x_send, x_ss.at[0])
            for i in range(early, nt):
                send_gate(i)

    state = jnp.zeros((N, LW), F32)
    for b in range(nt):
        stl[b, 0:N, :] = state
        state = loc_s[b, N : N + 1, :] * state + loc_s[b, 0:N, :]
    msg[0:N, :] = state.astype(BF)

    def state_copy(k, src):
        return remote(msg, st_in.at[src], st_ss.at[k], st_rs.at[k], {"context": lax.rem(c + k, nc)})

    for k in range(1, nc):
        @pl.when(c + k < nc)
        def _(k=k):
            state_copy(k, c).start()

    for k in range(1, nc):
        @pl.when(c >= k)
        def _(k=k):
            state_copy(k, lax.rem(c + nc - k, nc)).wait_recv()

    inc_s[...] = jnp.zeros_like(inc_s)

    def chain(k, carry):
        inc_s[...] = st_in[k, N : N + 16, :].astype(F32)[0:1, :] * inc_s[...] + st_in[k, 0:N, :].astype(F32)
        return carry

    lax.fori_loop(0, c, chain, 0)
    own_w.wait()
    skip = skip_s[0:1, :]
    ones = jnp.ones((8, LW), BF)

    nx, ny = grid_of(nt)
    xi, yi = lax.rem(t, nx), lax.div(t, nx)
    top, low = slice(0, L // 2), slice(L // 2, L)
    xo = nx - 1 - xi

    def to_x(u, by):
        return remote(
            rs_send.at[by, xo, top, spans[u]], rs_xa.at[by, :, spans[u]], rs_ss.at[0], rs_rs.at[u, 0],
            {"tensor": yi * nx + xo},
        )

    def to_y(u, j, bx):
        ty = lax.rem(yi + j, ny)
        return remote(
            rs_send.at[ty, bx, low, spans[u]], rs_yb.at[ny - j - 1, bx, :, spans[u]], rs_ss.at[1], rs_rs.at[u, 1],
            {"tensor": ty * nx + xi},
        )

    def send_block(u, by, bx):
        @pl.when(bx != xi)
        def _():
            to_x(u, by).start()

        for j in range(1, ny):
            @pl.when(lax.rem(yi + j, ny) == by)
            def _(j=j):
                to_y(u, j, bx).start()

    def send_unit(u):
        if nx > 1:
            to_x(u, slice(None)).start()
        for j in range(1, ny):
            to_y(u, j, slice(None)).start()

    def second(u):
        cols = spans[u]
        if nx > 1:
            landed(rs_xa.at[:, :, cols], rs_rs.at[u, 0])
        if ny > 1:
            landed(rs_yb.at[:, :, :, cols], rs_rs.at[u, 1])
        for j in range(1, ny):
            ty = lax.rem(yi + j, ny)
            acc = rs_send[ty, xi, top, cols].astype(F32)
            if nx > 1:
                acc = acc + rs_xa[ty, :, cols].astype(F32)
            sum_a[j - 1, :, cols] = acc.astype(BF)
            remote(
                sum_a.at[j - 1, :, cols], in_a.at[ny - j - 1, :, cols], rs_ss.at[2], rs_rs.at[u, 2], {"tensor": ty * nx + xi}
            ).start()
        if nx > 1:
            acc = rs_send[yi, xo, low, cols].astype(F32)
            for j in range(1, ny):
                acc = acc + rs_yb[j - 1, xo, :, cols].astype(F32)
            sum_b[:, cols] = acc.astype(BF)
            remote(
                sum_b.at[:, cols], in_b.at[:, cols], rs_ss.at[3], rs_rs.at[u, 3], {"tensor": yi * nx + xo}
            ).start()

    units = [(0, None, 0, W)] + [(s, ch) + chunks[ch] for s in range(1, nf) for ch in range(len(chunks))]
    spans = [pl.ds(pl.multiple_of(order[s] * W + off, 128), wide) for s, _, off, wide in units]

    def gate(e, carry):
        b = peer(e)
        rows = pl.ds(pl.multiple_of(b * L, L), L)

        @pl.when(e == 0)
        def _():
            own_z.wait()

        if steps > 1:
            @pl.when(e == nt - 1)
            def _():
                w_arrive(1, 0)

        @pl.when(e > 0)
        def _():
            remote(
                z_ref.at[:, own_cols], z_all.at[rows, :], z_ss.at[0], z_rs.at[e], {"tensor": b}
            ).wait_recv()

        start = (stl[b, 0:N, :] + stl[b, N : N + 1, :] * inc_s[...]).astype(BF)
        reach = dot(jnp.exp(a_s[rows, :]).astype(BF), spread16)
        y = y_s[rows, :] + reach * dot(bc_all[rows, N : 2 * N], start)
        y = y + skip * x_all[rows, :].astype(F32)
        z = z_all[rows, :].astype(F32)
        g = y * (z / (1.0 + jnp.exp(-z)))
        out = (g * gain_ref[...][None, :]).astype(BF)
        g_s[rows, :] = out
        adx[b, 0:16, :] = dot(down_ref[...], out, 1, 1)
        adx[b, 16:24, :] = dot(ones, (g * g).astype(BF), 1, 1)

        @pl.when(e > 0)
        def _():
            remote(adx.at[b], ad_in.at[e], ad_ss.at[0], ad_rs.at[0], {"tensor": b}).start()

        by, bx = lax.div(b, nx), lax.rem(b, nx)
        rs_send[by, bx, :, spans[0]] = dot(out, wbuf[f]).astype(BF)

        @pl.when(e > 0)
        def _():
            send_block(0, by, bx)

        return carry

    lax.fori_loop(0, nt, gate, 0)

    def project(u):
        slot, ch, off, wide = units[u]
        w_ready(slot, ch)

        def lap(by, carry):
            rows = pl.ds(pl.multiple_of(by * (nx * L), L), nx * L)
            out = dot(g_s[rows, :], wbuf[order[slot], :, off : off + wide]).astype(BF)
            for bx in range(nx):
                rs_send[by, bx, :, spans[u]] = out[bx * L : (bx + 1) * L]
            return carry

        lax.fori_loop(0, ny, lap, 0)

    nch = len(chunks)
    for ch in range(nch):
        project(1 + ch)
        send_unit(1 + ch)
    landed(ad_in.at[1:nt], ad_rs.at[0])
    red = adx[t]
    for e in range(1, nt):
        red = red + ad_in[e]
    scale_row = lax.rsqrt(red[16:17, :] / (LW * nt) + EPS)
    ad16 = red[0:16, :].astype(BF)
    factor = 2.0 / math.sqrt(L * nt * nc * nf)
    ag_own[...] = (factor * scale_row * cu).astype(BF)
    for e in range(1, nt):
        copy(ag_own, ag_all.at[t], ag_ss.at[0], ag_rs.at[0], {"tensor": pt[e]})
    gb_own[...] = dot((factor * scale_row * ad16.astype(F32)).astype(BF), cot_ref[...]).astype(BF)
    part = gb_own.shape[1] // nt
    own_part = pl.ds(pl.multiple_of(t * part, 128), part)
    for e in range(1, nt):
        copy(
            gb_own.at[:, pl.ds(pl.multiple_of(pt[e] * part, 128), part)],
            gb_in.at[e], ga_ss.at[0], ga_rs.at[0], {"tensor": pt[e]},
        )
    scale_col = dot(jnp.broadcast_to(scale_row, (8, L)), jnp.full((8, 128), 0.125, F32), 0, 0, HI)[:, 0:1]
    if steps > 1:
        for ch in range(1, nch):
            w_arrive(1, ch)
    for s in range(2, nf - 1):
        if s > 2:
            for ch in range(nch):
                w_arrive(s - 1, ch)
        for ch in range(nch):
            project(1 + (s - 1) * nch + ch)
            send_unit(1 + (s - 1) * nch + ch)
    second(0)
    for ch in range(nch):
        second(1 + ch)
    landed(ag_all.at[0 : nt - 1], ag_rs.at[0])
    landed(gb_in.at[1:nt], ga_rs.at[0])
    def finish(u):
        cols = spans[u]
        up_part = rs_send[yi, xi, top, cols].astype(F32)
        low_part = rs_send[yi, xi, low, cols].astype(F32)
        if nx > 1:
            landed(in_b.at[:, cols], rs_rs.at[u, 3])
            up_part = up_part + rs_xa[yi, :, cols].astype(F32)
            low_part = low_part + in_b[:, cols].astype(F32)
        if ny > 1:
            landed(in_a.at[:, :, cols], rs_rs.at[u, 2])
        for j in range(1, ny):
            up_part = up_part + in_a[j - 1, :, cols].astype(F32)
            low_part = low_part + rs_yb[j - 1, xi, :, cols].astype(F32)
        acc = jnp.concatenate([up_part, low_part], axis=0) + 2.0 * dot(ad16, up_ref[:, cols], 0, 0)
        mixed_ref[:, cols] = (scale_col * acc).astype(BF)

    ag_all[t] = ag_own[...]
    grad = jnp.zeros((16, LW), F32)
    for s in range(nt):
        grad = grad + dot(ag_all[s], g_s[s * L : (s + 1) * L, :])
    comb[:, 0:LW] = grad
    acc = gb_own[:, own_part].astype(F32)
    for e in range(1, nt):
        acc = acc + gb_in[e].astype(F32)
    comb[:, LW : LW + part] = acc
    lanes = (LW + part) // 128
    per = -(-lanes // nc)

    def seg(i):
        return pl.ds(pl.multiple_of(jnp.minimum(i * per, lanes - per) * 128, 128), per * 128)

    ccs = [
        copy(comb.at[:, seg(lax.rem(c + k, nc))], comb_c.at[k], cc_ss.at[k], cc_rs.at[k], {"context": lax.rem(c + k, nc)})
        for k in range(1, nc)
    ]
    finish(0)
    for cp in ccs:
        cp.wait()
    acc = comb[:, seg(c)]
    for k in range(1, nc):
        acc = acc + comb_c[k]
    comb2[...] = acc.astype(BF)
    comb_f[f] = comb2[...]
    for u in range(1 + nch, 1 + (nf - 2) * nch):
        second(u)
    for ch in range(nch):
        finish(1 + ch)
    last = 1 + (nf - 2) * nch
    for ch in range(nch):

        if steps > 2:
            w_arrive(steps - 1, ch)
        if ch == 0:
            for k in range(1, nf):
                copy(comb2, comb_f.at[f], cf_ss.at[0], cf_rs.at[0], {"fsdp": lax.rem(f + k, nf)})
        if nf > 2:

            project(last + ch)
            send_unit(last + ch)
        if ch == 0:

            for u in range(1 + nch, last):
                finish(u)
    if nf > 2:

        for ch in range(nch - 1):
            second(last + ch)
    landed(comb_f.at[0 : nf - 1], cf_rs.at[0])
    acc = comb_f[0].astype(F32)
    for k in range(1, nf):
        acc = acc + comb_f[k].astype(F32)
    seg_own[...] = acc
    sgs = [copy(seg_own, seg_in.at[c], sg_ss.at[k], sg_rs.at[k], {"context": lax.rem(c + k, nc)}) for k in range(1, nc)]
    seg_in[c] = acc
    if nf > 2:
        second(last + nch - 1)
    for cp in sgs:
        cp.wait()
    for i in range(nc):
        full[:, seg(i)] = seg_in[i]
    ga_ref[...] = full[:, 0:LW]
    fin[t] = full[:, LW : LW + part]
    for e in range(1, nt):
        copy(fin.at[t], fin.at[t], fin_ss.at[0], fin_rs.at[0], {"tensor": pt[e]})
    if nf > 2:
        for ch in range(nch):
            finish(last + ch)
    landed(fin.at[0 : nt - 1], fin_rs.at[0])
    for s in range(nt):
        gb_ref[:, s * part : (s + 1) * part] = fin[s]
    sent(dt_all.at[0 : nt - 1], dt_ss.at[0])
    for k in range(1, nc):
        @pl.when(c + k < nc)
        def _(k=k):
            state_copy(k, c).wait_send()

    sent(bc_all.at[0 : (nt - 1) * L, :], bc_ss.at[0])
    sent(z_all.at[0 : (nt - 1) * L, :], z_ss.at[0])
    sent(ad_in.at[1:nt], ad_ss.at[0])
    sent(ag_all.at[0 : nt - 1], ag_ss.at[0])
    sent(gb_in.at[1:nt], ga_ss.at[0])
    sent(comb_f.at[0 : nf - 1], cf_ss.at[0])
    sent(fin.at[0 : nt - 1], fin_ss.at[0])
    if nx > 1:
        sent(rs_xa, rs_ss.at[0])
        sent(in_b, rs_ss.at[3])
    if ny > 1:
        sent(rs_yb, rs_ss.at[1])
        sent(in_a, rs_ss.at[2])
    for s in range(steps):
        for dr in range(2):
            @pl.when(sends(dr, s))
            def _(dr=dr, s=s):
                sent(wbuf.at[0, 0:R, :], w_ss.at[dr, s])

            if nc > 1:
                @pl.when(gets(dr, s))
                def _(dr=dr, s=s):
                    sent(wbuf.at[0, 0 : (nc - 1) * R, :], wf_ss.at[dr, s])


def write_out(mixed, ga, gb, mixed_out, ga_out, gb_out, sem):
    copies = [
        pltpu.make_async_copy(src, dst, sem.at[i])
        for i, (src, dst) in enumerate(((mixed, mixed_out), (ga, ga_out), (gb, gb_out)))
    ]
    for cp in copies:
        cp.start()
    for cp in copies:
        cp.wait()


def shards(x, bc, z, dt, taps, bias, step_bias, rate, skip, gain, w, down, up, cot):
    nt, nf, nc = lax.axis_size("tensor"), lax.axis_size("fsdp"), lax.axis_size("context")
    L, full = x.shape[1], x.shape[2]
    LW, hl, W, M = gain.shape[0], step_bias.shape[0], w.shape[1], cot.shape[2]
    BC = bc.shape[2]
    N = BC // 2
    HR = -(-hl // 8) * 8
    T = nt * L
    part = M // nt
    nx, ny = grid_of(nt)
    my = max(ny - 1, 1)
    dt = dt[0].T
    down = down.T
    nch = len(column_chunks(W))
    units = 1 + (nf - 1) * nch
    lanes = (LW + part) // 128
    SW = -(-lanes // nc) * 128
    vm = pl.BlockSpec(memory_space=pltpu.VMEM)
    hbm = pl.BlockSpec(memory_space=pl.ANY)
    V = pltpu.VMEM
    D = pltpu.SemaphoreType.DMA
    scratch = [
        V((L, full), BF), V((L, BC), BF), V(dt.shape, BF), V(taps.shape, F32), V((full + BC,), F32), V((LW,), F32),
        V(down.shape, BF), V(up.shape, BF), V((L, M), BF),
        V((HALO, full), BF), V((HALO, BC), BF), V((nt - 1, L, LW), BF), V((T, LW), BF), V((T, LW), BF),
        V((T, BC), BF), V((nt,) + dt.shape, BF), V((nf, LW, W), BF), V((T, 128), F32), V((T, 128), F32),
        V((nt, HR, L), F32), V((nt, HR, L), F32),
        V((nt, N + 8, LW), F32), V((nt, N + 8, LW), F32), V((8, LW), F32), V((N + 16, LW), BF), V((nc, N + 16, LW), BF), V((N, LW), F32),
        V((128, LW), F32), V((T, LW), F32), V((T, LW), BF), V((nt, 24, L), F32), V((nt, 24, L), F32),
        V((16, L), BF), V((nt, 16, L), BF), V((16, M), BF), V((nt, 16, part), BF),
        V((16, LW + part), F32), V((nc, 16, SW), F32), V((16, SW), BF), V((nf, 16, SW), BF),
        V((16, SW), F32), V((nc, 16, SW), F32), V((16, LW + part), F32),
        V((nt, 16, part), F32), V((ny, nx, L, M), BF), V((ny, L // 2, M), BF), V((my, nx, L // 2, M), BF),
        V((my, L // 2, M), BF), V((my, L // 2, M), BF), V((L // 2, M), BF), V((L // 2, M), BF),
        D((9,)), D((2,)), D((2,)), D((1,)), D((1,)), D((1,)), D((nt,)), D((1,)), D((nt,)), D((1,)), D((nt,)),
        D((2, nf - 1)), D((2, nf - 1, nch)), D((2, nf - 1)), D((2, nf - 1, nch)), D((nc,)), D((nc,)),
        D((1,)), D((1,)), D((1,)), D((1,)), D((1,)), D((1,)), D((nc,)), D((nc,)), D((1,)), D((1,)),
        D((nc,)), D((nc,)), D((1,)), D((1,)), D((4,)), D((units, 4)), D((2,)),
    ]
    mixed, ga, gb = pl.pallas_call(
        functools.partial(kernel, nt, nf, nc, hl),
        out_shape=(V((L, M), BF), V((16, LW), F32), V((16, M), F32)),
        in_specs=[hbm, hbm, hbm, hbm, hbm, hbm, vm, vm, vm, hbm, hbm, hbm, hbm, hbm],
        out_specs=(vm, vm, vm),
        scratch_shapes=scratch,
        compiler_params=pltpu.CompilerParams(
            collective_id=0, has_side_effects=True, vmem_limit_bytes=62 * 1024 * 1024
        ),
    )(x[0], bc[0], z[0], dt, taps, bias, step_bias[None], rate[None], skip[None], gain, w, down, up, cot[0])
    mixed, ga, gb = (pltpu.with_memory_space_constraint(v, pltpu.VMEM) for v in (mixed, ga, gb))
    mixed, ga, gb = pl.pallas_call(
        write_out,
        out_shape=(
            jax.ShapeDtypeStruct((L, M), BF),
            jax.ShapeDtypeStruct((16, LW), F32),
            jax.ShapeDtypeStruct((16, M), F32),
        ),
        in_specs=[vm, vm, vm],
        out_specs=(hbm, hbm, hbm),
        scratch_shapes=[D((3,))],
    )(mixed, ga, gb)
    return mixed[None], ga.T, gb


def solution(mesh):
    tokens = P("fsdp", ("context", "tensor"), None)
    placed = (
        tokens, tokens, tokens, tokens, P(), P(), P("tensor"), P("tensor"), P("tensor"), P("tensor"),
        P("tensor", "fsdp"), P("tensor", None), P(), tokens,
    )
    return jax.shard_map(
        shards, mesh=mesh, in_specs=placed, out_specs=(tokens, P("tensor", None), P()), check_vma=False
    )
```

```python
import functools
import math

import jax
import jax.numpy as jnp
from jax import lax
from jax.experimental import pallas as pl
from jax.experimental.pallas import tpu as pltpu
from jax.sharding import PartitionSpec as P

EPS = 1e-05
MESH = pl.DeviceIdType.MESH
HI = lax.Precision.HIGHEST
BF = jnp.bfloat16
F32 = jnp.float32
HALO = 8


def dot(a, b, ca=1, cb=0, precision=None):
    return lax.dot_general(
        a, b, (((ca,), (cb,)), ((), ())), preferred_element_type=F32, precision=precision
    )


def iota(shape, dim):
    return lax.broadcasted_iota(jnp.int32, shape, dim)


def pick(values, i):
    out = jnp.int32(values[0])
    for k in range(1, len(values)):
        out = jnp.where(i == k, jnp.int32(values[k]), out)
    return out


def grid_of(count):
    return 2, count // 2


def column_chunks(width):
    first = max(width // 256 * 128, 128)
    cuts = sorted({0, min(first, width), min(max(width - 128, first), width), width})
    return [(a, b - a) for a, b in zip(cuts, cuts[1:])]


def kernel(
    nt, nf, nc, hl,
    x_hbm, bc_hbm, z_ref, dt_hbm, taps_hbm, bias_hbm, sb_ref, dr_ref, sk_ref, gain_hbm, w_ref, down_hbm, up_hbm, cot_hbm,
    mixed_ref, ga_ref, gb_ref,
    x_ref, bc_ref, dt_ref, taps_ref, bias_ref, gain_ref, down_ref, up_ref, cot_ref,
    halo_x, halo_bc, x_send, x_all, z_all, bc_all, dt_all, wbuf, a_s, step_s, at_s, stept_s,
    stl, loc_s, skip_s, msg, st_in, inc_s, e_s, y_s, g_s, adx, ad_in, ag_own, ag_all, gb_own, gb_in,
    comb, comb_c, comb2, comb_f, seg_own, seg_in, full, fin, rs_send, rs_in, sums, sums_in, rs_near,
    ld, h_ss, h_rs, dt_ss, dt_rs, bc_ss, bc_rs, x_ss, x_rs, z_ss, z_rs, w_ss, w_rs, wf_ss, wf_rs, st_ss, st_rs,
    ad_ss, ad_rs, ag_ss, ag_rs, ga_ss, ga_rs, cc_ss, cc_rs, cf_ss, cf_rs, sg_ss, sg_rs, fin_ss, fin_rs, rs_ss, rs_rs, loc,
):
    t = lax.axis_index("tensor")
    f = lax.axis_index("fsdp")
    c = lax.axis_index("context")
    L = x_ref.shape[0]
    LW = x_all.shape[1]
    W = w_ref.shape[1]
    N = bc_ref.shape[1] // 2
    R = w_ref.shape[0] // nc
    HS = LW // hl
    idx = c * nt + t
    total = nc * nt
    bits = [1 << i for i in range(nt.bit_length() - 1)]
    chunks = column_chunks(W)
    nch = len(chunks)
    steps = nf - 1

    def peer(e):
        out = 0
        for bit in bits:
            out = out + bit * lax.rem(lax.div(t, bit) + lax.div(e, bit), 2)
        return out

    def peers():
        return [peer(jnp.int32(e)) for e in range(nt)]

    pt = peers()

    def place(i):
        return {"context": i // nt, "tensor": lax.rem(i, nt)}

    def remote(src, dst, ss, rs, dev):
        return pltpu.make_async_remote_copy(
            src_ref=src, dst_ref=dst, send_sem=ss, recv_sem=rs, device_id=dev, device_id_type=MESH
        )

    def sent(region, sem):
        remote(region, region, sem, sem, {"tensor": pt[nt - 1]}).wait_send()

    def landed(region, sem):
        remote(region, region, sem, sem, {"tensor": pt[nt - 1]}).wait_recv()

    def copy(src, dst, ss, rs, dev):
        cp = remote(src, dst, ss, rs, dev)
        cp.start()
        return cp

    loads = []
    for i, (src, dst) in enumerate((
        (x_hbm, x_ref), (bc_hbm, bc_ref), (dt_hbm, dt_ref), (taps_hbm, taps_ref), (bias_hbm, bias_ref),
        (gain_hbm, gain_ref), (down_hbm, down_ref), (up_hbm, up_ref), (cot_hbm, cot_ref),
    )):
        cp = pltpu.make_async_copy(src, dst, ld.at[i])
        cp.start()
        loads.append(cp)
    own_w = pltpu.make_async_copy(w_ref, wbuf.at[f], loc.at[0])
    own_w.start()
    own_rows = pl.ds(pl.multiple_of(t * L, L), L)
    own_cols = pl.ds(pl.multiple_of(t * LW, 128), LW)
    own_z = pltpu.make_async_copy(z_ref.at[:, own_cols], z_all.at[own_rows, :], loc.at[1])
    own_z.start()

    nxt, prv = lax.rem(idx + 1, total), lax.rem(idx + total - 1, total)
    bar = pltpu.get_barrier_semaphore()
    greet = [{"tensor": pt[e]} for e in range(1, nt)]
    greet += [{"context": lax.rem(c + k, nc)} for k in range(1, nc)]
    greet += [place(nxt), place(prv)]
    for dev in greet:
        pl.semaphore_signal(bar, inc=1, device_id=dev, device_id_type=MESH)
    for near, to in ((f >= 1, f - 1), (f + 1 < nf, f + 1)):
        @pl.when(near)
        def _(to=to):
            pl.semaphore_signal(bar, inc=1, device_id={"fsdp": to}, device_id_type=MESH)

    pl.semaphore_wait(bar, len(greet) + (f >= 1).astype(jnp.int32) + (f + 1 < nf).astype(jnp.int32))

    share = pl.ds(pl.multiple_of(c * R, 16), R)

    def w_copy(dr, s, ch, q):
        cols = pl.ds(chunks[ch][0], chunks[ch][1])
        src = w_ref.at[share, cols] if s == 0 else wbuf.at[q, share, cols]
        to = f + 1 if dr == 0 else f - 1
        return remote(src, wbuf.at[q, share, cols], w_ss.at[dr, s], w_rs.at[dr, s, ch], {"fsdp": to})

    def w_share(dr, s, ch, q, k):
        region = wbuf.at[q, share, pl.ds(chunks[ch][0], chunks[ch][1])]
        return remote(region, region, wf_ss.at[dr, s], wf_rs.at[dr, s, ch], {"context": lax.rem(c + k, nc)})

    def has_next(dr):
        return f + 1 < nf if dr == 0 else f >= 1

    def sends(dr, s):
        return (f - s >= 0) & (f + 1 < nf) if dr == 0 else (f + s < nf) & (f >= 1)

    def gets(dr, s):
        return f - 1 - s >= 0 if dr == 0 else f + 1 + s < nf

    def came(dr, s):
        return f - 1 - s if dr == 0 else f + 1 + s

    for ch in range(len(chunks)):
        for dr in range(2):
            @pl.when(sends(dr, 0))
            def _(dr=dr, ch=ch):
                w_copy(dr, 0, ch, f).start()

    for cp in loads:
        cp.wait()
    h1 = copy(x_ref.at[L - HALO : L, :], halo_x, h_ss.at[0], h_rs.at[0], place(nxt))
    h2 = copy(bc_ref.at[L - HALO : L, :], halo_bc, h_ss.at[1], h_rs.at[1], place(nxt))
    for e in range(1, nt):
        copy(dt_ref, dt_all.at[t], dt_ss.at[0], dt_rs.at[0], {"tensor": pt[e]})
    dt_all[t] = dt_ref[...]

    def w_arrive(s, ch):
        for dr in range(2):
            @pl.when(gets(dr, s))
            def _(dr=dr):
                q = came(dr, s)
                w_copy(dr, s, ch, q).wait_recv()
                if s + 1 < steps:
                    @pl.when(has_next(dr))
                    def _():
                        w_copy(dr, s + 1, ch, q).start()
                for k in range(1, nc):
                    w_share(dr, s, ch, q, k).start()

    table = [sorted(range(nf), key=lambda q, g=g: (abs(q - g), q)) for g in range(nf)]
    order = [pick([table[g][i] for g in range(nf)], f) for i in range(nf)]
    way = [pick([int(table[g][i] > g) for g in range(nf)], f) for i in range(nf)]
    dist = [pick([max(abs(table[g][i] - g) - 1, 0) for g in range(nf)], f) for i in range(nf)]

    def w_ready(slot, ch):
        region = wbuf.at[order[slot], 0 : (nc - 1) * R, pl.ds(chunks[ch][0], chunks[ch][1])]
        if nc > 1:
            landed(region, wf_rs.at[way[slot], dist[slot], ch])

    def send_gate(e):
        cols = pl.ds(pl.multiple_of(pt[e] * LW, 128), LW)
        return copy(z_ref.at[:, cols], z_all.at[own_rows, :], z_ss.at[0], z_rs.at[e], {"tensor": pt[e]})

    early = nt - 1 if nt > 2 else nt
    for e in range(1, early):
        send_gate(e)
    h1.wait()
    h2.wait()
    live = (idx > 0).astype(F32)

    def conv(src, halo, col, tap_col):
        lanes = pl.ds(col, 128)
        wide = pl.ds(tap_col, 128)
        ext = jnp.concatenate([halo[HALO - 8 : HALO, lanes].astype(F32) * live, src[:, lanes].astype(F32)], axis=0)
        acc = bias_ref[wide][None, :] + taps_ref[0:1, wide] * ext[5 : 5 + L]
        for k in range(1, 4):
            acc = acc + taps_ref[k : k + 1, wide] * ext[5 + k : 5 + k + L]
        return (acc / (1.0 + jnp.exp(-acc))).astype(BF)

    wide0 = x_ref.shape[1]
    for j in range(2 * N // 128):
        bc_all[own_rows, j * 128 : (j + 1) * 128] = conv(bc_ref, halo_bc, j * 128, wide0 + j * 128)
    bcs = [
        copy(bc_all.at[own_rows, :], bc_all.at[own_rows, :], bc_ss.at[0], bc_rs.at[e], {"tensor": pt[e]})
        for e in range(1, nt)
    ]
    xs = []

    def conv_group(e, store):
        base = pt[e] * LW

        def lap(j, carry):
            col = pl.multiple_of(base + j * 128, 128)
            store(pl.ds(pl.multiple_of(j * 128, 128), 128), conv(x_ref, halo_x, col, col))
            return carry

        lax.fori_loop(0, LW // 128, lap, 0)

    for e in range(1, nt):
        def put(lanes, val, e=e):
            x_send[e - 1, :, lanes] = val

        conv_group(e, put)
        xs.append(copy(x_send.at[e - 1], x_all.at[own_rows, :], x_ss.at[0], x_rs.at[e], {"tensor": pt[e]}))
    def put_own(lanes, val):
        x_all[own_rows, lanes] = val

    conv_group(0, put_own)
    e_s[...] = (iota((128, LW), 1) // HS == iota((128, LW), 0)).astype(F32)
    spread16 = e_s[...].astype(BF)

    def spread(rows):
        return dot(jnp.broadcast_to(rows, (8, 128)), e_s[...], precision=HI)

    landed(dt_all.at[0 : nt - 1], dt_rs.at[0])
    HR = at_s.shape[1]
    HA = dt_ref.shape[0]
    sel = ((iota((HA, 128), 0) == iota((HA, 128), 1) + t * hl) & (iota((HA, 128), 1) < hl)).astype(BF)
    sel_t = ((iota((HR, HA), 1) == iota((HR, HA), 0) + t * hl) & (iota((HR, HA), 0) < hl)).astype(BF)
    eye = (iota((HR, 128), 0) == iota((HR, 128), 1)).astype(F32)
    place_head = (iota((hl, 128), 0) == iota((hl, 128), 1)).astype(F32)
    hp = [
        dot(jnp.broadcast_to(v[...], (8, hl)), place_head, precision=HI)[0:1, :] for v in (sb_ref, dr_ref, sk_ref)
    ]
    hp_t = [dot(eye, jnp.broadcast_to(v, (8, 128)), 1, 1, HI)[:, 0:1] for v in hp[0:2]]
    tri = (iota((L, L), 0) >= iota((L, L), 1)).astype(F32)

    def softplus(v):
        return jnp.maximum(v, 0.0) + jnp.log1p(jnp.exp(-jnp.abs(v)))

    for b in range(nt):
        rows = slice(b * L, (b + 1) * L)
        raw = dt_all[b]
        step = softplus(dot(raw, sel, 0, 0) + hp[0])
        step_s[rows, :] = step
        a_s[rows, :] = dot(tri, -step * jnp.exp(hp[1]), precision=HI)
        step_t = softplus(dot(sel_t, raw) + hp_t[0])
        stept_s[b] = step_t
        at_s[b] = dot(-step_t * jnp.exp(hp_t[1]), tri, 1, 1, HI)
    before = jnp.zeros((1, 128), F32)
    for b in range(nt):
        last = a_s[(b + 1) * L - 1 : (b + 1) * L, :]
        stl[b, N : N + 8, :] = spread(jnp.exp(before))
        loc_s[b, N : N + 8, :] = spread(jnp.exp(last))
        before = before + last
    msg[N : N + 16, :] = jnp.broadcast_to(spread(jnp.exp(before))[0:1, :], (16, LW)).astype(BF)
    skip_s[...] = spread(hp[2])
    cu = dot(up_ref[...], cot_ref[...], 1, 1)
    left = iota((L, 2 * HS), 1) < HS

    def spans_of(e):
        b = pt[e]
        rows = pl.ds(pl.multiple_of(b * L, L), L)
        if e > 0:
            bcs[e - 1].wait_recv()
            xs[e - 1].wait_recv()
        a = a_s[rows, :]
        weight = (jnp.exp(a[L - 1 : L, :] - a) * step_s[rows, :]).astype(BF)
        xw = (x_all[rows, :].astype(F32) * dot(weight, spread16)).astype(BF)
        loc_s[b, 0:N, :] = dot(bc_all[rows, 0:N], xw, 0, 0)
        gram = dot(bc_all[rows, N : 2 * N], bc_all[rows, 0:N], 1, 1)
        gram = jnp.where(iota((L, L), 0) >= iota((L, L), 1), gram, 0.0)
        at = at_s[b]
        stt = stept_s[b]
        for pair in range(hl // 2):
            lanes = slice(pair * 2 * HS, (pair + 1) * 2 * HS)
            xp = x_all[rows, lanes]
            out = []
            for h in (2 * pair, 2 * pair + 1):
                gap = jnp.minimum(a[:, h : h + 1] - at[h : h + 1, :], 0.0)
                m = (jnp.exp(gap) * gram * stt[h : h + 1, :]).astype(BF)
                out.append(dot(m, xp))
            y_s[rows, lanes] = jnp.where(left, out[0], out[1])

    for e in range(nt):

        spans_of(e)
        if e == 0:
            w_arrive(0, 0)
        if e == min(1, nt - 2):
            for ch in range(1, len(chunks)):
                w_arrive(0, ch)
        if e == nt - 2:
            sent(x_send, x_ss.at[0])
            for i in range(early, nt):
                send_gate(i)

    state = jnp.zeros((N, LW), F32)
    for b in range(nt):
        stl[b, 0:N, :] = state
        state = loc_s[b, N : N + 1, :] * state + loc_s[b, 0:N, :]
    msg[0:N, :] = state.astype(BF)

    def state_copy(k, src):
        return remote(msg, st_in.at[src], st_ss.at[k], st_rs.at[k], {"context": lax.rem(c + k, nc)})

    for k in range(1, nc):
        @pl.when(c + k < nc)
        def _(k=k):
            state_copy(k, c).start()

    if steps > 1:
        w_arrive(1, 0)
    for k in range(1, nc):
        @pl.when(c >= k)
        def _(k=k):
            state_copy(k, lax.rem(c + nc - k, nc)).wait_recv()

    inc_s[...] = jnp.zeros_like(inc_s)

    def chain(k, carry):
        inc_s[...] = st_in[k, N : N + 16, :].astype(F32)[0:1, :] * inc_s[...] + st_in[k, 0:N, :].astype(F32)
        return carry

    lax.fori_loop(0, c, chain, 0)
    own_w.wait()
    skip = skip_s[0:1, :]
    ones = jnp.ones((8, LW), BF)

    nx, ny = grid_of(nt)
    xi, yi = lax.rem(t, nx), lax.div(t, nx)
    top, low = slice(0, L // 2), slice(L // 2, L)
    xo = nx - 1 - xi

    def to_x(u, by, count):
        return remote(
            rs_send.at[pl.ds(by, count), xo, top, spans[u]], rs_in.at[pl.ds(by, count), :, spans[u]],
            rs_ss.at[0], rs_rs.at[u, 0], {"tensor": yi * nx + xo},
        )

    def to_y(u, j, bx, count):
        ty = lax.rem(yi + j, ny)
        src = rs_send.at[ty, pl.ds(bx, count), low, spans[u]]
        dst = rs_in.at[pl.ds(ny + (ny - j - 1) * nx + bx, count), :, spans[u]]
        return remote(src, dst, rs_ss.at[0], rs_rs.at[u, 0], {"tensor": ty * nx + xi})

    def send_block(u, by, bx):
        @pl.when(bx != xi)
        def _():
            to_x(u, by, 1).start()

        for j in range(1, ny):
            @pl.when(lax.rem(yi + j, ny) == by)
            def _(j=j):
                to_y(u, j, bx, 1).start()

    def send_unit(u):
        if u == len(units) - 1:
            for e in range(1, nt):
                remote(
                    rs_send.at[lax.div(pt[e], nx), lax.rem(pt[e], nx), :, spans[u]], rs_near.at[e - 1],
                    rs_ss.at[2], rs_rs.at[u, 0], {"tensor": pt[e]},
                ).start()
            return
        to_x(u, 0, ny).start()
        for j in range(1, ny):
            to_y(u, j, 0, nx).start()

    def from_y(j, bx, cols):
        return rs_in[ny + (j - 1) * nx + bx, :, cols].astype(F32)

    def second(u):
        cols = spans[u]
        landed(rs_in.at[:, :, cols], rs_rs.at[u, 0])
        for j in range(1, ny):
            ty = lax.rem(yi + j, ny)
            sums[j - 1, :, cols] = (rs_send[ty, xi, top, cols].astype(F32) + rs_in[ty, :, cols].astype(F32)).astype(BF)
            remote(
                sums.at[j - 1, :, cols], sums_in.at[ny - j - 1, :, cols], rs_ss.at[1], rs_rs.at[u, 1],
                {"tensor": ty * nx + xi},
            ).start()
        acc = rs_send[yi, xo, low, cols].astype(F32)
        for j in range(1, ny):
            acc = acc + from_y(j, xo, cols)
        sums[ny - 1, :, cols] = acc.astype(BF)
        remote(
            sums.at[ny - 1, :, cols], sums_in.at[ny - 1, :, cols], rs_ss.at[1], rs_rs.at[u, 1],
            {"tensor": yi * nx + xo},
        ).start()

    units = [(s, 0, W) for s in range(nf - 1)] + [(nf - 1,) + chunk for chunk in chunks]
    spans = [pl.ds(pl.multiple_of(order[s] * W + off, 128), wide) for s, off, wide in units]

    def gate(e, carry):
        b = peer(e)
        rows = pl.ds(pl.multiple_of(b * L, L), L)

        @pl.when(e == 0)
        def _():
            own_z.wait()

        if steps > 1:
            @pl.when(e == nt - 1)
            def _():
                for ch in range(1, nch - 1):
                    w_arrive(1, ch)

        @pl.when(e > 0)
        def _():
            remote(
                z_ref.at[:, own_cols], z_all.at[rows, :], z_ss.at[0], z_rs.at[e], {"tensor": b}
            ).wait_recv()

        start = (stl[b, 0:N, :] + stl[b, N : N + 1, :] * inc_s[...]).astype(BF)
        reach = dot(jnp.exp(a_s[rows, :]).astype(BF), spread16)
        y = y_s[rows, :] + reach * dot(bc_all[rows, N : 2 * N], start)
        y = y + skip * x_all[rows, :].astype(F32)
        z = z_all[rows, :].astype(F32)
        g = y * (z / (1.0 + jnp.exp(-z)))
        out = (g * gain_ref[...][None, :]).astype(BF)
        g_s[rows, :] = out
        adx[b, 0:16, :] = dot(down_ref[...], out, 1, 1)
        adx[b, 16:24, :] = dot(ones, (g * g).astype(BF), 1, 1)

        @pl.when(e > 0)
        def _():
            remote(adx.at[b], ad_in.at[e], ad_ss.at[0], ad_rs.at[0], {"tensor": b}).start()

        by, bx = lax.div(b, nx), lax.rem(b, nx)
        rs_send[by, bx, :, spans[0]] = dot(out, wbuf[f]).astype(BF)

        @pl.when(e > 0)
        def _():
            send_block(0, by, bx)

        return carry

    lax.fori_loop(0, nt, gate, 0)

    def project(u):
        slot, off, wide = units[u]
        for ch in range(nch):
            if off <= chunks[ch][0] < off + wide:
                w_ready(slot, ch)

        def lap(by, carry):
            rows = pl.ds(pl.multiple_of(by * (nx * L), L), nx * L)
            out = dot(g_s[rows, :], wbuf[order[slot], :, off : off + wide]).astype(BF)
            for bx in range(nx):
                rs_send[by, bx, :, spans[u]] = out[bx * L : (bx + 1) * L]
            return carry

        lax.fori_loop(0, ny, lap, 0)

    project(1)
    send_unit(1)
    if steps > 1:
        for ch in range(max(nch - 1, 1), nch):
            w_arrive(1, ch)
    landed(ad_in.at[1:nt], ad_rs.at[0])
    red = adx[t]
    for e in range(1, nt):
        red = red + ad_in[e]
    scale_row = lax.rsqrt(red[16:17, :] / (LW * nt) + EPS)
    ad16 = red[0:16, :].astype(BF)
    factor = 2.0 / math.sqrt(L * nt * nc * nf)
    ag_own[...] = (factor * scale_row * cu).astype(BF)
    for e in range(1, nt):
        copy(ag_own, ag_all.at[t], ag_ss.at[0], ag_rs.at[0], {"tensor": pt[e]})
    gb_own[...] = dot((factor * scale_row * ad16.astype(F32)).astype(BF), cot_ref[...]).astype(BF)
    part = gb_own.shape[1] // nt
    own_part = pl.ds(pl.multiple_of(t * part, 128), part)
    for e in range(1, nt):
        copy(
            gb_own.at[:, pl.ds(pl.multiple_of(pt[e] * part, 128), part)],
            gb_in.at[e], ga_ss.at[0], ga_rs.at[0], {"tensor": pt[e]},
        )
    scale_col = dot(jnp.broadcast_to(scale_row, (8, L)), jnp.full((8, 128), 0.125, F32), 0, 0, HI)[:, 0:1]
    for s in range(2, nf - 1):
        if s > 2:
            for ch in range(nch):
                w_arrive(s - 1, ch)
        project(s)
        send_unit(s)
    second(0)
    second(1)
    landed(ag_all.at[0 : nt - 1], ag_rs.at[0])
    landed(gb_in.at[1:nt], ga_rs.at[0])
    def finish(u):
        cols = spans[u]
        if u == len(units) - 1:
            landed(rs_near, rs_rs.at[u, 0])
            acc = rs_send[yi, xi, :, cols].astype(F32)
            for e in range(1, nt):
                acc = acc + rs_near[e - 1].astype(F32)
        else:
            landed(sums_in.at[:, :, cols], rs_rs.at[u, 1])
            up_part = rs_send[yi, xi, top, cols].astype(F32) + rs_in[yi, :, cols].astype(F32)
            low_part = rs_send[yi, xi, low, cols].astype(F32) + sums_in[ny - 1, :, cols].astype(F32)
            for j in range(1, ny):
                up_part = up_part + sums_in[j - 1, :, cols].astype(F32)
                low_part = low_part + from_y(j, xi, cols)
            acc = jnp.concatenate([up_part, low_part], axis=0)
        acc = acc + 2.0 * dot(ad16, up_ref[:, cols], 0, 0)
        mixed_ref[:, cols] = (scale_col * acc).astype(BF)

    ag_all[t] = ag_own[...]
    grad = jnp.zeros((16, LW), F32)
    for s in range(nt):
        grad = grad + dot(ag_all[s], g_s[s * L : (s + 1) * L, :])
    comb[:, 0:LW] = grad
    acc = gb_own[:, own_part].astype(F32)
    for e in range(1, nt):
        acc = acc + gb_in[e].astype(F32)
    comb[:, LW : LW + part] = acc
    lanes = (LW + part) // 128
    per = -(-lanes // nc)

    def seg(i):
        return pl.ds(pl.multiple_of(jnp.minimum(i * per, lanes - per) * 128, 128), per * 128)

    ccs = [
        copy(comb.at[:, seg(lax.rem(c + k, nc))], comb_c.at[k], cc_ss.at[k], cc_rs.at[k], {"context": lax.rem(c + k, nc)})
        for k in range(1, nc)
    ]
    last = nf - 1
    for u in range(2, last):
        second(u)
    near = dist[nf - 1] < steps - 1

    def last_slot(ch):
        project(last + ch)
        send_unit(last + ch)

    @pl.when(near)
    def _():
        for ch in range(nch):
            last_slot(ch)

    w_arrive(steps - 1, 0)

    @pl.when(jnp.logical_not(near))
    def _():
        last_slot(0)

    finish(0)
    for cp in ccs:
        cp.wait()
    acc = comb[:, seg(c)]
    for k in range(1, nc):
        acc = acc + comb_c[k]
    comb2[...] = acc.astype(BF)
    comb_f[f] = comb2[...]
    finish(1)
    for k in range(1, nf):
        copy(comb2, comb_f.at[f], cf_ss.at[0], cf_rs.at[0], {"fsdp": lax.rem(f + k, nf)})
    for ch in range(1, nch):
        w_arrive(steps - 1, ch)

        @pl.when(jnp.logical_not(near))
        def _(ch=ch):
            last_slot(ch)

        if ch == 1:
            for u in range(2, last):
                finish(u)
            second(last)
    landed(comb_f.at[0 : nf - 1], cf_rs.at[0])
    acc = comb_f[0].astype(F32)
    for k in range(1, nf):
        acc = acc + comb_f[k].astype(F32)
    seg_own[...] = acc
    sgs = [copy(seg_own, seg_in.at[c], sg_ss.at[k], sg_rs.at[k], {"context": lax.rem(c + k, nc)}) for k in range(1, nc)]
    seg_in[c] = acc
    for ch in range(1, nch - 1):
        second(last + ch)
    for cp in sgs:
        cp.wait()
    for i in range(nc):
        full[:, seg(i)] = seg_in[i]
    ga_ref[...] = full[:, 0:LW]
    fin[t] = full[:, LW : LW + part].astype(BF)
    for e in range(1, nt):
        copy(fin.at[t], fin.at[t], fin_ss.at[0], fin_rs.at[0], {"tensor": pt[e]})
    for ch in range(nch):
        finish(last + ch)
    landed(fin.at[0 : nt - 1], fin_rs.at[0])
    for s in range(nt):
        gb_ref[:, s * part : (s + 1) * part] = fin[s].astype(F32)
    sent(dt_all.at[0 : nt - 1], dt_ss.at[0])
    for k in range(1, nc):
        @pl.when(c + k < nc)
        def _(k=k):
            state_copy(k, c).wait_send()

    sent(bc_all.at[0 : (nt - 1) * L, :], bc_ss.at[0])
    sent(z_all.at[0 : (nt - 1) * L, :], z_ss.at[0])
    sent(ad_in.at[1:nt], ad_ss.at[0])
    sent(ag_all.at[0 : nt - 1], ag_ss.at[0])
    sent(gb_in.at[1:nt], ga_ss.at[0])
    sent(comb_f.at[0 : nf - 1], cf_ss.at[0])
    sent(fin.at[0 : nt - 1], fin_ss.at[0])
    head = slice(0, rs_in.shape[2] - chunks[-1][1])
    sent(rs_in.at[:, :, head], rs_ss.at[0])
    sent(sums_in.at[:, :, head], rs_ss.at[1])
    sent(rs_near, rs_ss.at[2])
    for s in range(steps):
        for dr in range(2):
            @pl.when(sends(dr, s))
            def _(dr=dr, s=s):
                sent(wbuf.at[0, 0:R, :], w_ss.at[dr, s])

            if nc > 1:
                @pl.when(gets(dr, s))
                def _(dr=dr, s=s):
                    sent(wbuf.at[0, 0 : (nc - 1) * R, :], wf_ss.at[dr, s])


def write_out(mixed, ga, gb, mixed_out, ga_out, gb_out, sem):
    copies = [
        pltpu.make_async_copy(src, dst, sem.at[i])
        for i, (src, dst) in enumerate(((mixed, mixed_out), (ga, ga_out), (gb, gb_out)))
    ]
    for cp in copies:
        cp.start()
    for cp in copies:
        cp.wait()


def shards(x, bc, z, dt, taps, bias, step_bias, rate, skip, gain, w, down, up, cot):
    nt, nf, nc = lax.axis_size("tensor"), lax.axis_size("fsdp"), lax.axis_size("context")
    L, full = x.shape[1], x.shape[2]
    LW, hl, W, M = gain.shape[0], step_bias.shape[0], w.shape[1], cot.shape[2]
    BC = bc.shape[2]
    N = BC // 2
    HR = -(-hl // 8) * 8
    T = nt * L
    part = M // nt
    nx, ny = grid_of(nt)
    dt = dt[0].T
    down = down.T
    nch = len(column_chunks(W))
    units = nf - 1 + nch
    lanes = (LW + part) // 128
    SW = -(-lanes // nc) * 128
    vm = pl.BlockSpec(memory_space=pltpu.VMEM)
    hbm = pl.BlockSpec(memory_space=pl.ANY)
    V = pltpu.VMEM
    D = pltpu.SemaphoreType.DMA
    scratch = [
        V((L, full), BF), V((L, BC), BF), V(dt.shape, BF), V(taps.shape, F32), V((full + BC,), F32), V((LW,), F32),
        V(down.shape, BF), V(up.shape, BF), V((L, M), BF),
        V((HALO, full), BF), V((HALO, BC), BF), V((nt - 1, L, LW), BF), V((T, LW), BF), V((T, LW), BF),
        V((T, BC), BF), V((nt,) + dt.shape, BF), V((nf, LW, W), BF), V((T, 128), F32), V((T, 128), F32),
        V((nt, HR, L), F32), V((nt, HR, L), F32),
        V((nt, N + 8, LW), F32), V((nt, N + 8, LW), F32), V((8, LW), F32), V((N + 16, LW), BF), V((nc, N + 16, LW), BF), V((N, LW), F32),
        V((128, LW), F32), V((T, LW), F32), V((T, LW), BF), V((nt, 24, L), F32), V((nt, 24, L), F32),
        V((16, L), BF), V((nt, 16, L), BF), V((16, M), BF), V((nt, 16, part), BF),
        V((16, LW + part), F32), V((nc, 16, SW), F32), V((16, SW), BF), V((nf, 16, SW), BF),
        V((16, SW), F32), V((nc, 16, SW), F32), V((16, LW + part), F32),
        V((nt, 16, part), BF), V((ny, nx, L, M), BF), V((ny + (ny - 1) * nx, L // 2, M), BF),
        V((ny, L // 2, M), BF), V((ny, L // 2, M), BF), V((nt - 1, L, column_chunks(W)[-1][1]), BF),
        D((9,)), D((2,)), D((2,)), D((1,)), D((1,)), D((1,)), D((nt,)), D((1,)), D((nt,)), D((1,)), D((nt,)),
        D((2, nf - 1)), D((2, nf - 1, nch)), D((2, nf - 1)), D((2, nf - 1, nch)), D((nc,)), D((nc,)),
        D((1,)), D((1,)), D((1,)), D((1,)), D((1,)), D((1,)), D((nc,)), D((nc,)), D((1,)), D((1,)),
        D((nc,)), D((nc,)), D((1,)), D((1,)), D((3,)), D((units, 2)), D((2,)),
    ]
    mixed, ga, gb = pl.pallas_call(
        functools.partial(kernel, nt, nf, nc, hl),
        out_shape=(V((L, M), BF), V((16, LW), F32), V((16, M), F32)),
        in_specs=[hbm, hbm, hbm, hbm, hbm, hbm, vm, vm, vm, hbm, hbm, hbm, hbm, hbm],
        out_specs=(vm, vm, vm),
        scratch_shapes=scratch,
        compiler_params=pltpu.CompilerParams(
            collective_id=0, has_side_effects=True, vmem_limit_bytes=62 * 1024 * 1024
        ),
    )(x[0], bc[0], z[0], dt, taps, bias, step_bias[None], rate[None], skip[None], gain, w, down, up, cot[0])
    mixed, ga, gb = (pltpu.with_memory_space_constraint(v, pltpu.VMEM) for v in (mixed, ga, gb))
    mixed, ga, gb = pl.pallas_call(
        write_out,
        out_shape=(
            jax.ShapeDtypeStruct((L, M), BF),
            jax.ShapeDtypeStruct((16, LW), F32),
            jax.ShapeDtypeStruct((16, M), F32),
        ),
        in_specs=[vm, vm, vm],
        out_specs=(hbm, hbm, hbm),
        scratch_shapes=[D((3,))],
    )(mixed, ga, gb)
    return mixed[None], ga.T, gb


def solution(mesh):
    tokens = P("fsdp", ("context", "tensor"), None)
    placed = (
        tokens, tokens, tokens, tokens, P(), P(), P("tensor"), P("tensor"), P("tensor"), P("tensor"),
        P("tensor", "fsdp"), P("tensor", None), P(), tokens,
    )
    return jax.shard_map(
        shards, mesh=mesh, in_specs=placed, out_specs=(tokens, P("tensor", None), P()), check_vma=False
    )
```

```python
import functools
import math

import jax
import jax.numpy as jnp
from jax import lax
from jax.experimental import pallas as pl
from jax.experimental.pallas import tpu as pltpu
from jax.sharding import PartitionSpec as P

EPS = 1e-05
MESH = pl.DeviceIdType.MESH
HI = lax.Precision.HIGHEST
BF = jnp.bfloat16
F32 = jnp.float32
HALO = 8


def dot(a, b, ca=1, cb=0, precision=None):
    return lax.dot_general(
        a, b, (((ca,), (cb,)), ((), ())), preferred_element_type=F32, precision=precision
    )


def iota(shape, dim):
    return lax.broadcasted_iota(jnp.int32, shape, dim)


def pick(values, i):
    out = jnp.int32(values[0])
    for k in range(1, len(values)):
        out = jnp.where(i == k, jnp.int32(values[k]), out)
    return out


def grid_of(count):
    return 2, count // 2


def column_chunks(width):
    cuts = sorted({0, max(width - 256, 128), max(width - 128, 128), width})
    return [(a, b - a) for a, b in zip(cuts, cuts[1:])]


def kernel(
    nt, nf, nc, hl,
    x_hbm, bc_hbm, z_ref, dt_hbm, taps_hbm, bias_hbm, sb_hbm, dr_hbm, sk_hbm, gain_hbm, w_ref, down_hbm, up_hbm, cot_hbm,
    mixed_ref, ga_ref, gb_ref,
    x_ref, bc_ref, dt_ref, taps_ref, bias_ref, gain_ref, down_ref, up_ref, cot_ref, sb_ref, dr_ref, sk_ref,
    halo_x, halo_bc, x_send, x_all, z_all, bc_all, dt_all, wbuf, a_s, step_s, at_s, stept_s,
    stl, loc_s, skip_s, msg, st_in, inc_s, e_s, y_s, g_s, adx, ad_in, ag_own, ag_all, gb_own, gb_in,
    comb, comb_c, comb2, comb_f, tot, seg_in, full, fin, rs_send, rs_in, sums, sums_in, rs_near,
    ld, h_ss, h_rs, dt_ss, dt_rs, bc_ss, bc_rs, x_ss, x_rs, z_ss, z_rs, w_ss, w_rs, wf_ss, wf_rs, st_ss, st_rs,
    ad_ss, ad_rs, ag_ss, ag_rs, ga_ss, ga_rs, cc_ss, cc_rs, cf_ss, cf_rs, tot_ss, tot_rs, sg_ss, sg_rs, fin_ss, fin_rs, rs_ss, rs_rs, loc,
):
    t = lax.axis_index("tensor")
    f = lax.axis_index("fsdp")
    c = lax.axis_index("context")
    L = x_ref.shape[0]
    LW = x_all.shape[1]
    W = w_ref.shape[1]
    N = bc_ref.shape[1] // 2
    R = w_ref.shape[0] // nc
    HS = LW // hl
    idx = c * nt + t
    total = nc * nt
    bits = [1 << i for i in range(nt.bit_length() - 1)]
    chunks = column_chunks(W)
    nch = len(chunks)
    steps = nf - 1

    def peer(e):
        out = 0
        for bit in bits:
            out = out + bit * lax.rem(lax.div(t, bit) + lax.div(e, bit), 2)
        return out

    def peers():
        return [peer(jnp.int32(e)) for e in range(nt)]

    pt = peers()

    def place(i):
        return {"context": i // nt, "tensor": lax.rem(i, nt)}

    def remote(src, dst, ss, rs, dev):
        return pltpu.make_async_remote_copy(
            src_ref=src, dst_ref=dst, send_sem=ss, recv_sem=rs, device_id=dev, device_id_type=MESH
        )

    def sent(region, sem):
        remote(region, region, sem, sem, {"tensor": pt[nt - 1]}).wait_send()

    def landed(region, sem):
        remote(region, region, sem, sem, {"tensor": pt[nt - 1]}).wait_recv()

    def copy(src, dst, ss, rs, dev):
        cp = remote(src, dst, ss, rs, dev)
        cp.start()
        return cp

    own_w = pltpu.make_async_copy(w_ref, wbuf.at[f], loc.at[0])
    own_w.start()
    loads = []
    for i, (src, dst) in enumerate((
        (x_hbm, x_ref), (bc_hbm, bc_ref), (dt_hbm, dt_ref), (taps_hbm, taps_ref), (bias_hbm, bias_ref),
        (gain_hbm, gain_ref), (down_hbm, down_ref), (up_hbm, up_ref), (cot_hbm, cot_ref),
        (sb_hbm, sb_ref), (dr_hbm, dr_ref), (sk_hbm, sk_ref),
    )):
        cp = pltpu.make_async_copy(src, dst, ld.at[i])
        cp.start()
        loads.append(cp)
    own_rows = pl.ds(pl.multiple_of(t * L, L), L)
    own_cols = pl.ds(pl.multiple_of(t * LW, 128), LW)
    own_z = pltpu.make_async_copy(z_ref.at[:, own_cols], z_all.at[own_rows, :], loc.at[1])
    own_z.start()

    nxt, prv = lax.rem(idx + 1, total), lax.rem(idx + total - 1, total)
    bar = pltpu.get_barrier_semaphore()
    greet = [{"tensor": pt[e]} for e in range(1, nt)]
    greet += [{"context": lax.rem(c + k, nc)} for k in range(1, nc)]
    greet += [place(nxt), place(prv)]
    for dev in greet:
        pl.semaphore_signal(bar, inc=1, device_id=dev, device_id_type=MESH)
    for near, to in ((f >= 1, f - 1), (f + 1 < nf, f + 1)):
        @pl.when(near)
        def _(to=to):
            pl.semaphore_signal(bar, inc=1, device_id={"fsdp": to}, device_id_type=MESH)

    pl.semaphore_wait(bar, len(greet) + (f >= 1).astype(jnp.int32) + (f + 1 < nf).astype(jnp.int32))

    own_w.wait()
    share = pl.ds(pl.multiple_of(c * R, 16), R)

    def w_copy(dr, s, ch, q):
        cols = pl.ds(chunks[ch][0], chunks[ch][1])
        src = wbuf.at[q, share, cols]
        to = f + 1 if dr == 0 else f - 1
        return remote(src, wbuf.at[q, share, cols], w_ss.at[dr, s], w_rs.at[q - dr, ch], {"fsdp": to})

    def w_share(dr, s, ch, q, k):
        region = wbuf.at[q, share, pl.ds(chunks[ch][0], chunks[ch][1])]
        return remote(region, region, wf_ss.at[q - dr], wf_rs.at[q - dr, ch], {"context": lax.rem(c + k, nc)})

    def has_next(dr):
        return f + 1 < nf if dr == 0 else f >= 1

    def sends(dr, s):
        return (f - s >= 0) & (f + 1 < nf) if dr == 0 else (f + s < nf) & (f >= 1)

    def gets(dr, s):
        return f - 1 - s >= 0 if dr == 0 else f + 1 + s < nf

    def came(dr, s):
        return f - 1 - s if dr == 0 else f + 1 + s

    for ch in range(len(chunks)):
        for dr in range(2):
            @pl.when(sends(dr, 0))
            def _(dr=dr, ch=ch):
                w_copy(dr, 0, ch, f).start()

    for cp in loads:
        cp.wait()
    h1 = copy(x_ref.at[L - HALO : L, :], halo_x, h_ss.at[0], h_rs.at[0], place(nxt))
    h2 = copy(bc_ref.at[L - HALO : L, :], halo_bc, h_ss.at[1], h_rs.at[1], place(nxt))
    for e in range(1, nt):
        copy(dt_ref, dt_all.at[t], dt_ss.at[0], dt_rs.at[0], {"tensor": pt[e]})
    dt_all[t] = dt_ref[...]

    def w_arrive(s, ch):
        for dr in range(2):
            @pl.when(gets(dr, s))
            def _(dr=dr):
                q = came(dr, s)
                w_copy(dr, s, ch, q).wait_recv()
                if s + 1 < steps:
                    @pl.when(has_next(dr))
                    def _():
                        w_copy(dr, s + 1, ch, q).start()
                for k in range(1, nc):
                    w_share(dr, s, ch, q, k).start()

    table = [sorted(range(nf), key=lambda q, g=g: (abs(q - g), q)) for g in range(nf)]
    order = [pick([table[g][i] for g in range(nf)], f) for i in range(nf)]
    way = [pick([int(table[g][i] > g) for g in range(nf)], f) for i in range(nf)]
    dist = [pick([max(abs(table[g][i] - g) - 1, 0) for g in range(nf)], f) for i in range(nf)]

    def w_ready(slot, ch):
        region = wbuf.at[order[slot], 0 : (nc - 1) * R, pl.ds(chunks[ch][0], chunks[ch][1])]
        if nc > 1:
            landed(region, wf_rs.at[order[slot] - way[slot], ch])

    def send_gate(e):
        cols = pl.ds(pl.multiple_of(pt[e] * LW, 128), LW)
        return copy(z_ref.at[:, cols], z_all.at[own_rows, :], z_ss.at[0], z_rs.at[e - 1], {"tensor": pt[e]})

    early = nt - 1 if nt > 2 else nt
    for e in range(1, early):
        send_gate(e)
    h1.wait()
    h2.wait()
    live = (idx > 0).astype(F32)

    def conv(src, halo, col, tap_col):
        lanes = pl.ds(col, 128)
        wide = pl.ds(tap_col, 128)
        ext = jnp.concatenate([halo[HALO - 8 : HALO, lanes].astype(F32) * live, src[:, lanes].astype(F32)], axis=0)
        acc = bias_ref[wide][None, :] + taps_ref[0:1, wide] * ext[5 : 5 + L]
        for k in range(1, 4):
            acc = acc + taps_ref[k : k + 1, wide] * ext[5 + k : 5 + k + L]
        return (acc / (1.0 + jnp.exp(-acc))).astype(BF)

    wide0 = x_ref.shape[1]
    for j in range(2 * N // 128):
        bc_all[own_rows, j * 128 : (j + 1) * 128] = conv(bc_ref, halo_bc, j * 128, wide0 + j * 128)
    bcs = [
        copy(bc_all.at[own_rows, :], bc_all.at[own_rows, :], bc_ss.at[0], bc_rs.at[e - 1], {"tensor": pt[e]})
        for e in range(1, nt)
    ]
    xs = []

    def conv_group(e, store):
        base = pt[e] * LW

        def lap(j, carry):
            col = pl.multiple_of(base + j * 128, 128)
            store(pl.ds(pl.multiple_of(j * 128, 128), 128), conv(x_ref, halo_x, col, col))
            return carry

        lax.fori_loop(0, LW // 128, lap, 0)

    for e in range(1, nt):
        def put(lanes, val, e=e):
            x_send[e - 1, :, lanes] = val

        conv_group(e, put)
        xs.append(copy(x_send.at[e - 1], x_all.at[own_rows, :], x_ss.at[0], x_rs.at[e - 1], {"tensor": pt[e]}))
    def put_own(lanes, val):
        x_all[own_rows, lanes] = val

    conv_group(0, put_own)
    e_s[...] = (iota((128, LW), 1) // HS == iota((128, LW), 0)).astype(F32)
    spread16 = e_s[...].astype(BF)

    def spread(rows):
        return dot(jnp.broadcast_to(rows, (8, 128)), e_s[...], precision=HI)

    landed(dt_all.at[0 : nt - 1], dt_rs.at[0])
    HR = at_s.shape[1]
    HA = dt_ref.shape[0]
    sel = ((iota((HA, 128), 0) == iota((HA, 128), 1) + t * hl) & (iota((HA, 128), 1) < hl)).astype(BF)
    sel_t = ((iota((HR, HA), 1) == iota((HR, HA), 0) + t * hl) & (iota((HR, HA), 0) < hl)).astype(BF)
    eye = (iota((HR, 128), 0) == iota((HR, 128), 1)).astype(F32)
    place_head = (iota((hl, 128), 0) == iota((hl, 128), 1)).astype(F32)
    hp = [
        dot(jnp.broadcast_to(v[...], (8, hl)), place_head, precision=HI)[0:1, :] for v in (sb_ref, dr_ref, sk_ref)
    ]
    hp_t = [dot(eye, jnp.broadcast_to(v, (8, 128)), 1, 1, HI)[:, 0:1] for v in hp[0:2]]
    tri = (iota((L, L), 0) >= iota((L, L), 1)).astype(F32)

    def softplus(v):
        return jnp.maximum(v, 0.0) + jnp.log1p(jnp.exp(-jnp.abs(v)))

    for b in range(nt):
        rows = slice(b * L, (b + 1) * L)
        raw = dt_all[b]
        step = softplus(dot(raw, sel, 0, 0) + hp[0])
        step_s[rows, :] = step
        a_s[rows, :] = dot(tri, -step * jnp.exp(hp[1]), precision=HI)
        step_t = softplus(dot(sel_t, raw) + hp_t[0])
        stept_s[b] = step_t
        at_s[b] = dot(-step_t * jnp.exp(hp_t[1]), tri, 1, 1, HI)
    before = jnp.zeros((1, 128), F32)
    for b in range(nt):
        last = a_s[(b + 1) * L - 1 : (b + 1) * L, :]
        stl[b, N : N + 8, :] = spread(jnp.exp(before))
        loc_s[b, N : N + 8, :] = spread(jnp.exp(last))
        before = before + last
    msg[N : N + 16, :] = jnp.broadcast_to(spread(jnp.exp(before))[0:1, :], (16, LW)).astype(BF)
    skip_s[...] = spread(hp[2])
    cu = dot(up_ref[...], cot_ref[...], 1, 1)
    left = iota((L, 2 * HS), 1) < HS

    def spans_of(e):
        b = pt[e]
        rows = pl.ds(pl.multiple_of(b * L, L), L)
        if e > 0:
            bcs[e - 1].wait_recv()
            xs[e - 1].wait_recv()
        a = a_s[rows, :]
        weight = (jnp.exp(a[L - 1 : L, :] - a) * step_s[rows, :]).astype(BF)
        xw = (x_all[rows, :].astype(F32) * dot(weight, spread16)).astype(BF)
        loc_s[b, 0:N, :] = dot(bc_all[rows, 0:N], xw, 0, 0)
        gram = dot(bc_all[rows, N : 2 * N], bc_all[rows, 0:N], 1, 1)
        gram = jnp.where(iota((L, L), 0) >= iota((L, L), 1), gram, 0.0)
        at = at_s[b]
        stt = stept_s[b]
        for pair in range(hl // 2):
            lanes = slice(pair * 2 * HS, (pair + 1) * 2 * HS)
            xp = x_all[rows, lanes]
            out = []
            for h in (2 * pair, 2 * pair + 1):
                gap = jnp.minimum(a[:, h : h + 1] - at[h : h + 1, :], 0.0)
                m = (jnp.exp(gap) * gram * stt[h : h + 1, :]).astype(BF)
                out.append(dot(m, xp))
            y_s[rows, lanes] = jnp.where(left, out[0], out[1])

    for e in range(nt):

        spans_of(e)
        if e == 0:
            w_arrive(0, 0)
        if e == min(1, nt - 2):
            for ch in range(1, len(chunks)):
                w_arrive(0, ch)
        if e == nt - 2:
            sent(x_send, x_ss.at[0])
            for i in range(early, nt):
                send_gate(i)

    state = jnp.zeros((N, LW), F32)
    for b in range(nt):
        stl[b, 0:N, :] = state
        state = loc_s[b, N : N + 1, :] * state + loc_s[b, 0:N, :]
    msg[0:N, :] = state.astype(BF)

    def state_copy(k, src):
        return remote(msg, st_in.at[src], st_ss.at[k - 1], st_rs.at[k - 1], {"context": lax.rem(c + k, nc)})

    for k in range(1, nc):
        @pl.when(c + k < nc)
        def _(k=k):
            state_copy(k, c).start()

    for k in range(1, nc):
        @pl.when(c >= k)
        def _(k=k):
            state_copy(k, lax.rem(c + nc - k, nc)).wait_recv()

    inc_s[...] = jnp.zeros_like(inc_s)

    def chain(k, carry):
        inc_s[...] = st_in[k, N : N + 16, :].astype(F32)[0:1, :] * inc_s[...] + st_in[k, 0:N, :].astype(F32)
        return carry

    lax.fori_loop(0, c, chain, 0)
    skip = skip_s[0:1, :]
    ones = jnp.ones((8, LW), BF)

    nx, ny = grid_of(nt)
    xi, yi = lax.rem(t, nx), lax.div(t, nx)
    top, low = slice(0, L // 2), slice(L // 2, L)
    xo = nx - 1 - xi

    def to_x(u, by, count):
        return remote(
            rs_send.at[pl.ds(by, count), xo, top, spans[u]], rs_in.at[pl.ds(by, count), :, spans[u]],
            rs_ss.at[0], rs_rs.at[u, 0], {"tensor": yi * nx + xo},
        )

    def to_y(u, j, bx, count):
        ty = lax.rem(yi + j, ny)
        src = rs_send.at[ty, pl.ds(bx, count), low, spans[u]]
        dst = rs_in.at[pl.ds(ny + (ny - j - 1) * nx + bx, count), :, spans[u]]
        return remote(src, dst, rs_ss.at[0], rs_rs.at[u, 0], {"tensor": ty * nx + xi})

    def send_block(u, by, bx):
        @pl.when(bx != xi)
        def _():
            to_x(u, by, 1).start()

        for j in range(1, ny):
            @pl.when(lax.rem(yi + j, ny) == by)
            def _(j=j):
                to_y(u, j, bx, 1).start()

    def near_cols(u):
        return pl.ds(units[u][1] - chunks[0][1], units[u][2])

    def send_unit(u):
        if u >= nf:
            for e in range(nt - 1, 0, -1):
                remote(
                    rs_send.at[lax.div(pt[e], nx), lax.rem(pt[e], nx), :, spans[u]], rs_near.at[e - 1, :, near_cols(u)],
                    rs_ss.at[2], rs_rs.at[u, 0], {"tensor": pt[e]},
                ).start()
            return
        to_x(u, 0, ny).start()
        for j in range(1, ny):
            to_y(u, j, 0, nx).start()

    def from_y(j, bx, cols):
        return rs_in[ny + (j - 1) * nx + bx, :, cols].astype(F32)

    def second(u):
        cols = spans[u]
        landed(rs_in.at[:, :, cols], rs_rs.at[u, 0])
        for j in range(1, ny):
            ty = lax.rem(yi + j, ny)
            sums[j - 1, :, cols] = (rs_send[ty, xi, top, cols].astype(F32) + rs_in[ty, :, cols].astype(F32)).astype(BF)
            remote(
                sums.at[j - 1, :, cols], sums_in.at[ny - j - 1, :, cols], rs_ss.at[1], rs_rs.at[u, 1],
                {"tensor": ty * nx + xi},
            ).start()
        acc = rs_send[yi, xo, low, cols].astype(F32)
        for j in range(1, ny):
            acc = acc + from_y(j, xo, cols)
        sums[ny - 1, :, cols] = acc.astype(BF)
        remote(
            sums.at[ny - 1, :, cols], sums_in.at[ny - 1, :, cols], rs_ss.at[1], rs_rs.at[u, 1],
            {"tensor": yi * nx + xo},
        ).start()

    units = [(s, 0, W) for s in range(nf - 1)] + [(nf - 1,) + chunk for chunk in chunks]
    spans = [pl.ds(pl.multiple_of(order[s] * W + off, 128), wide) for s, off, wide in units]

    def gate(e, carry):
        b = peer(e)
        rows = pl.ds(pl.multiple_of(b * L, L), L)

        @pl.when(e == 0)
        def _():
            own_z.wait()

        if steps > 1:
            @pl.when(e == 1)
            def _():
                w_arrive(1, 0)

            @pl.when(e == nt - 1)
            def _():
                for ch in range(1, nch - 1):
                    w_arrive(1, ch)

        @pl.when(e > 0)
        def _():
            remote(
                z_ref.at[:, own_cols], z_all.at[rows, :], z_ss.at[0], z_rs.at[e - 1], {"tensor": b}
            ).wait_recv()

        start = (stl[b, 0:N, :] + stl[b, N : N + 1, :] * inc_s[...]).astype(BF)
        reach = dot(jnp.exp(a_s[rows, :]).astype(BF), spread16)
        y = y_s[rows, :] + reach * dot(bc_all[rows, N : 2 * N], start)
        y = y + skip * x_all[rows, :].astype(F32)
        z = z_all[rows, :].astype(F32)
        g = y * (z / (1.0 + jnp.exp(-z)))
        out = (g * gain_ref[...][None, :]).astype(BF)
        g_s[rows, :] = out
        adx[b, 0:16, :] = dot(down_ref[...], out, 1, 1)
        adx[b, 16:24, :] = dot(ones, (g * g).astype(BF), 1, 1)

        @pl.when(e > 0)
        def _():
            remote(adx.at[b], ad_in.at[e], ad_ss.at[0], ad_rs.at[0], {"tensor": b}).start()

        by, bx = lax.div(b, nx), lax.rem(b, nx)
        rs_send[by, bx, :, spans[0]] = dot(out, wbuf[f]).astype(BF)

        @pl.when(e > 0)
        def _():
            send_block(0, by, bx)

        return carry

    lax.fori_loop(0, nt, gate, 0)

    def project(u):
        slot, off, wide = units[u]
        for ch in range(nch):
            if off <= chunks[ch][0] < off + wide:
                w_ready(slot, ch)

        def lap(by, carry):
            rows = pl.ds(pl.multiple_of(by * (nx * L), L), nx * L)
            out = dot(g_s[rows, :], wbuf[order[slot], :, off : off + wide]).astype(BF)
            for bx in range(nx):
                rs_send[by, bx, :, spans[u]] = out[bx * L : (bx + 1) * L]
            return carry

        lax.fori_loop(0, ny, lap, 0)

    project(1)
    send_unit(1)
    if steps > 1:
        for ch in range(max(nch - 1, 1), nch):
            w_arrive(1, ch)
    landed(ad_in.at[1:nt], ad_rs.at[0])
    red = adx[t]
    for e in range(1, nt):
        red = red + ad_in[e]
    scale_row = lax.rsqrt(red[16:17, :] / (LW * nt) + EPS)
    ad16 = red[0:16, :].astype(BF)
    factor = 2.0 / math.sqrt(L * nt * nc * nf)
    ag_own[...] = (factor * scale_row * cu).astype(BF)
    for e in range(1, nt):
        copy(ag_own, ag_all.at[t], ag_ss.at[0], ag_rs.at[0], {"tensor": pt[e]})
    gb_own[...] = dot((factor * scale_row * ad16.astype(F32)).astype(BF), cot_ref[...]).astype(BF)
    part = gb_own.shape[1] // nt
    own_part = pl.ds(pl.multiple_of(t * part, 128), part)
    for e in range(1, nt):
        copy(
            gb_own.at[:, pl.ds(pl.multiple_of(pt[e] * part, 128), part)],
            gb_in.at[e], ga_ss.at[0], ga_rs.at[0], {"tensor": pt[e]},
        )
    scale_col = dot(jnp.broadcast_to(scale_row, (8, L)), jnp.full((8, 128), 0.125, F32), 0, 0, HI)[:, 0:1]
    for s in range(2, nf - 1):
        if s > 2:
            for ch in range(nch):
                w_arrive(s - 1, ch)
        project(s)
        send_unit(s)
    second(0)
    second(1)
    landed(ag_all.at[0 : nt - 1], ag_rs.at[0])
    landed(gb_in.at[1:nt], ga_rs.at[0])
    def finish(u):
        cols = spans[u]
        if u >= nf:
            landed(rs_near.at[:, :, near_cols(u)], rs_rs.at[u, 0])
            acc = rs_send[yi, xi, :, cols].astype(F32)
            for e in range(1, nt):
                acc = acc + rs_near[e - 1, :, near_cols(u)].astype(F32)
        else:
            landed(sums_in.at[:, :, cols], rs_rs.at[u, 1])
            up_part = rs_send[yi, xi, top, cols].astype(F32) + rs_in[yi, :, cols].astype(F32)
            low_part = rs_send[yi, xi, low, cols].astype(F32) + sums_in[ny - 1, :, cols].astype(F32)
            for j in range(1, ny):
                up_part = up_part + sums_in[j - 1, :, cols].astype(F32)
                low_part = low_part + from_y(j, xi, cols)
            acc = jnp.concatenate([up_part, low_part], axis=0)
        acc = acc + 2.0 * dot(ad16, up_ref[:, cols], 0, 0)
        mixed_ref[:, cols] = (scale_col * acc).astype(BF)

    ag_all[t] = ag_own[...]
    grad = jnp.zeros((16, LW), F32)
    for s in range(nt):
        grad = grad + dot(ag_all[s], g_s[s * L : (s + 1) * L, :])
    comb[:, 0:LW] = grad
    acc = gb_own[:, own_part].astype(F32)
    for e in range(1, nt):
        acc = acc + gb_in[e].astype(F32)
    comb[:, LW : LW + part] = acc
    lanes = (LW + part) // 128
    per = -(-lanes // nc)

    def seg(i):
        return pl.ds(pl.multiple_of(jnp.minimum(i * per, lanes - per) * 128, 128), per * 128)

    ccs = [
        copy(comb.at[:, seg(lax.rem(c + k, nc))], comb_c.at[k], cc_ss.at[k - 1], cc_rs.at[k - 1], {"context": lax.rem(c + k, nc)})
        for k in range(1, nc)
    ]
    for cp in ccs:
        cp.wait()
    acc = comb[:, seg(c)]
    for k in range(1, nc):
        acc = acc + comb_c[k]
    comb2[...] = acc.astype(BF)
    mid = (nf - 1) // 2

    @pl.when(f != mid)
    def _():
        copy(comb2, comb_f.at[f], cf_ss.at[0], cf_rs.at[0], {"fsdp": mid})

    last = nf - 1
    for u in range(2, last):
        second(u)
    near = dist[nf - 1] < steps - 1

    def last_slot(ch):
        project(last + ch)
        send_unit(last + ch)

    @pl.when(near)
    def _():
        for ch in range(nch):
            last_slot(ch)

    w_arrive(steps - 1, 0)

    @pl.when(jnp.logical_not(near))
    def _():
        last_slot(0)

    finish(0)
    @pl.when(f == mid)
    def _():
        landed(comb_f.at[0 : nf - 1], cf_rs.at[0])
        comb_f[mid] = comb2[...]
        acc = comb_f[0].astype(F32)
        for k in range(1, nf):
            acc = acc + comb_f[k].astype(F32)
        tot[...] = acc.astype(BF)
        for k in range(1, nf):
            copy(tot, tot, tot_ss.at[0], tot_rs.at[0], {"fsdp": lax.rem(mid + k, nf)})

    finish(1)
    for ch in range(1, nch):
        w_arrive(steps - 1, ch)
        if ch == nch - 1:
            @pl.when(f != mid)
            def _():
                landed(tot, tot_rs.at[0])

            sgs = [
                copy(tot, seg_in.at[c], sg_ss.at[k - 1], sg_rs.at[k - 1], {"context": lax.rem(c + k, nc)})
                for k in range(1, nc)
            ]
            seg_in[c] = tot[...]

        @pl.when(jnp.logical_not(near))
        def _(ch=ch):
            last_slot(ch)

        if ch == 1:
            for u in range(2, last):
                finish(u)
            second(last)
    for cp in sgs:
        cp.wait()
    for i in range(nc):
        full[:, seg(i)] = seg_in[i].astype(F32)
    ga_ref[...] = full[:, 0:LW]
    fin[t] = full[:, LW : LW + part].astype(BF)
    for e in range(nt - 1, 0, -1):
        copy(fin.at[t], fin.at[t], fin_ss.at[0], fin_rs.at[0], {"tensor": pt[e]})
    for ch in range(nch):
        finish(last + ch)
    landed(fin.at[0 : nt - 1], fin_rs.at[0])
    for s in range(nt):
        gb_ref[:, s * part : (s + 1) * part] = fin[s].astype(F32)
    sent(dt_all.at[0 : nt - 1], dt_ss.at[0])
    for k in range(1, nc):
        @pl.when(c + k < nc)
        def _(k=k):
            state_copy(k, c).wait_send()

    sent(bc_all.at[0 : (nt - 1) * L, :], bc_ss.at[0])
    sent(z_all.at[0 : (nt - 1) * L, :], z_ss.at[0])
    sent(ad_in.at[1:nt], ad_ss.at[0])
    sent(ag_all.at[0 : nt - 1], ag_ss.at[0])
    sent(gb_in.at[1:nt], ga_ss.at[0])

    @pl.when(f != mid)
    def _():
        sent(comb2, cf_ss.at[0])

    @pl.when(f == mid)
    def _():
        sent(comb_f.at[0 : nf - 1], tot_ss.at[0])

    sent(fin.at[0 : nt - 1], fin_ss.at[0])
    head = slice(0, rs_in.shape[2] - W + chunks[0][1])
    sent(rs_in.at[:, :, head], rs_ss.at[0])
    sent(sums_in.at[:, :, head], rs_ss.at[1])
    sent(rs_near, rs_ss.at[2])
    for s in range(steps):
        for dr in range(2):
            @pl.when(sends(dr, s))
            def _(dr=dr, s=s):
                sent(wbuf.at[0, 0:R, :], w_ss.at[dr, s])

            if nc > 1:
                @pl.when(gets(dr, s))
                def _(dr=dr, s=s):
                    sent(wbuf.at[0, 0 : (nc - 1) * R, :], wf_ss.at[came(dr, s) - dr])


def write_out(mixed, ga, gb, mixed_out, ga_out, gb_out, sem):
    copies = [
        pltpu.make_async_copy(src, dst, sem.at[i])
        for i, (src, dst) in enumerate(((mixed, mixed_out), (ga, ga_out), (gb, gb_out)))
    ]
    for cp in copies:
        cp.start()
    for cp in copies:
        cp.wait()


def shards(x, bc, z, dt, taps, bias, step_bias, rate, skip, gain, w, down, up, cot):
    nt, nf, nc = lax.axis_size("tensor"), lax.axis_size("fsdp"), lax.axis_size("context")
    L, full = x.shape[1], x.shape[2]
    LW, hl, W, M = gain.shape[0], step_bias.shape[0], w.shape[1], cot.shape[2]
    BC = bc.shape[2]
    N = BC // 2
    HR = -(-hl // 8) * 8
    T = nt * L
    part = M // nt
    nx, ny = grid_of(nt)
    dt = dt[0].T
    down = down.T
    nch = len(column_chunks(W))
    units = nf - 1 + nch
    lanes = (LW + part) // 128
    SW = -(-lanes // nc) * 128
    vm = pl.BlockSpec(memory_space=pltpu.VMEM)
    hbm = pl.BlockSpec(memory_space=pl.ANY)
    V = pltpu.VMEM
    D = pltpu.SemaphoreType.DMA
    scratch = [
        V((L, full), BF), V((L, BC), BF), V(dt.shape, BF), V(taps.shape, F32), V((full + BC,), F32), V((LW,), F32),
        V(down.shape, BF), V(up.shape, BF), V((L, M), BF), V((1, hl), F32), V((1, hl), F32), V((1, hl), F32),
        V((HALO, full), BF), V((HALO, BC), BF), V((nt - 1, L, LW), BF), V((T, LW), BF), V((T, LW), BF),
        V((T, BC), BF), V((nt,) + dt.shape, BF), V((nf, LW, W), BF), V((T, 128), F32), V((T, 128), F32),
        V((nt, HR, L), F32), V((nt, HR, L), F32),
        V((nt, N + 8, LW), F32), V((nt, N + 8, LW), F32), V((8, LW), F32), V((N + 16, LW), BF), V((nc, N + 16, LW), BF), V((N, LW), F32),
        V((128, LW), F32), V((T, LW), F32), V((T, LW), BF), V((nt, 24, L), F32), V((nt, 24, L), F32),
        V((16, L), BF), V((nt, 16, L), BF), V((16, M), BF), V((nt, 16, part), BF),
        V((16, LW + part), F32), V((nc, 16, SW), F32), V((16, SW), BF), V((nf, 16, SW), BF),
        V((16, SW), BF), V((nc, 16, SW), BF), V((16, LW + part), F32),
        V((nt, 16, part), BF), V((ny, nx, L, M), BF), V((ny + (ny - 1) * nx, L // 2, M), BF),
        V((ny, L // 2, M), BF), V((ny, L // 2, M), BF), V((nt - 1, L, W - column_chunks(W)[0][1]), BF),
        D((12,)), D((2,)), D((2,)), D((1,)), D((1,)), D((1,)), D((nt - 1,)), D((1,)), D((nt - 1,)), D((1,)), D((nt - 1,)),
        D((2, nf - 1)), D((nf - 1, nch)), D((nf - 1,)), D((nf - 1, nch)), D((nc - 1,)), D((nc - 1,)),
        D((1,)), D((1,)), D((1,)), D((1,)), D((1,)), D((1,)), D((nc - 1,)), D((nc - 1,)), D((1,)), D((1,)), D((1,)), D((1,)),
        D((nc - 1,)), D((nc - 1,)), D((1,)), D((1,)), D((3,)), D((units, 2)), D((2,)),
    ]
    mixed, ga, gb = pl.pallas_call(
        functools.partial(kernel, nt, nf, nc, hl),
        out_shape=(V((L, M), BF), V((16, LW), F32), V((16, M), F32)),
        in_specs=[hbm] * 14,
        out_specs=(vm, vm, vm),
        scratch_shapes=scratch,
        compiler_params=pltpu.CompilerParams(
            collective_id=0, has_side_effects=True, vmem_limit_bytes=62 * 1024 * 1024
        ),
    )(x[0], bc[0], z[0], dt, taps, bias, step_bias[None], rate[None], skip[None], gain, w, down, up, cot[0])
    mixed, ga, gb = (pltpu.with_memory_space_constraint(v, pltpu.VMEM) for v in (mixed, ga, gb))
    mixed, ga, gb = pl.pallas_call(
        write_out,
        out_shape=(
            jax.ShapeDtypeStruct((L, M), BF),
            jax.ShapeDtypeStruct((16, LW), F32),
            jax.ShapeDtypeStruct((16, M), F32),
        ),
        in_specs=[vm, vm, vm],
        out_specs=(hbm, hbm, hbm),
        scratch_shapes=[D((3,))],
    )(mixed, ga, gb)
    return mixed[None], ga.T, gb


def solution(mesh):
    tokens = P("fsdp", ("context", "tensor"), None)
    placed = (
        tokens, tokens, tokens, tokens, P(), P(), P("tensor"), P("tensor"), P("tensor"), P("tensor"),
        P("tensor", "fsdp"), P("tensor", None), P(), tokens,
    )
    return jax.shard_map(
        shards, mesh=mesh, in_specs=placed, out_specs=(tokens, P("tensor", None), P()), check_vma=False
    )
```

```python
import functools
import math

import jax
import jax.numpy as jnp
from jax import lax
from jax.experimental import pallas as pl
from jax.experimental.pallas import tpu as pltpu
from jax.sharding import PartitionSpec as P

EPS = 1e-05
MESH = pl.DeviceIdType.MESH
HI = lax.Precision.HIGHEST
BF = jnp.bfloat16
F32 = jnp.float32
HALO = 8


def dot(a, b, ca=1, cb=0, precision=None):
    return lax.dot_general(
        a, b, (((ca,), (cb,)), ((), ())), preferred_element_type=F32, precision=precision
    )


def iota(shape, dim):
    return lax.broadcasted_iota(jnp.int32, shape, dim)


def pick(values, i):
    out = jnp.int32(values[0])
    for k in range(1, len(values)):
        out = jnp.where(i == k, jnp.int32(values[k]), out)
    return out


def grid_of(count):
    return 2, count // 2


def column_chunks(width):
    cuts = sorted({0, max(width - 256, 128), max(width - 128, 128), width})
    return [(a, b - a) for a, b in zip(cuts, cuts[1:])]


def kernel(
    nt, nf, nc, hl,
    x_hbm, bc_hbm, z_ref, dt_hbm, taps_hbm, bias_hbm, sb_hbm, dr_hbm, sk_hbm, gain_hbm, w_ref, down_hbm, up_hbm, cot_hbm,
    mixed_ref, ga_ref, gb_ref,
    x_ref, bc_ref, dt_ref, taps_ref, bias_ref, gain_ref, down_ref, up_ref, cot_ref, sb_ref, dr_ref, sk_ref,
    halo_x, halo_bc, x_send, x_all, z_all, bc_all, dt_all, wbuf, a_s, step_s, at_s, stept_s,
    stl, loc_s, skip_s, msg, st_in, inc_s, e_s, y_s, g_s, adx, ad_in, ag_own, ag_all, gb_own, gb_in,
    comb, comb_c, comb2, comb_f, tot, seg_in, full, fin, rs_send, rs_in, sums, sums_in, rs_near,
    ld, h_ss, h_rs, dt_ss, dt_rs, bc_ss, bc_rs, x_ss, x_rs, z_ss, z_rs, w_ss, w_rs, wf_ss, wf_rs, st_ss, st_rs,
    ad_ss, ad_rs, ag_ss, ag_rs, ga_ss, ga_rs, cc_ss, cc_rs, cf_ss, cf_rs, tot_ss, tot_rs, sg_ss, sg_rs, fin_ss, fin_rs, rs_ss, rs_rs, loc,
):
    t = lax.axis_index("tensor")
    f = lax.axis_index("fsdp")
    c = lax.axis_index("context")
    L = x_ref.shape[0]
    LW = x_all.shape[1]
    W = w_ref.shape[1]
    N = bc_ref.shape[1] // 2
    R = w_ref.shape[0] // nc
    HS = LW // hl
    idx = c * nt + t
    total = nc * nt
    bits = [1 << i for i in range(nt.bit_length() - 1)]
    chunks = column_chunks(W)
    nch = len(chunks)
    steps = nf - 1

    def peer(e):
        out = 0
        for bit in bits:
            out = out + bit * lax.rem(lax.div(t, bit) + lax.div(e, bit), 2)
        return out

    def peers():
        return [peer(jnp.int32(e)) for e in range(nt)]

    pt = peers()

    def place(i):
        return {"context": i // nt, "tensor": lax.rem(i, nt)}

    def remote(src, dst, ss, rs, dev):
        return pltpu.make_async_remote_copy(
            src_ref=src, dst_ref=dst, send_sem=ss, recv_sem=rs, device_id=dev, device_id_type=MESH
        )

    def sent(region, sem):
        remote(region, region, sem, sem, {"tensor": pt[nt - 1]}).wait_send()

    def landed(region, sem):
        remote(region, region, sem, sem, {"tensor": pt[nt - 1]}).wait_recv()

    def copy(src, dst, ss, rs, dev):
        cp = remote(src, dst, ss, rs, dev)
        cp.start()
        return cp

    own_w = pltpu.make_async_copy(w_ref, wbuf.at[f], loc.at[0])
    own_w.start()
    loads = []
    for i, (src, dst) in enumerate((
        (x_hbm, x_ref), (bc_hbm, bc_ref), (dt_hbm, dt_ref), (taps_hbm, taps_ref), (bias_hbm, bias_ref),
        (gain_hbm, gain_ref), (down_hbm, down_ref), (up_hbm, up_ref), (cot_hbm, cot_ref),
        (sb_hbm, sb_ref), (dr_hbm, dr_ref), (sk_hbm, sk_ref),
    )):
        cp = pltpu.make_async_copy(src, dst, ld.at[i])
        cp.start()
        loads.append(cp)
    own_rows = pl.ds(pl.multiple_of(t * L, L), L)
    own_cols = pl.ds(pl.multiple_of(t * LW, 128), LW)
    own_z = pltpu.make_async_copy(z_ref.at[:, own_cols], z_all.at[own_rows, :], loc.at[1])
    own_z.start()

    nxt, prv = lax.rem(idx + 1, total), lax.rem(idx + total - 1, total)
    bar = pltpu.get_barrier_semaphore()
    greet = [{"tensor": pt[e]} for e in range(1, nt)]
    greet += [{"context": lax.rem(c + k, nc)} for k in range(1, nc)]
    greet += [place(nxt), place(prv)]
    for dev in greet:
        pl.semaphore_signal(bar, inc=1, device_id=dev, device_id_type=MESH)
    for near, to in ((f >= 1, f - 1), (f + 1 < nf, f + 1)):
        @pl.when(near)
        def _(to=to):
            pl.semaphore_signal(bar, inc=1, device_id={"fsdp": to}, device_id_type=MESH)

    pl.semaphore_wait(bar, len(greet) + (f >= 1).astype(jnp.int32) + (f + 1 < nf).astype(jnp.int32))

    own_w.wait()
    share = pl.ds(pl.multiple_of(c * R, 16), R)

    def w_copy(dr, s, ch, q):
        cols = pl.ds(chunks[ch][0], chunks[ch][1])
        src = wbuf.at[q, share, cols]
        to = f + 1 if dr == 0 else f - 1
        return remote(src, wbuf.at[q, share, cols], w_ss.at[dr, s], w_rs.at[q - dr, ch], {"fsdp": to})

    def w_share(dr, s, ch, q, k):
        region = wbuf.at[q, share, pl.ds(chunks[ch][0], chunks[ch][1])]
        return remote(region, region, wf_ss.at[q - dr], wf_rs.at[q - dr, ch], {"context": lax.rem(c + k, nc)})

    def has_next(dr):
        return f + 1 < nf if dr == 0 else f >= 1

    def sends(dr, s):
        return (f - s >= 0) & (f + 1 < nf) if dr == 0 else (f + s < nf) & (f >= 1)

    def gets(dr, s):
        return f - 1 - s >= 0 if dr == 0 else f + 1 + s < nf

    def came(dr, s):
        return f - 1 - s if dr == 0 else f + 1 + s

    for ch in range(len(chunks)):
        for dr in range(2):
            @pl.when(sends(dr, 0))
            def _(dr=dr, ch=ch):
                w_copy(dr, 0, ch, f).start()

    for cp in loads:
        cp.wait()
    h1 = copy(x_ref.at[L - HALO : L, :], halo_x, h_ss.at[0], h_rs.at[0], place(nxt))
    h2 = copy(bc_ref.at[L - HALO : L, :], halo_bc, h_ss.at[1], h_rs.at[1], place(nxt))
    for e in range(1, nt):
        copy(dt_ref, dt_all.at[t], dt_ss.at[0], dt_rs.at[0], {"tensor": pt[e]})
    dt_all[t] = dt_ref[...]

    def w_arrive(s, ch):
        for dr in range(2):
            @pl.when(gets(dr, s))
            def _(dr=dr):
                q = came(dr, s)
                w_copy(dr, s, ch, q).wait_recv()
                if s + 1 < steps:
                    @pl.when(has_next(dr))
                    def _():
                        w_copy(dr, s + 1, ch, q).start()
                for k in range(1, nc):
                    w_share(dr, s, ch, q, k).start()

    table = [sorted(range(nf), key=lambda q, g=g: (abs(q - g), q)) for g in range(nf)]
    order = [pick([table[g][i] for g in range(nf)], f) for i in range(nf)]
    way = [pick([int(table[g][i] > g) for g in range(nf)], f) for i in range(nf)]
    dist = [pick([max(abs(table[g][i] - g) - 1, 0) for g in range(nf)], f) for i in range(nf)]

    def w_ready(slot, ch):
        region = wbuf.at[order[slot], 0 : (nc - 1) * R, pl.ds(chunks[ch][0], chunks[ch][1])]
        if nc > 1:
            landed(region, wf_rs.at[order[slot] - way[slot], ch])

    def send_gate(e):
        cols = pl.ds(pl.multiple_of(pt[e] * LW, 128), LW)
        return copy(z_ref.at[:, cols], z_all.at[own_rows, :], z_ss.at[0], z_rs.at[e - 1], {"tensor": pt[e]})

    early = nt - 1 if nt > 2 else nt
    for e in range(1, early):
        send_gate(e)
    h1.wait()
    h2.wait()
    live = (idx > 0).astype(F32)

    def conv(src, halo, col, tap_col):
        lanes = pl.ds(col, 128)
        wide = pl.ds(tap_col, 128)
        ext = jnp.concatenate([halo[HALO - 8 : HALO, lanes].astype(F32) * live, src[:, lanes].astype(F32)], axis=0)
        acc = bias_ref[wide][None, :] + taps_ref[0:1, wide] * ext[5 : 5 + L]
        for k in range(1, 4):
            acc = acc + taps_ref[k : k + 1, wide] * ext[5 + k : 5 + k + L]
        return (acc / (1.0 + jnp.exp(-acc))).astype(BF)

    wide0 = x_ref.shape[1]
    for j in range(2 * N // 128):
        bc_all[own_rows, j * 128 : (j + 1) * 128] = conv(bc_ref, halo_bc, j * 128, wide0 + j * 128)
    bcs = [
        copy(bc_all.at[own_rows, :], bc_all.at[own_rows, :], bc_ss.at[0], bc_rs.at[e - 1], {"tensor": pt[e]})
        for e in range(1, nt)
    ]
    xs = []

    def conv_group(e, store):
        base = pt[e] * LW

        def lap(j, carry):
            col = pl.multiple_of(base + j * 128, 128)
            store(pl.ds(pl.multiple_of(j * 128, 128), 128), conv(x_ref, halo_x, col, col))
            return carry

        lax.fori_loop(0, LW // 128, lap, 0)

    for e in range(1, nt):
        def put(lanes, val, e=e):
            x_send[e - 1, :, lanes] = val

        conv_group(e, put)
        xs.append(copy(x_send.at[e - 1], x_all.at[own_rows, :], x_ss.at[0], x_rs.at[e - 1], {"tensor": pt[e]}))
    def put_own(lanes, val):
        x_all[own_rows, lanes] = val

    conv_group(0, put_own)
    e_s[...] = (iota((128, LW), 1) // HS == iota((128, LW), 0)).astype(F32)
    spread16 = e_s[...].astype(BF)

    def spread(rows):
        return dot(jnp.broadcast_to(rows, (8, 128)), e_s[...], precision=HI)

    landed(dt_all.at[0 : nt - 1], dt_rs.at[0])
    HR = at_s.shape[1]
    HA = dt_ref.shape[0]
    sel = ((iota((HA, 128), 0) == iota((HA, 128), 1) + t * hl) & (iota((HA, 128), 1) < hl)).astype(BF)
    sel_t = ((iota((HR, HA), 1) == iota((HR, HA), 0) + t * hl) & (iota((HR, HA), 0) < hl)).astype(BF)
    eye = (iota((HR, 128), 0) == iota((HR, 128), 1)).astype(F32)
    place_head = (iota((hl, 128), 0) == iota((hl, 128), 1)).astype(F32)
    hp = [
        dot(jnp.broadcast_to(v[...], (8, hl)), place_head, precision=HI)[0:1, :] for v in (sb_ref, dr_ref, sk_ref)
    ]
    hp_t = [dot(eye, jnp.broadcast_to(v, (8, 128)), 1, 1, HI)[:, 0:1] for v in hp[0:2]]
    tri = (iota((L, L), 0) >= iota((L, L), 1)).astype(F32)

    def softplus(v):
        return jnp.maximum(v, 0.0) + jnp.log1p(jnp.exp(-jnp.abs(v)))

    for b in range(nt):
        rows = slice(b * L, (b + 1) * L)
        raw = dt_all[b]
        step = softplus(dot(raw, sel, 0, 0) + hp[0])
        step_s[rows, :] = step
        a_s[rows, :] = dot(tri, -step * jnp.exp(hp[1]), precision=HI)
        step_t = softplus(dot(sel_t, raw) + hp_t[0])
        stept_s[b] = step_t
        at_s[b] = dot(-step_t * jnp.exp(hp_t[1]), tri, 1, 1, HI)
    before = jnp.zeros((1, 128), F32)
    for b in range(nt):
        last = a_s[(b + 1) * L - 1 : (b + 1) * L, :]
        stl[b, N : N + 8, :] = spread(jnp.exp(before))
        loc_s[b, N : N + 8, :] = spread(jnp.exp(last))
        before = before + last
    msg[N : N + 16, :] = jnp.broadcast_to(spread(jnp.exp(before))[0:1, :], (16, LW)).astype(BF)
    skip_s[...] = spread(hp[2])
    cu = dot(up_ref[...], cot_ref[...], 1, 1)
    left = iota((L, 2 * HS), 1) < HS

    def spans_of(e):
        b = pt[e]
        rows = pl.ds(pl.multiple_of(b * L, L), L)
        if e > 0:
            bcs[e - 1].wait_recv()
            xs[e - 1].wait_recv()
        a = a_s[rows, :]
        weight = (jnp.exp(a[L - 1 : L, :] - a) * step_s[rows, :]).astype(BF)
        xw = (x_all[rows, :].astype(F32) * dot(weight, spread16)).astype(BF)
        loc_s[b, 0:N, :] = dot(bc_all[rows, 0:N], xw, 0, 0)
        gram = dot(bc_all[rows, N : 2 * N], bc_all[rows, 0:N], 1, 1)
        gram = jnp.where(iota((L, L), 0) >= iota((L, L), 1), gram, 0.0)
        at = at_s[b]
        stt = stept_s[b]
        for pair in range(hl // 2):
            lanes = slice(pair * 2 * HS, (pair + 1) * 2 * HS)
            xp = x_all[rows, lanes]
            out = []
            for h in (2 * pair, 2 * pair + 1):
                gap = jnp.minimum(a[:, h : h + 1] - at[h : h + 1, :], 0.0)
                m = (jnp.exp(gap) * gram * stt[h : h + 1, :]).astype(BF)
                out.append(dot(m, xp))
            y_s[rows, lanes] = jnp.where(left, out[0], out[1])

    for e in range(nt):

        spans_of(e)
        if e == 0:
            w_arrive(0, 0)
        if e == min(1, nt - 2):
            for ch in range(1, len(chunks)):
                w_arrive(0, ch)
        if e == nt - 2:
            sent(x_send, x_ss.at[0])
            for i in range(early, nt):
                send_gate(i)

    state = jnp.zeros((N, LW), F32)
    for b in range(nt):
        stl[b, 0:N, :] = state
        state = loc_s[b, N : N + 1, :] * state + loc_s[b, 0:N, :]
    msg[0:N, :] = state.astype(BF)

    def state_copy(k, src):
        return remote(msg, st_in.at[src], st_ss.at[k - 1], st_rs.at[k - 1], {"context": lax.rem(c + k, nc)})

    for k in range(1, nc):
        @pl.when(c + k < nc)
        def _(k=k):
            state_copy(k, c).start()

    for k in range(1, nc):
        @pl.when(c >= k)
        def _(k=k):
            state_copy(k, lax.rem(c + nc - k, nc)).wait_recv()

    inc_s[...] = jnp.zeros_like(inc_s)

    def chain(k, carry):
        inc_s[...] = st_in[k, N : N + 16, :].astype(F32)[0:1, :] * inc_s[...] + st_in[k, 0:N, :].astype(F32)
        return carry

    lax.fori_loop(0, c, chain, 0)
    skip = skip_s[0:1, :]
    ones = jnp.ones((8, LW), BF)

    nx, ny = grid_of(nt)
    xi, yi = lax.rem(t, nx), lax.div(t, nx)
    top, low = slice(0, L // 2), slice(L // 2, L)
    xo = nx - 1 - xi

    def to_x(u, by, count):
        return remote(
            rs_send.at[pl.ds(by, count), xo, top, spans[u]], rs_in.at[pl.ds(by, count), :, spans[u]],
            rs_ss.at[0], rs_rs.at[u, 0], {"tensor": yi * nx + xo},
        )

    def to_y(u, j, bx, count):
        ty = lax.rem(yi + j, ny)
        src = rs_send.at[ty, pl.ds(bx, count), low, spans[u]]
        dst = rs_in.at[pl.ds(ny + (ny - j - 1) * nx + bx, count), :, spans[u]]
        return remote(src, dst, rs_ss.at[0], rs_rs.at[u, 0], {"tensor": ty * nx + xi})

    def send_block(u, by, bx):
        @pl.when(bx != xi)
        def _():
            to_x(u, by, 1).start()

        for j in range(1, ny):
            @pl.when(lax.rem(yi + j, ny) == by)
            def _(j=j):
                to_y(u, j, bx, 1).start()

    def near_cols(u):
        return pl.ds(units[u][1] - chunks[0][1], units[u][2])

    def send_unit(u):
        if u >= nf:
            for e in range(nt - 1, 0, -1):
                remote(
                    rs_send.at[lax.div(pt[e], nx), lax.rem(pt[e], nx), :, spans[u]], rs_near.at[e - 1, :, near_cols(u)],
                    rs_ss.at[2], rs_rs.at[u, 0], {"tensor": pt[e]},
                ).start()
            return
        to_x(u, 0, ny).start()
        for j in range(1, ny):
            to_y(u, j, 0, nx).start()

    def from_y(j, bx, cols):
        return rs_in[ny + (j - 1) * nx + bx, :, cols].astype(F32)

    def second(u):
        cols = spans[u]
        landed(rs_in.at[:, :, cols], rs_rs.at[u, 0])
        for j in range(1, ny):
            ty = lax.rem(yi + j, ny)
            sums[j - 1, :, cols] = (rs_send[ty, xi, top, cols].astype(F32) + rs_in[ty, :, cols].astype(F32)).astype(BF)
            remote(
                sums.at[j - 1, :, cols], sums_in.at[ny - j - 1, :, cols], rs_ss.at[1], rs_rs.at[u, 1],
                {"tensor": ty * nx + xi},
            ).start()
        acc = rs_send[yi, xo, low, cols].astype(F32)
        for j in range(1, ny):
            acc = acc + from_y(j, xo, cols)
        sums[ny - 1, :, cols] = acc.astype(BF)
        remote(
            sums.at[ny - 1, :, cols], sums_in.at[ny - 1, :, cols], rs_ss.at[1], rs_rs.at[u, 1],
            {"tensor": yi * nx + xo},
        ).start()

    units = [(s, 0, W) for s in range(nf - 1)] + [(nf - 1,) + chunk for chunk in chunks]
    spans = [pl.ds(pl.multiple_of(order[s] * W + off, 128), wide) for s, off, wide in units]

    def gate(e, carry):
        b = peer(e)
        rows = pl.ds(pl.multiple_of(b * L, L), L)

        @pl.when(e == 0)
        def _():
            own_z.wait()

        if steps > 1:
            @pl.when(e == 1)
            def _():
                w_arrive(1, 0)

            @pl.when(e == nt - 1)
            def _():
                for ch in range(1, nch - 1):
                    w_arrive(1, ch)

        @pl.when(e > 0)
        def _():
            remote(
                z_ref.at[:, own_cols], z_all.at[rows, :], z_ss.at[0], z_rs.at[e - 1], {"tensor": b}
            ).wait_recv()

        start = (stl[b, 0:N, :] + stl[b, N : N + 1, :] * inc_s[...]).astype(BF)
        reach = dot(jnp.exp(a_s[rows, :]).astype(BF), spread16)
        y = y_s[rows, :] + reach * dot(bc_all[rows, N : 2 * N], start)
        y = y + skip * x_all[rows, :].astype(F32)
        z = z_all[rows, :].astype(F32)
        g = y * (z / (1.0 + jnp.exp(-z)))
        out = (g * gain_ref[...][None, :]).astype(BF)
        g_s[rows, :] = out
        adx[b, 0:16, :] = dot(down_ref[...], out, 1, 1)
        adx[b, 16:24, :] = dot(ones, (g * g).astype(BF), 1, 1)

        @pl.when(e > 0)
        def _():
            remote(adx.at[b], ad_in.at[e], ad_ss.at[0], ad_rs.at[0], {"tensor": b}).start()

        by, bx = lax.div(b, nx), lax.rem(b, nx)
        rs_send[by, bx, :, spans[0]] = dot(out, wbuf[f]).astype(BF)

        @pl.when(e > 0)
        def _():
            send_block(0, by, bx)

        return carry

    lax.fori_loop(0, nt, gate, 0)

    def project(u):
        slot, off, wide = units[u]
        for ch in range(nch):
            if off <= chunks[ch][0] < off + wide:
                w_ready(slot, ch)

        def lap(by, carry):
            rows = pl.ds(pl.multiple_of(by * (nx * L), L), nx * L)
            out = dot(g_s[rows, :], wbuf[order[slot], :, off : off + wide]).astype(BF)
            for bx in range(nx):
                rs_send[by, bx, :, spans[u]] = out[bx * L : (bx + 1) * L]
            return carry

        lax.fori_loop(0, ny, lap, 0)

    project(1)
    send_unit(1)
    if steps > 1:
        for ch in range(max(nch - 1, 1), nch):
            w_arrive(1, ch)
    landed(ad_in.at[1:nt], ad_rs.at[0])
    red = adx[t]
    for e in range(1, nt):
        red = red + ad_in[e]
    scale_row = lax.rsqrt(red[16:17, :] / (LW * nt) + EPS)
    ad16 = red[0:16, :].astype(BF)
    factor = 2.0 / math.sqrt(L * nt * nc * nf)
    ag_own[...] = (factor * scale_row * cu).astype(BF)
    for e in range(1, nt):
        copy(ag_own, ag_all.at[t], ag_ss.at[0], ag_rs.at[0], {"tensor": pt[e]})
    gb_own[...] = dot((factor * scale_row * ad16.astype(F32)).astype(BF), cot_ref[...]).astype(BF)
    part = gb_own.shape[1] // nt
    own_part = pl.ds(pl.multiple_of(t * part, 128), part)
    for e in range(1, nt):
        copy(
            gb_own.at[:, pl.ds(pl.multiple_of(pt[e] * part, 128), part)],
            gb_in.at[e], ga_ss.at[0], ga_rs.at[0], {"tensor": pt[e]},
        )
    scale_col = dot(jnp.broadcast_to(scale_row, (8, L)), jnp.full((8, 128), 0.125, F32), 0, 0, HI)[:, 0:1]
    for s in range(2, nf - 1):
        if s > 2:
            for ch in range(nch):
                w_arrive(s - 1, ch)
        project(s)
        send_unit(s)
    second(0)
    second(1)
    landed(ag_all.at[0 : nt - 1], ag_rs.at[0])
    landed(gb_in.at[1:nt], ga_rs.at[0])
    def finish(u):
        cols = spans[u]
        if u >= nf:
            landed(rs_near.at[:, :, near_cols(u)], rs_rs.at[u, 0])
            acc = rs_send[yi, xi, :, cols].astype(F32)
            for e in range(1, nt):
                acc = acc + rs_near[e - 1, :, near_cols(u)].astype(F32)
        else:
            landed(sums_in.at[:, :, cols], rs_rs.at[u, 1])
            up_part = rs_send[yi, xi, top, cols].astype(F32) + rs_in[yi, :, cols].astype(F32)
            low_part = rs_send[yi, xi, low, cols].astype(F32) + sums_in[ny - 1, :, cols].astype(F32)
            for j in range(1, ny):
                up_part = up_part + sums_in[j - 1, :, cols].astype(F32)
                low_part = low_part + from_y(j, xi, cols)
            acc = jnp.concatenate([up_part, low_part], axis=0)
        acc = acc + 2.0 * dot(ad16, up_ref[:, cols], 0, 0)
        mixed_ref[:, cols] = (scale_col * acc).astype(BF)

    ag_all[t] = ag_own[...]
    grad = jnp.zeros((16, LW), F32)
    for s in range(nt):
        grad = grad + dot(ag_all[s], g_s[s * L : (s + 1) * L, :])
    comb[:, 0:LW] = grad
    acc = gb_own[:, own_part].astype(F32)
    for e in range(1, nt):
        acc = acc + gb_in[e].astype(F32)
    comb[:, LW : LW + part] = acc
    lanes = (LW + part) // 128
    per = -(-lanes // nc)

    def seg(i):
        return pl.ds(pl.multiple_of(jnp.minimum(i * per, lanes - per) * 128, 128), per * 128)

    ccs = [
        copy(comb.at[:, seg(lax.rem(c + k, nc))], comb_c.at[k], cc_ss.at[k - 1], cc_rs.at[k - 1], {"context": lax.rem(c + k, nc)})
        for k in range(1, nc)
    ]
    for cp in ccs:
        cp.wait()
    acc = comb[:, seg(c)]
    for k in range(1, nc):
        acc = acc + comb_c[k]
    comb2[...] = acc.astype(BF)
    mid = (nf - 1) // 2

    @pl.when(f != mid)
    def _():
        copy(comb2, comb_f.at[f], cf_ss.at[0], cf_rs.at[0], {"fsdp": mid})

    w_arrive(steps - 1, 0)
    last = nf - 1
    for u in range(2, last):
        second(u)
    near = dist[nf - 1] < steps - 1

    def last_slot(ch):
        project(last + ch)
        send_unit(last + ch)

    @pl.when(near)
    def _():
        for ch in range(nch):
            last_slot(ch)


    @pl.when(jnp.logical_not(near))
    def _():
        last_slot(0)

    finish(0)
    @pl.when(f == mid)
    def _():
        landed(comb_f.at[0 : nf - 1], cf_rs.at[0])
        comb_f[mid] = comb2[...]
        acc = comb_f[0].astype(F32)
        for k in range(1, nf):
            acc = acc + comb_f[k].astype(F32)
        tot[...] = acc.astype(BF)
        for k in range(1, nf):
            copy(tot, tot, tot_ss.at[0], tot_rs.at[0], {"fsdp": lax.rem(mid + k, nf)})

    finish(1)
    for ch in range(1, nch):
        w_arrive(steps - 1, ch)
        if ch == nch - 1:
            @pl.when(f != mid)
            def _():
                landed(tot, tot_rs.at[0])

            sgs = [
                copy(tot, seg_in.at[c], sg_ss.at[k - 1], sg_rs.at[k - 1], {"context": lax.rem(c + k, nc)})
                for k in range(1, nc)
            ]
            seg_in[c] = tot[...]
            for cp in sgs:
                cp.wait()
            for i in range(nc):
                full[:, seg(i)] = seg_in[i].astype(F32)
            ga_ref[...] = full[:, 0:LW]
            fin[t] = full[:, LW : LW + part].astype(BF)
            for e in range(nt - 1, 0, -1):
                copy(fin.at[t], fin.at[t], fin_ss.at[0], fin_rs.at[0], {"tensor": pt[e]})

        @pl.when(jnp.logical_not(near))
        def _(ch=ch):
            last_slot(ch)

        if ch == 1:
            for u in range(2, last):
                finish(u)
            second(last)
    for ch in range(nch):
        finish(last + ch)
    landed(fin.at[0 : nt - 1], fin_rs.at[0])
    for s in range(nt):
        gb_ref[:, s * part : (s + 1) * part] = fin[s].astype(F32)
    sent(dt_all.at[0 : nt - 1], dt_ss.at[0])
    for k in range(1, nc):
        @pl.when(c + k < nc)
        def _(k=k):
            state_copy(k, c).wait_send()

    sent(bc_all.at[0 : (nt - 1) * L, :], bc_ss.at[0])
    sent(z_all.at[0 : (nt - 1) * L, :], z_ss.at[0])
    sent(ad_in.at[1:nt], ad_ss.at[0])
    sent(ag_all.at[0 : nt - 1], ag_ss.at[0])
    sent(gb_in.at[1:nt], ga_ss.at[0])

    @pl.when(f != mid)
    def _():
        sent(comb2, cf_ss.at[0])

    @pl.when(f == mid)
    def _():
        sent(comb_f.at[0 : nf - 1], tot_ss.at[0])

    sent(fin.at[0 : nt - 1], fin_ss.at[0])
    head = slice(0, rs_in.shape[2] - W + chunks[0][1])
    sent(rs_in.at[:, :, head], rs_ss.at[0])
    sent(sums_in.at[:, :, head], rs_ss.at[1])
    sent(rs_near, rs_ss.at[2])
    for s in range(steps):
        for dr in range(2):
            @pl.when(sends(dr, s))
            def _(dr=dr, s=s):
                sent(wbuf.at[0, 0:R, :], w_ss.at[dr, s])

            if nc > 1:
                @pl.when(gets(dr, s))
                def _(dr=dr, s=s):
                    sent(wbuf.at[0, 0 : (nc - 1) * R, :], wf_ss.at[came(dr, s) - dr])


def write_out(mixed, ga, gb, mixed_out, ga_out, gb_out, sem):
    copies = [
        pltpu.make_async_copy(src, dst, sem.at[i])
        for i, (src, dst) in enumerate(((mixed, mixed_out), (ga, ga_out), (gb, gb_out)))
    ]
    for cp in copies:
        cp.start()
    for cp in copies:
        cp.wait()


def shards(x, bc, z, dt, taps, bias, step_bias, rate, skip, gain, w, down, up, cot):
    nt, nf, nc = lax.axis_size("tensor"), lax.axis_size("fsdp"), lax.axis_size("context")
    L, full = x.shape[1], x.shape[2]
    LW, hl, W, M = gain.shape[0], step_bias.shape[0], w.shape[1], cot.shape[2]
    BC = bc.shape[2]
    N = BC // 2
    HR = -(-hl // 8) * 8
    T = nt * L
    part = M // nt
    nx, ny = grid_of(nt)
    dt = dt[0].T
    down = down.T
    nch = len(column_chunks(W))
    units = nf - 1 + nch
    lanes = (LW + part) // 128
    SW = -(-lanes // nc) * 128
    vm = pl.BlockSpec(memory_space=pltpu.VMEM)
    hbm = pl.BlockSpec(memory_space=pl.ANY)
    V = pltpu.VMEM
    D = pltpu.SemaphoreType.DMA
    scratch = [
        V((L, full), BF), V((L, BC), BF), V(dt.shape, BF), V(taps.shape, F32), V((full + BC,), F32), V((LW,), F32),
        V(down.shape, BF), V(up.shape, BF), V((L, M), BF), V((1, hl), F32), V((1, hl), F32), V((1, hl), F32),
        V((HALO, full), BF), V((HALO, BC), BF), V((nt - 1, L, LW), BF), V((T, LW), BF), V((T, LW), BF),
        V((T, BC), BF), V((nt,) + dt.shape, BF), V((nf, LW, W), BF), V((T, 128), F32), V((T, 128), F32),
        V((nt, HR, L), F32), V((nt, HR, L), F32),
        V((nt, N + 8, LW), F32), V((nt, N + 8, LW), F32), V((8, LW), F32), V((N + 16, LW), BF), V((nc, N + 16, LW), BF), V((N, LW), F32),
        V((128, LW), F32), V((T, LW), F32), V((T, LW), BF), V((nt, 24, L), F32), V((nt, 24, L), F32),
        V((16, L), BF), V((nt, 16, L), BF), V((16, M), BF), V((nt, 16, part), BF),
        V((16, LW + part), F32), V((nc, 16, SW), F32), V((16, SW), BF), V((nf, 16, SW), BF),
        V((16, SW), BF), V((nc, 16, SW), BF), V((16, LW + part), F32),
        V((nt, 16, part), BF), V((ny, nx, L, M), BF), V((ny + (ny - 1) * nx, L // 2, M), BF),
        V((ny, L // 2, M), BF), V((ny, L // 2, M), BF), V((nt - 1, L, W - column_chunks(W)[0][1]), BF),
        D((12,)), D((2,)), D((2,)), D((1,)), D((1,)), D((1,)), D((nt - 1,)), D((1,)), D((nt - 1,)), D((1,)), D((nt - 1,)),
        D((2, nf - 1)), D((nf - 1, nch)), D((nf - 1,)), D((nf - 1, nch)), D((nc - 1,)), D((nc - 1,)),
        D((1,)), D((1,)), D((1,)), D((1,)), D((1,)), D((1,)), D((nc - 1,)), D((nc - 1,)), D((1,)), D((1,)), D((1,)), D((1,)),
        D((nc - 1,)), D((nc - 1,)), D((1,)), D((1,)), D((3,)), D((units, 2)), D((2,)),
    ]
    mixed, ga, gb = pl.pallas_call(
        functools.partial(kernel, nt, nf, nc, hl),
        out_shape=(V((L, M), BF), V((16, LW), F32), V((16, M), F32)),
        in_specs=[hbm] * 14,
        out_specs=(vm, vm, vm),
        scratch_shapes=scratch,
        compiler_params=pltpu.CompilerParams(
            collective_id=0, has_side_effects=True, vmem_limit_bytes=62 * 1024 * 1024
        ),
    )(x[0], bc[0], z[0], dt, taps, bias, step_bias[None], rate[None], skip[None], gain, w, down, up, cot[0])
    mixed, ga, gb = (pltpu.with_memory_space_constraint(v, pltpu.VMEM) for v in (mixed, ga, gb))
    mixed, ga, gb = pl.pallas_call(
        write_out,
        out_shape=(
            jax.ShapeDtypeStruct((L, M), BF),
            jax.ShapeDtypeStruct((16, LW), F32),
            jax.ShapeDtypeStruct((16, M), F32),
        ),
        in_specs=[vm, vm, vm],
        out_specs=(hbm, hbm, hbm),
        scratch_shapes=[D((3,))],
    )(mixed, ga, gb)
    return mixed[None], ga.T, gb


def solution(mesh):
    tokens = P("fsdp", ("context", "tensor"), None)
    placed = (
        tokens, tokens, tokens, tokens, P(), P(), P("tensor"), P("tensor"), P("tensor"), P("tensor"),
        P("tensor", "fsdp"), P("tensor", None), P(), tokens,
    )
    return jax.shard_map(
        shards, mesh=mesh, in_specs=placed, out_specs=(tokens, P("tensor", None), P()), check_vma=False
    )
```
